32 devices in a mesh: dp: 4 (over y, x), frame: 8 (over z, core).
Axes of the slice: x: 2, y: 2, z: 4, core: 2. Of those that a mesh axis runs over, the one named last changes fastest.
Arguments:
- frames_in: bfloat16 [4, 8, 64, 1024], P('dp', 'frame'), may hold values from -6 to 6
- bottleneck: bfloat16 [4, 4, 1024], P('dp'), may hold values from -6 to 6
- spatial_entry: bfloat16 [1024, 1536], replicated, may hold values from -2 to 2
- spatial_exit: bfloat16 [1024, 512], replicated, may hold values from -0.25 to 0.25
- temporal_entry: bfloat16 [1024, 1536], replicated, may hold values from -2 to 2
- temporal_exit: bfloat16 [1024, 512], replicated, may hold values from -0.25 to 0.25
- output_grad: bfloat16 [4, 8, 64, 1024], P('dp', 'frame'), may hold values from -6 to 6
- joined_grad: bfloat16 [4, 4, 1024], P('dp'), may hold values from -6 to 6
Outputs:
- frames_delta: bfloat16 [4, 8, 64, 1024], P('dp', 'frame')
- bottleneck_delta: bfloat16 [4, 4, 1024], P('dp')
- spatialin_grad: bfloat16 [1024, 1536], P(('dp', 'frame'))
- spatialout_grad: bfloat16 [1024, 512], P(('dp', 'frame'))
- temporalin_grad: bfloat16 [1024, 1536], P(('dp', 'frame'))
- temporalout_grad: bfloat16 [1024, 512], P(('dp', 'frame'))
The draws below stay inside these ranges and needn't reach their ends.
All inputs are finite; a program needn't handle non-finite values.
Results may differ from the reference program's by a relative error of at most 0.024.
Values may be sent and summed in bfloat16 or wider, within the bound.
A program may use at most 64 MiB of HBM per device.

```python
import math
import jax
import jax.numpy as jnp
from jax import lax

D = 1024
HEAD = 64
HEADS = 8
BOT = 4
CLIPS = 4
FRAMES = 8
PATCHES = 64


def entry_draw(key):
    base_key = jax.random.fold_in(key, 0)
    drawn = jax.random.normal(base_key, (D, 3 * HEADS * HEAD), jnp.float32) / math.sqrt(D)
    return jnp.clip(drawn, -2.0, 2.0)


def draw_spatial_entry(key, part):
    return entry_draw(jax.random.fold_in(key, 17)).astype(jnp.bfloat16)


def draw_temporal_entry(key, part):
    return entry_draw(jax.random.fold_in(key, 29)).astype(jnp.bfloat16)


def strengthened(values, key, source, target, blocks, factor):
    owner, partner = [(jnp.arange(values.shape[dim]) // (values.shape[dim] // blocks)).reshape([-1 if axis == dim else 1 for axis in range(values.ndim)]) for dim in (source, target)]
    chosen = jax.random.permutation(key, blocks)[partner]
    strong = (owner == chosen) | (owner == (partner + blocks // 2) % blocks)
    return jnp.where(strong, factor * values, values)


def block_levels(stream_key, extent, cuts, least, largest):
    level = 1.0
    for dim, parts in cuts:
        draws = jax.random.uniform(jax.random.fold_in(jax.random.fold_in(stream_key, 6), dim), (parts,), jnp.float32, least / len(cuts), largest / len(cuts))
        level = level * jnp.repeat(jnp.exp(draws), extent[dim] // parts).reshape((-1,) + (1,) * (len(extent) - 1 - dim))
    return level


def scatter_about(own_key, dims, spread, limit, cuts=(), dtype=jnp.bfloat16):
    loudness = block_levels(own_key, dims, cuts, -0.22, 0.18) if cuts else 1.0
    array = jax.random.normal(own_key, dims, jnp.float32) * spread * loudness
    return jnp.minimum(jnp.maximum(array, -limit), limit).astype(dtype)


def noise_with(stream_key, shape, deviation, limit, cuts, heavy, dtype=jnp.bfloat16):
    values = deviation * jax.random.normal(stream_key, shape, jnp.float32)
    if cuts:
        values = values * block_levels(stream_key, shape, cuts, -0.22, 0.18)
    return jnp.clip(strengthened(values, jax.random.fold_in(stream_key, 3), *heavy), -limit, limit).astype(dtype)


def setup_inputs(seed: int = 0) -> dict:
    arg_keys = jax.random.split(jax.random.key(seed), 9)
    return {
        "frames_in": scatter_about(arg_keys[0], (CLIPS, FRAMES, PATCHES, D), 1.0, 6.0, ((0, 4), (1, 8))),
        "bottleneck": scatter_about(arg_keys[1], (CLIPS, BOT, D), 1.0, 6.0, ((0, 4),)),
        "spatial_entry": draw_spatial_entry(jax.random.fold_in(arg_keys[8], 71), 0),
        "spatial_exit": scatter_about(arg_keys[3], (D, HEADS * HEAD), (HEADS * HEAD) ** -0.5, 0.25),
        "temporal_entry": draw_temporal_entry(jax.random.fold_in(arg_keys[8], 71), 0),
        "temporal_exit": scatter_about(arg_keys[5], (D, HEADS * HEAD), (HEADS * HEAD) ** -0.5, 0.25),
        "output_grad": noise_with(arg_keys[6], (CLIPS, FRAMES, PATCHES, D), 1.0, 6.0, ((0, 4), (1, 8)), (1, 3, 8, 2.0)),
        "joined_grad": scatter_about(arg_keys[7], (CLIPS, BOT, D), 1.0, 6.0, ((0, 4),)),
    }


EPSILON = 1e-05

def product_form(form, left, right):
    left, right = lax.optimization_barrier((left, right))
    return jnp.einsum(form, left.astype(jnp.float32), right.astype(jnp.float32), preferred_element_type=jnp.float32)

def product_general(left, right, numbers):
    left, right = lax.optimization_barrier((left, right))
    return lax.dot_general(left.astype(jnp.float32), right.astype(jnp.float32), numbers, preferred_element_type=jnp.float32)

def normalize(inputs):
    widened = lax.optimization_barrier(inputs).astype(jnp.float32)
    centred = widened - lax.optimization_barrier(jnp.mean(widened, axis=-1, keepdims=True))
    inverse = lax.rsqrt(lax.optimization_barrier(jnp.mean(centred * centred, axis=-1, keepdims=True)) + EPSILON)
    return (centred * inverse, inverse)

def attend(inputs, entry_weight, head_count):
    normed, inverse = normalize(inputs)
    normed_low = normed.astype(jnp.bfloat16)
    mixture = product_general(normed_low, entry_weight, (((3,), (0,)), ((), ()))).astype(jnp.bfloat16)
    lead_count, seq_length, side_count = (inputs.shape[0], inputs.shape[1], inputs.shape[2])
    head_width = entry_weight.shape[1] // 3
    head_size = head_width // head_count
    pieces = mixture.reshape(lead_count, seq_length, side_count, 3, head_count, head_size)
    queries = pieces[:, :, :, 0]
    key_heads = pieces[:, :, :, 1]
    values = pieces[:, :, :, 2]
    factor = 1.0 / math.sqrt(head_size)
    scores = product_form('albhe,ambhe->abhlm', queries, key_heads) * factor
    scores = scores - lax.optimization_barrier(jnp.max(scores, axis=-1, keepdims=True))
    expon = jnp.exp(scores)
    softmax_weights = expon / lax.optimization_barrier(jnp.sum(expon, axis=-1, keepdims=True))
    softmax_low = softmax_weights.astype(jnp.bfloat16)
    attended = product_form('abhlm,ambhe->albhe', softmax_low, values).astype(jnp.bfloat16)
    attended = attended.reshape(lead_count, seq_length, side_count, head_width)
    return (normed, inverse, normed_low, queries, key_heads, values, softmax_weights, softmax_low, attended)

def project_out(inputs, attended, exit_weight):
    return lax.optimization_barrier(inputs).astype(jnp.float32) + product_general(attended, exit_weight, (((3,), (1,)), ((), ())))

def backward(cotangent, saved, entry_weight, exit_weight, head_count):
    normed, inverse, normed_low, queries, key_heads, values, softmax_weights, softmax_low, attended = saved
    lead_count, seq_length, side_count = (cotangent.shape[0], cotangent.shape[1], cotangent.shape[2])
    head_width = exit_weight.shape[1]
    head_size = head_width // head_count
    factor = 1.0 / math.sqrt(head_size)
    rows_dims = (((0, 1, 2), (0, 1, 2)), ((), ()))
    exit_grad = product_general(cotangent, attended, rows_dims)
    attended_grad = product_general(cotangent, exit_weight, (((3,), (0,)), ((), ()))).astype(jnp.bfloat16)
    attended_grad = attended_grad.reshape(lead_count, seq_length, side_count, head_count, head_size)
    softmax_grad = product_form('albhe,ambhe->abhlm', attended_grad, values)
    values_grad = product_form('abhlm,albhe->ambhe', softmax_low, attended_grad)
    centre = lax.optimization_barrier(jnp.sum(softmax_weights * softmax_grad, axis=-1, keepdims=True))
    scores_grad = (softmax_weights * (softmax_grad - centre) * factor).astype(jnp.bfloat16)
    queries_grad = product_form('abhlm,ambhe->albhe', scores_grad, key_heads)
    keys_grad = product_form('abhlm,albhe->ambhe', scores_grad, queries)
    mixture_grad = jnp.stack([queries_grad, keys_grad, values_grad], axis=3).astype(jnp.bfloat16)
    mixture_grad = mixture_grad.reshape(lead_count, seq_length, side_count, 3 * head_width)
    entry_grad = product_general(normed_low, mixture_grad, rows_dims)
    normed_grad = product_general(mixture_grad, entry_weight, (((3,), (1,)), ((), ())))
    inner_term = normed_grad - lax.optimization_barrier(jnp.mean(normed_grad, axis=-1, keepdims=True)) - normed * lax.optimization_barrier(jnp.mean(normed_grad * normed, axis=-1, keepdims=True))
    inputs_grad = lax.optimization_barrier(cotangent).astype(jnp.float32) + inverse * inner_term
    return (inputs_grad, entry_grad, exit_grad)

def reference(frames_in, bottleneck, spatial_entry, spatial_exit, temporal_entry, temporal_exit, output_grad, joined_grad):

    def per_clip(carry, items):
        frames, bottle, output_cot, joined_cot = items
        tokens_in = jnp.concatenate([frames, jnp.broadcast_to(bottle[None], (FRAMES, BOT, D))], axis=1)
        sequences = tokens_in[:, :, None, :]
        spatial_saved = attend(sequences, spatial_entry, HEADS)
        block_out = project_out(sequences, spatial_saved[8], spatial_exit)
        states = block_out[:, :PATCHES, 0, :].astype(jnp.bfloat16)[None]
        temporal_saved = attend(states, temporal_entry, HEADS)
        states_grad, temporal_in, temporal_out = backward(output_cot[None], temporal_saved, temporal_entry, temporal_exit, HEADS)
        state_grads = states_grad[0].astype(jnp.bfloat16)
        joined_rows = (lax.optimization_barrier(joined_cot).astype(jnp.float32) / FRAMES).astype(jnp.bfloat16)
        cotangent = jnp.concatenate([state_grads, jnp.broadcast_to(joined_rows[None], (FRAMES, BOT, D))], axis=1)[:, :, None, :]
        tokens_grad, spatial_in, spatial_out = backward(cotangent, spatial_saved, spatial_entry, spatial_exit, HEADS)
        frames_delta = tokens_grad[:, :PATCHES, 0, :].astype(jnp.bfloat16)
        bottleneck_delta = lax.optimization_barrier(jnp.sum(tokens_grad[:, PATCHES:, 0, :], axis=0)).astype(jnp.bfloat16)
        updated = (carry[0] + spatial_in, carry[1] + spatial_out, carry[2] + temporal_in, carry[3] + temporal_out)
        return (updated, (frames_delta, bottleneck_delta))
    start = (jnp.zeros((D, 3 * HEADS * HEAD), jnp.float32), jnp.zeros((D, HEADS * HEAD), jnp.float32), jnp.zeros((D, 3 * HEADS * HEAD), jnp.float32), jnp.zeros((D, HEADS * HEAD), jnp.float32))
    totals, stacked = lax.scan(per_clip, start, (frames_in, bottleneck, output_grad, joined_grad))
    grad_factor = 1.0 / math.sqrt(CLIPS * FRAMES * PATCHES)
    spatialin_grad = (totals[0] * grad_factor).astype(jnp.bfloat16)
    spatialout_grad = (totals[1] * grad_factor).astype(jnp.bfloat16)
    temporalin_grad = (totals[2] * grad_factor).astype(jnp.bfloat16)
    temporalout_grad = (totals[3] * grad_factor).astype(jnp.bfloat16)
    return (stacked[0], stacked[1], spatialin_grad, spatialout_grad, temporalin_grad, temporalout_grad)
```

```python
import functools
import math

import jax
import jax.numpy as jnp
from jax import lax
from jax.experimental import pallas as pl
from jax.experimental.pallas import tpu as pltpu
from jax.sharding import PartitionSpec as P

HEADS = 8
EPSILON = 1e-05
MESH = pl.DeviceIdType.MESH
F32 = jnp.float32
BF16 = jnp.bfloat16


def dot(left, right, left_dim=1, right_dim=0):
    return lax.dot_general(
        left, right, (((left_dim,), (right_dim,)), ((), ())), preferred_element_type=F32
    )


def normalize(widened):
    centred = widened - jnp.mean(widened, axis=-1, keepdims=True)
    inverse = lax.rsqrt(jnp.mean(centred * centred, axis=-1, keepdims=True) + EPSILON)
    return centred * inverse, inverse


def head_masks(width, dtype):
    lanes = lax.broadcasted_iota(jnp.int32, (1, width), 1)
    size = width // HEADS
    return [
        jnp.where((lanes >= h * size) & (lanes < (h + 1) * size), 1.0, 0.0).astype(dtype)
        for h in range(HEADS)
    ]


def stack_heads(rows):
    return jnp.concatenate([rows * m for m in head_masks(rows.shape[1], rows.dtype)], axis=0)


def merge_heads(stacked):
    count = stacked.shape[0] // HEADS
    masks = head_masks(stacked.shape[1], stacked.dtype)
    total = stacked[:count] * masks[0]
    for h in range(1, HEADS):
        total = total + stacked[h * count : (h + 1) * count] * masks[h]
    return total


def attend(normed_low, entry_ref, mask, between):
    mixture = dot(normed_low, entry_ref[...]).astype(BF16)
    between()
    width = mixture.shape[1] // 3
    queries, key_rows, values = (mixture[:, i * width : (i + 1) * width] for i in range(3))
    factor = 1.0 / math.sqrt(width // HEADS)
    query_stack = stack_heads(queries)
    scores = dot(query_stack, key_rows, 1, 1) * factor
    scores = jnp.where(mask, scores, -1e30)
    scores = scores - jnp.max(scores, axis=-1, keepdims=True)
    expon = jnp.where(mask, jnp.exp(scores), 0.0)
    weights = expon / jnp.sum(expon, axis=-1, keepdims=True)
    weights_low = weights.astype(BF16)
    attended = merge_heads(dot(weights_low, values)).astype(BF16)
    return attended, (query_stack, key_rows, values, weights, weights_low)


def backward_mixture(cotangent, exit_ref, saved, emit):
    query_stack, key_rows, values, weights, weights_low = saved
    factor = 1.0 / math.sqrt(values.shape[1] // HEADS)
    attended_grad = dot(cotangent, exit_ref[...]).astype(BF16)
    grad_stack = stack_heads(attended_grad)
    values_grad = dot(weights_low, grad_stack, 0, 0).astype(BF16)
    emit(2, values_grad)
    softmax_grad = dot(grad_stack, values, 1, 1)
    centre = jnp.sum(weights * softmax_grad, axis=-1, keepdims=True)
    scores_grad = (weights * (softmax_grad - centre) * factor).astype(BF16)
    keys_grad = dot(scores_grad, query_stack, 0, 0).astype(BF16)
    emit(1, keys_grad)
    queries_grad = merge_heads(dot(scores_grad, key_rows)).astype(BF16)
    emit(0, queries_grad)
    return jnp.concatenate([queries_grad, keys_grad, values_grad], axis=1)


def backward_inputs(mixture_grad, entry_ref, cotangent, normed, inverse):
    normed_grad = dot(mixture_grad, entry_ref[...], 1, 1)
    inner = (
        normed_grad
        - jnp.mean(normed_grad, axis=-1, keepdims=True)
        - normed * jnp.mean(normed_grad * normed, axis=-1, keepdims=True)
    )
    return cotangent + inverse * inner


def kernel(
    frame_groups,
    row_groups,
    column_groups,
    grad_factor,
    frames_hbm,
    bottle_hbm,
    output_grad_hbm,
    joined_hbm,
    spatial_entry_hbm,
    spatial_exit_hbm,
    temporal_entry_hbm,
    temporal_exit_hbm,
    frames_delta_hbm,
    bottle_delta_hbm,
    spatialin_hbm,
    spatialout_hbm,
    temporalin_hbm,
    temporalout_hbm,
    frames_ref,
    bottle_ref,
    og_send,
    joined_ref,
    se_ref,
    so_ref,
    te_ref,
    to_ref,
    frames_delta_ref,
    bottle_delta_ref,
    spatialin_ref,
    spatialout_ref,
    temporalin_ref,
    temporalout_ref,
    tokens,
    cot_ref,
    s_normed,
    t_normed,
    og_recv,
    st_send,
    st_recv,
    sg_send,
    sg_recv,
    bot_sum,
    bot_recv,
    s_nl_send,
    s_nl,
    s_att_send,
    s_att,
    s_c_send,
    s_c,
    s_mg_send,
    s_mg,
    t_nl_send,
    t_nl,
    t_att_send,
    t_att,
    t_c_send,
    t_c,
    t_mg_send,
    t_mg,
    *tail,
):
    bits = frame_groups.bit_length() - 1
    part = tail[0]
    received = tail[1 : 1 + bits]
    sums = (part,) + tuple(tail[1 + bits : 1 + 2 * bits])
    (
        load_sem,
        out_sem,
        f_send_sem,
        f_recv_sem,
        d_send_sem,
        d_recv_sem,
        r_send_sem,
        r_recv_sem,
        x_send_sem,
        x_recv_sem,
    ) = tail[1 + 2 * bits :]
    frame = lax.axis_index("frame")
    data = lax.axis_index("dp")
    row_at = data // column_groups
    column_at = lax.rem(data, column_groups)
    data_groups = row_groups * column_groups
    patches, model = frames_ref.shape
    bottles = bottle_ref.shape[0]
    rows = tokens.shape[0]
    sent_rows = s_nl.shape[1]
    group = og_send.shape[1]
    width = to_ref.shape[1]
    block = width // column_groups
    side = [lax.rem(frame // (1 << s), 2) for s in range(bits)]

    loads = {}

    def load(name, src, dst):
        loads[name] = pltpu.make_async_copy(src, dst, load_sem.at[len(loads)])
        loads[name].start()

    load("frames", frames_hbm, frames_ref)
    load("bottle", bottle_hbm, bottle_ref)
    load("se", spatial_entry_hbm, se_ref)
    load("og", output_grad_hbm, og_send)
    load("so", spatial_exit_hbm, so_ref)
    load("te", temporal_entry_hbm, te_ref)
    load("to", temporal_exit_hbm, to_ref)
    load("joined", joined_hbm, joined_ref)

    barrier = pltpu.get_barrier_semaphore()
    for k in range(1, frame_groups):
        pl.semaphore_signal(
            barrier,
            inc=1,
            device_id={"frame": lax.rem(frame + k, frame_groups)},
            device_id_type=MESH,
        )
    for k in range(1, data_groups):
        pl.semaphore_signal(
            barrier, inc=1, device_id={"dp": lax.rem(data + k, data_groups)}, device_id_type=MESH
        )

    pending = []

    def push(src, dst, send_sem, recv_sem, device):
        copy = pltpu.make_async_remote_copy(
            src_ref=src,
            dst_ref=dst,
            send_sem=send_sem,
            recv_sem=recv_sem,
            device_id=device,
            device_id_type=MESH,
        )
        copy.start()
        pending.append(copy)
        return copy

    def arrive(copies):
        for copy in copies:
            copy.wait_recv()

    def across(k):
        peer = frame
        for s in range(bits):
            if k >> s & 1:
                peer = peer + (1 << s) * (1 - 2 * side[s])
        return peer

    def exchange_frames(send, dst, phase):
        copies = []
        for k in reversed(range(1, frame_groups)):
            peer = across(k)
            copies.append(
                push(
                    send.at[peer],
                    dst.at[frame],
                    f_send_sem.at[phase, k],
                    f_recv_sem.at[phase, k],
                    {"frame": peer},
                )
            )
        dst[frame] = send[frame]
        return copies

    def spread(send, dst, by_row, phase):
        copies = []
        for k in reversed(range(1, data_groups)):
            peer_row = lax.rem(row_at + k // column_groups, row_groups)
            peer_column = lax.rem(column_at + k % column_groups, column_groups)
            copies.append(
                push(
                    send.at[peer_row if by_row else peer_column],
                    dst.at[data],
                    d_send_sem.at[phase, k],
                    d_recv_sem.at[phase, k],
                    {"dp": peer_row * column_groups + peer_column},
                )
            )
        dst[data] = send[row_at if by_row else column_at]
        return copies

    def put_blocks(dst, value):
        count, kept, size = dst.shape
        for i in range(count):
            dst[i] = value[:kept, i * size : (i + 1) * size]

    def share_rows(send, dst, value, phase):
        put_blocks(send, value)
        return spread(send, dst, True, phase)

    def share_columns(send, dst, value, phase):
        put_blocks(send, value)
        return spread(send, dst, False, phase)

    og_copies = []

    def enter():
        with jax.named_scope("a02_enter"):
            pl.semaphore_wait(barrier, frame_groups + data_groups - 2)
            loads["og"].wait()
            og_copies.extend(exchange_frames(og_send, og_recv, 0))

    with jax.named_scope("a01_norm"):
        loads["frames"].wait()
        loads["bottle"].wait()
        tokens[:patches] = frames_ref[...].astype(F32)
        tokens[patches:] = jnp.zeros((rows - patches, model), F32)
        tokens[patches : patches + bottles] = bottle_ref[...].astype(F32)
        normed, s_inverse = normalize(tokens[...])
        s_normed[...] = normed
        s_low = normed.astype(BF16)
        loads["se"].wait()
    columns = lax.broadcasted_iota(jnp.int32, (HEADS * rows, rows), 1)
    attended, s_saved = attend(s_low, se_ref, columns < patches + bottles, enter)
    with jax.named_scope("a03_states"):
        loads["so"].wait()
        states = (tokens[:patches] + dot(attended[:patches], so_ref[...], 1, 1)).astype(BF16)
        st_send[...] = states.astype(F32).reshape(frame_groups, group, model).astype(BF16)
        st_copies = exchange_frames(st_send, st_recv, 1)
        s_nl_copies = share_rows(s_nl_send, s_nl, s_low, 0)
        s_att_copies = share_columns(s_att_send, s_att, attended, 1)

    t_rows = frame_groups * group
    with jax.named_scope("a04_waitog"):
        arrive(og_copies)
    t_cot = og_recv[...].astype(F32).reshape(t_rows, model)
    t_cot_low = t_cot.astype(BF16)
    t_c_copies = share_rows(t_c_send, t_c, t_cot_low, 4)
    with jax.named_scope("a05_waitst"):
        arrive(st_copies)
    with jax.named_scope("a06_tempfwd"):
        normed, t_inverse = normalize(st_recv[...].astype(F32).reshape(t_rows, model))
        t_normed[...] = normed
        t_low = normed.astype(BF16)
        loads["te"].wait()
        shape = (HEADS * t_rows, t_rows)
        row_patch = lax.broadcasted_iota(jnp.int32, shape, 0) & (group - 1)
        column_patch = lax.broadcasted_iota(jnp.int32, shape, 1) & (group - 1)
        attended, t_saved = attend(t_low, te_ref, row_patch == column_patch, lambda: None)
        t_att_copies = share_columns(t_att_send, t_att, attended, 3)
        t_nl_copies = share_rows(t_nl_send, t_nl, t_low, 2)
    t_copies = {}

    def keep_temporal(i, value):
        t_copies[i] = share_columns(t_mg_send.at[i], t_mg.at[i], value, 5 + i)

    with jax.named_scope("a07_tempbwd"):
        loads["to"].wait()
        mixture_grad = backward_mixture(t_cot_low, to_ref, t_saved, keep_temporal)
        state_grads = backward_inputs(mixture_grad, te_ref, t_cot, t_normed[...], t_inverse)
        sg_send[...] = state_grads.reshape(frame_groups, group, model).astype(BF16)
        sg_copies = exchange_frames(sg_send, sg_recv, 2)

    owned = part.shape[3]

    def gradient(slot, left, right):
        def product_of(low, high):
            count = (high - low) * data_groups
            pieces = [ref[:, low:high] for ref in (left, right)]
            if (high - low) % 16:
                pieces = [p.astype(F32) for p in pieces]
            pieces = [p.reshape(count, p.shape[2]).astype(BF16) for p in pieces]
            return dot(pieces[0], pieces[1], 0, 0)

        product = product_of(0, patches)
        if left.shape[1] > patches:
            product = product + product_of(patches, left.shape[1])
        for f in range(frame_groups):
            place = sum((f >> s & 1) << (bits - 1 - s) for s in range(bits))
            for c in range(column_groups):
                start = (c * frame_groups + f) * owned
                part[slot, place, c] = product[start : start + owned].astype(BF16)

    def halves(step):
        half = frame_groups >> (step + 1)
        return half, side[step] * half, (1 - side[step]) * half

    def reduce_step(item, step):
        half, _, away = halves(step)
        slots = pl.ds(item["first"], item["count"])
        item["copy"] = push(
            sums[step].at[slots, pl.ds(away, half)],
            received[step].at[slots],
            r_send_sem.at[item["id"], step],
            r_recv_sem.at[item["id"], step],
            {"frame": across(1 << step)},
        )

    def advance(item):
        step = item["step"]
        item["step"] = step + 1
        slots = range(item["first"], item["first"] + item["count"])
        if step == 0:
            with jax.named_scope("g%d_wait" % item["id"]):
                arrive(item["needs"])
            with jax.named_scope("g%d_mm" % item["id"]):
                for slot in slots:
                    gradient(slot, *item["operands"](slot))
                reduce_step(item, 0)
        elif step <= bits:
            with jax.named_scope("g%d_r%d" % (item["id"], step)):
                item["copy"].wait_recv()
                half, kept, _ = halves(step - 1)
                for slot in slots:
                    total = sums[step - 1][slot, pl.ds(kept, half)].astype(F32) + received[
                        step - 1
                    ][slot].astype(F32)
                    if step == bits:
                        total = total * grad_factor
                    sums[step][slot] = total.astype(BF16)
                if step < bits:
                    reduce_step(item, step)
                else:
                    item["final"] = []
                    for slot in slots:
                        hand_columns(item, slot)
        elif step == bits + 1:
            with jax.named_scope("g%d_x" % item["id"]):
                arrive(item["final"])

    def target(slot, column):
        out, start = outputs[slot]
        return out.at[:, pl.ds(pl.multiple_of(start + column * block, block), block)]

    def hand_columns(item, slot):
        done = sums[bits]
        for k in range(1, column_groups):
            peer_column = lax.rem(column_at + k, column_groups)
            item["final"].append(
                push(
                    done.at[slot, 0, peer_column],
                    target(slot, column_at),
                    x_send_sem.at[slot, k],
                    x_recv_sem.at[slot, k],
                    {"dp": row_at * column_groups + peer_column},
                )
            )
        target(slot, column_at)[...] = done[slot, 0, column_at]

    outputs = [(temporalout_ref, 0)]
    outputs += [(temporalin_ref, i * width) for i in (2, 1, 0)]
    outputs += [(spatialout_ref, 0)]
    outputs += [(spatialin_ref, i * width) for i in (2, 1, 0)]

    def item(id, first, count, needs, operands):
        return {
            "id": id,
            "first": first,
            "count": count,
            "needs": needs,
            "operands": operands,
            "step": 0,
        }

    exits = item(0, 0, 1, t_c_copies + t_att_copies, lambda slot: (t_c, t_att))
    entries = item(
        1,
        1,
        3,
        t_nl_copies + t_copies[2] + t_copies[1] + t_copies[0],
        lambda slot: (t_nl, t_mg.at[3 - slot]),
    )
    cot_ref[patches:] = jnp.zeros((rows - patches, model), F32)
    loads["joined"].wait()
    cot_ref[patches : patches + bottles] = (
        (joined_ref[...].astype(F32) / frame_groups).astype(BF16).astype(F32)
    )
    advance(exits)
    with jax.named_scope("a08_waitsg"):
        arrive(sg_copies)
    cot_ref[:patches] = sg_recv[...].astype(F32).reshape(patches, model)
    s_cot_low = cot_ref[...].astype(BF16)
    s_c_copies = share_rows(s_c_send, s_c, s_cot_low, 8)
    s_copies = {}

    def keep_spatial(i, value):
        s_copies[i] = share_columns(s_mg_send.at[i], s_mg.at[i], value, 9 + i)

    with jax.named_scope("a09_spatbwd"):
        mixture_grad = backward_mixture(s_cot_low, so_ref, s_saved, keep_spatial)
        tokens_grad = backward_inputs(mixture_grad, se_ref, cot_ref[...], s_normed[...], s_inverse)
        frames_delta_ref[...] = tokens_grad[:patches].astype(BF16)
        bot_sum[0] = tokens_grad[patches : patches + bottles]

    stores = []

    def store(src, dst):
        copy = pltpu.make_async_copy(src, dst, out_sem.at[len(stores)])
        copy.start()
        stores.append(copy)

    store(frames_delta_ref, frames_delta_hbm)

    def bottle_send(step):
        return push(
            bot_sum.at[step],
            bot_recv.at[step],
            r_send_sem.at[6, step],
            r_recv_sem.at[6, step],
            {"frame": across(1 << step)},
        )

    bottle_copy = bottle_send(0)
    bottle_step = 0
    work = [exits, entries]
    work.append(item(2, 4, 1, s_c_copies + s_nl_copies + s_att_copies, lambda slot: (s_c, s_att)))
    for n, i in enumerate((2, 1, 0)):
        work.append(item(3 + n, 5 + n, 1, s_copies[i], lambda slot: (s_nl, s_mg.at[7 - slot])))
    started = 1
    while any(w["step"] < bits + 2 for w in work):
        if started < len(work):
            advance(work[started])
            started += 1
            active = work[: started - 1]
        else:
            active = work
        for w in active:
            if w["step"] < bits + 2:
                advance(w)
        if bottle_step < bits:
            bottle_copy.wait_recv()
            total = bot_sum[bottle_step] + bot_recv[bottle_step]
            bottle_step += 1
            if bottle_step < bits:
                bot_sum[bottle_step] = total
                bottle_copy = bottle_send(bottle_step)
            else:
                bottle_delta_ref[...] = total.astype(BF16)
                store(bottle_delta_ref, bottle_delta_hbm)
        if work[1]["step"] == bits + 2 and len(stores) == 2:
            store(temporalout_ref, temporalout_hbm)
            store(temporalin_ref, temporalin_hbm)
    with jax.named_scope("z1_store"):
        store(spatialout_ref, spatialout_hbm)
        store(spatialin_ref, spatialin_hbm)
        for copy in pending:
            copy.wait_send()
        for copy in stores:
            copy.wait()


def hand_over(*refs):
    count = len(refs) // 2
    for source, target in zip(refs[:count], refs[count:]):
        target[...] = source[...]


def per_device(
    frames_in,
    bottleneck,
    spatial_entry,
    spatial_exit,
    temporal_entry,
    temporal_exit,
    output_grad,
    joined_grad,
):
    clip_count, frames_local, patches, model = frames_in.shape
    bottles = bottleneck.shape[1]
    frame_groups = lax.axis_size("frame")
    data_groups = lax.axis_size("dp")
    assert clip_count == 1 and frames_local == 1
    entry_width = spatial_entry.shape[1]
    exit_width = spatial_exit.shape[1]
    group = patches // frame_groups
    assert group & (group - 1) == 0
    assert frame_groups & (frame_groups - 1) == 0 and data_groups & (data_groups - 1) == 0
    assert entry_width == 3 * exit_width
    bits = frame_groups.bit_length() - 1
    row_groups = 1 << ((data_groups.bit_length() - 1) // 2)
    column_groups = data_groups // row_groups
    rows = -(-(patches + bottles) // 16) * 16
    sent_rows = -(-(patches + bottles) // 8) * 8
    t_rows = patches
    wide = model // row_groups
    block = exit_width // column_groups
    owned = model // data_groups // frame_groups
    grad_factor = 1.0 / math.sqrt(patches * data_groups * frame_groups)

    def gather_set(count):
        return [
            pltpu.VMEM((row_groups, count, wide), BF16),
            pltpu.VMEM((data_groups, count, wide), BF16),
            pltpu.VMEM((column_groups, count, block), BF16),
            pltpu.VMEM((data_groups, count, block), BF16),
            pltpu.VMEM((row_groups, count, wide), BF16),
            pltpu.VMEM((data_groups, count, wide), BF16),
            pltpu.VMEM((3, column_groups, count, block), BF16),
            pltpu.VMEM((3, data_groups, count, block), BF16),
        ]

    moved = pltpu.VMEM((frame_groups, group, model), BF16)
    hbm = pl.BlockSpec(memory_space=pl.ANY)
    vmem = pl.BlockSpec(memory_space=pltpu.VMEM)
    out_shape = (
        jax.ShapeDtypeStruct((patches, model), BF16),
        jax.ShapeDtypeStruct((bottles, model), BF16),
        jax.ShapeDtypeStruct((owned, entry_width), BF16),
        jax.ShapeDtypeStruct((owned, exit_width), BF16),
        jax.ShapeDtypeStruct((owned, entry_width), BF16),
        jax.ShapeDtypeStruct((owned, exit_width), BF16),
    )
    outs = pl.pallas_call(
        functools.partial(kernel, frame_groups, row_groups, column_groups, grad_factor),
        out_shape=out_shape,
        in_specs=[hbm] * 8,
        out_specs=[hbm] * 6,
        scratch_shapes=[
            pltpu.VMEM((patches, model), BF16),
            pltpu.VMEM((bottles, model), BF16),
            moved,
            pltpu.VMEM((bottles, model), BF16),
            pltpu.VMEM(spatial_entry.shape, BF16),
            pltpu.VMEM(spatial_exit.shape, BF16),
            pltpu.VMEM(temporal_entry.shape, BF16),
            pltpu.VMEM(temporal_exit.shape, BF16),
            *[pltpu.VMEM(out.shape, BF16) for out in out_shape],
            pltpu.VMEM((rows, model), F32),
            pltpu.VMEM((rows, model), F32),
            pltpu.VMEM((rows, model), F32),
            pltpu.VMEM((t_rows, model), F32),
            moved,
            moved,
            moved,
            moved,
            moved,
            pltpu.VMEM((bits, bottles, model), F32),
            pltpu.VMEM((bits, bottles, model), F32),
            *gather_set(sent_rows),
            *gather_set(t_rows),
            pltpu.VMEM((8, frame_groups, column_groups, owned, block), BF16),
            *[
                pltpu.VMEM((8, frame_groups >> s, column_groups, owned, block), BF16)
                for s in range(1, bits + 1)
            ]
            * 2,
            pltpu.SemaphoreType.DMA((8,)),
            pltpu.SemaphoreType.DMA((6,)),
            pltpu.SemaphoreType.DMA((3, frame_groups)),
            pltpu.SemaphoreType.DMA((3, frame_groups)),
            pltpu.SemaphoreType.DMA((12, data_groups)),
            pltpu.SemaphoreType.DMA((12, data_groups)),
            pltpu.SemaphoreType.DMA((7, bits)),
            pltpu.SemaphoreType.DMA((7, bits)),
            pltpu.SemaphoreType.DMA((8, column_groups)),
            pltpu.SemaphoreType.DMA((8, column_groups)),
        ],
        compiler_params=pltpu.CompilerParams(
            collective_id=0, has_side_effects=True, vmem_limit_bytes=61 * 1024 * 1024
        ),
    )(
        frames_in.reshape(patches, model),
        bottleneck.reshape(bottles, model),
        output_grad.reshape(frame_groups, group, model),
        joined_grad.reshape(bottles, model),
        spatial_entry,
        spatial_exit,
        temporal_entry,
        temporal_exit,
    )
    outs = pl.pallas_call(
        hand_over,
        out_shape=[jax.ShapeDtypeStruct(out.shape, out.dtype) for out in outs],
        in_specs=[vmem] * len(outs),
        out_specs=[vmem] * len(outs),
        compiler_params=pltpu.CompilerParams(vmem_limit_bytes=61 * 1024 * 1024),
    )(*outs)
    return (outs[0].reshape(frames_in.shape), outs[1].reshape(bottleneck.shape), *outs[2:])


def solution(mesh):
    return jax.shard_map(
        per_device,
        mesh=mesh,
        in_specs=(
            P("dp", "frame", None, None),
            P("dp", None, None),
            P(),
            P(),
            P(),
            P(),
            P("dp", "frame", None, None),
            P("dp", None, None),
        ),
        out_specs=(
            P("dp", "frame", None, None),
            P("dp", None, None),
            P(("dp", "frame"), None),
            P(("dp", "frame"), None),
            P(("dp", "frame"), None),
            P(("dp", "frame"), None),
        ),
        check_vma=False,
    )
```

```python
import functools
import math

import jax
import jax.numpy as jnp
from jax import lax
from jax.experimental import pallas as pl
from jax.experimental.pallas import tpu as pltpu
from jax.sharding import PartitionSpec as P

HEADS = 8
EPSILON = 1e-05
MESH = pl.DeviceIdType.MESH
F32 = jnp.float32
BF16 = jnp.bfloat16


def dot(left, right, left_dim=1, right_dim=0):
    return lax.dot_general(
        left, right, (((left_dim,), (right_dim,)), ((), ())), preferred_element_type=F32
    )


def normalize(widened):
    centred = widened - jnp.mean(widened, axis=-1, keepdims=True)
    inverse = lax.rsqrt(jnp.mean(centred * centred, axis=-1, keepdims=True) + EPSILON)
    return centred * inverse, inverse


def head_masks(width, dtype):
    lanes = lax.broadcasted_iota(jnp.int32, (1, width), 1)
    size = width // HEADS
    return [
        jnp.where((lanes >= h * size) & (lanes < (h + 1) * size), 1.0, 0.0).astype(dtype)
        for h in range(HEADS)
    ]


def stack_heads(rows):
    return jnp.concatenate([rows * m for m in head_masks(rows.shape[1], rows.dtype)], axis=0)


def merge_heads(stacked):
    count = stacked.shape[0] // HEADS
    masks = head_masks(stacked.shape[1], stacked.dtype)
    total = stacked[:count] * masks[0]
    for h in range(1, HEADS):
        total = total + stacked[h * count : (h + 1) * count] * masks[h]
    return total


def attend(normed_low, entry_ref, mask):
    mixture = dot(normed_low, entry_ref[...]).astype(BF16)
    width = mixture.shape[1] // 3
    queries, key_rows, values = (mixture[:, i * width : (i + 1) * width] for i in range(3))
    factor = 1.0 / math.sqrt(width // HEADS)
    query_stack = stack_heads(queries)
    scores = dot(query_stack, key_rows, 1, 1) * factor
    scores = jnp.where(mask, scores, -1e30)
    scores = scores - jnp.max(scores, axis=-1, keepdims=True)
    expon = jnp.where(mask, jnp.exp(scores), 0.0)
    weights = expon / jnp.sum(expon, axis=-1, keepdims=True)
    weights_low = weights.astype(BF16)
    attended = merge_heads(dot(weights_low, values)).astype(BF16)
    return attended, (query_stack, key_rows, values, weights, weights_low)


def backward_mixture(cotangent, exit_ref, saved, emit):
    query_stack, key_rows, values, weights, weights_low = saved
    factor = 1.0 / math.sqrt(values.shape[1] // HEADS)
    attended_grad = dot(cotangent, exit_ref[...]).astype(BF16)
    grad_stack = stack_heads(attended_grad)
    values_grad = dot(weights_low, grad_stack, 0, 0).astype(BF16)
    emit(2, values_grad)
    softmax_grad = dot(grad_stack, values, 1, 1)
    centre = jnp.sum(weights * softmax_grad, axis=-1, keepdims=True)
    scores_grad = (weights * (softmax_grad - centre) * factor).astype(BF16)
    keys_grad = dot(scores_grad, query_stack, 0, 0).astype(BF16)
    emit(1, keys_grad)
    queries_grad = merge_heads(dot(scores_grad, key_rows)).astype(BF16)
    emit(0, queries_grad)
    return jnp.concatenate([queries_grad, keys_grad, values_grad], axis=1)


def backward_inputs(mixture_grad, entry_ref, cotangent, normed, inverse):
    normed_grad = dot(mixture_grad, entry_ref[...], 1, 1)
    inner = (
        normed_grad
        - jnp.mean(normed_grad, axis=-1, keepdims=True)
        - normed * jnp.mean(normed_grad * normed, axis=-1, keepdims=True)
    )
    return cotangent + inverse * inner


def kernel(
    frame_groups,
    row_groups,
    column_groups,
    grad_factor,
    frames_hbm,
    bottle_hbm,
    output_grad_hbm,
    joined_hbm,
    spatial_entry_hbm,
    spatial_exit_hbm,
    temporal_entry_hbm,
    temporal_exit_hbm,
    frames_delta_hbm,
    bottle_delta_hbm,
    spatialin_hbm,
    spatialout_hbm,
    temporalin_hbm,
    temporalout_hbm,
    frames_ref,
    bottle_ref,
    og_send,
    joined_ref,
    se_ref,
    so_ref,
    te_ref,
    to_ref,
    frames_delta_ref,
    bottle_delta_ref,
    spatialin_ref,
    spatialout_ref,
    temporalin_ref,
    temporalout_ref,
    tokens,
    cot_ref,
    s_normed,
    t_normed,
    og_recv,
    st_send,
    st_recv,
    sg_send,
    sg_recv,
    bot_sum,
    bot_recv,
    s_nl_send,
    s_nl,
    s_att_send,
    s_att,
    s_c_send,
    s_c,
    s_mg_send,
    s_mg,
    t_nl_send,
    t_nl,
    t_att_send,
    t_att,
    t_c_send,
    t_c,
    t_mg_send,
    t_mg,
    *tail,
):
    bits = frame_groups.bit_length() - 1
    part = tail[0]
    received = tail[1 : 1 + bits]
    sums = (part,) + tuple(tail[1 + bits : 1 + 2 * bits])
    (
        load_sem,
        out_sem,
        f_sem,
        d_sem,
        r_sem,
        rs_sem,
        x_sem,
        b_sem,
    ) = tail[1 + 2 * bits :]
    frame = lax.axis_index("frame")
    data = lax.axis_index("dp")
    row_at = data // column_groups
    column_at = lax.rem(data, column_groups)
    data_groups = row_groups * column_groups
    patches, model = frames_ref.shape
    bottles = bottle_ref.shape[0]
    rows = tokens.shape[0]
    group = og_send.shape[1]
    width = to_ref.shape[1]
    block = width // column_groups
    owned = part.shape[3]
    side = [lax.rem(frame // (1 << s), 2) for s in range(bits)]

    loads = {}

    def load(name, src, dst):
        loads[name] = pltpu.make_async_copy(src, dst, load_sem.at[len(loads)])
        loads[name].start()

    load("frames", frames_hbm, frames_ref)
    load("bottle", bottle_hbm, bottle_ref)
    load("se", spatial_entry_hbm, se_ref)
    load("so", spatial_exit_hbm, so_ref)

    barrier = pltpu.get_barrier_semaphore()
    for k in range(1, frame_groups):
        pl.semaphore_signal(
            barrier,
            inc=1,
            device_id={"frame": lax.rem(frame + k, frame_groups)},
            device_id_type=MESH,
        )
    for k in range(1, data_groups):
        pl.semaphore_signal(
            barrier, inc=1, device_id={"dp": lax.rem(data + k, data_groups)}, device_id_type=MESH
        )

    sent = []

    def push(src, dst, send_sem, recv_sem, device):
        copy = pltpu.make_async_remote_copy(
            src_ref=src,
            dst_ref=dst,
            send_sem=send_sem,
            recv_sem=recv_sem,
            device_id=device,
            device_id_type=MESH,
        )
        copy.start()
        return copy

    def drain(view, sem):
        pltpu.make_async_copy(view, view, sem).wait()

    def across(k):
        peer = frame
        for s in range(bits):
            if k >> s & 1:
                peer = peer + (1 << s) * (1 - 2 * side[s])
        return peer

    def exchange_frames(send, dst, phase):
        for k in reversed(range(1, frame_groups)):
            peer = across(k)
            push(
                send.at[peer],
                dst.at[frame],
                f_sem.at[0, phase],
                f_sem.at[1, phase],
                {"frame": peer},
            )
        dst[frame] = send[frame]
        sent.append((dst.at[pl.ds(0, frame_groups - 1)], f_sem.at[0, phase]))

    def arrive_frames(dst, phase):
        drain(dst.at[pl.ds(0, frame_groups - 1)], f_sem.at[1, phase])

    def clip(row, column):
        return row * column_groups + column

    def row_peers():
        return [lax.rem(row_at + k, row_groups) for k in range(1, row_groups)]

    def column_peers():
        return [lax.rem(column_at + k, column_groups) for k in range(1, column_groups)]

    def put_blocks(dst, value):
        count, kept, size = dst.shape
        for i in range(count):
            dst[i] = value[:kept, i * size : (i + 1) * size]

    def share(send, dst, value, by_row, phase):
        put_blocks(send, value)
        mine = row_at if by_row else column_at
        for peer_row in row_peers():
            push(
                send.at[peer_row if by_row else column_at],
                dst.at[data],
                d_sem.at[0, phase],
                d_sem.at[1 if by_row else 2, phase],
                {"dp": clip(peer_row, column_at)},
            )
        for peer_column in column_peers():
            push(
                send.at[row_at if by_row else peer_column],
                dst.at[data],
                d_sem.at[0, phase],
                d_sem.at[2 if by_row else 1, phase],
                {"dp": clip(row_at, peer_column)},
            )
        dst[data] = send[mine]
        sent.append((dst.at[pl.ds(0, data_groups - 1)], d_sem.at[0, phase]))
        return dst, by_row, phase

    def relay(shared):
        dst, by_row, phase = shared
        first = (row_groups if by_row else column_groups) - 1
        drain(dst.at[pl.ds(0, first)], d_sem.at[1, phase])
        for peer_row in row_peers():
            for peer_column in column_peers():
                source = clip(peer_row, column_at) if by_row else clip(row_at, peer_column)
                target = clip(row_at, peer_column) if by_row else clip(peer_row, column_at)
                push(
                    dst.at[source],
                    dst.at[source],
                    d_sem.at[0, phase],
                    d_sem.at[2, phase],
                    {"dp": target},
                )

    def finish(shared):
        dst, by_row, phase = shared
        first = (row_groups if by_row else column_groups) - 1
        drain(dst.at[pl.ds(0, data_groups - 1 - first)], d_sem.at[2, phase])

    def share_direct(send, dst, value, by_row, phase):
        put_blocks(send, value)
        for k in reversed(range(1, data_groups)):
            peer_row = lax.rem(row_at + k // column_groups, row_groups)
            peer_column = lax.rem(column_at + k % column_groups, column_groups)
            push(
                send.at[peer_row if by_row else peer_column],
                dst.at[data],
                d_sem.at[0, phase],
                d_sem.at[1, phase],
                {"dp": clip(peer_row, peer_column)},
            )
        dst[data] = send[row_at if by_row else column_at]
        sent.append((dst.at[pl.ds(0, data_groups - 1)], d_sem.at[0, phase]))
        return dst, by_row, phase

    def finish_direct(shared):
        dst, _, phase = shared
        drain(dst.at[pl.ds(0, data_groups - 1)], d_sem.at[1, phase])

    def gradient(slot, left, right):
        def product_of(low, high):
            count = (high - low) * data_groups
            pieces = [ref[:, low:high] for ref in (left, right)]
            if (high - low) % 16:
                pieces = [p.astype(F32) for p in pieces]
            pieces = [p.reshape(count, p.shape[2]).astype(BF16) for p in pieces]
            return dot(pieces[0], pieces[1], 0, 0)

        product = product_of(0, patches)
        if left.shape[1] > patches:
            product = product + product_of(patches, left.shape[1])
        for f in range(frame_groups):
            place = sum((f >> s & 1) << (bits - 1 - s) for s in range(bits))
            for c in range(column_groups):
                start = (c * frame_groups + f) * owned
                part[slot, place, c] = product[start : start + owned].astype(BF16)

    def send_half(item, step):
        first, count, index = item
        half = frame_groups >> (step + 1)
        slots = pl.ds(first, count)
        push(
            sums[step].at[slots, pl.ds((1 - side[step]) * half, half)],
            received[step].at[slots],
            rs_sem.at[index],
            r_sem.at[index, step],
            {"frame": across(1 << step)},
        )

    def halve(item, step):
        first, count, index = item
        half = frame_groups >> (step + 1)
        drain(received[step].at[pl.ds(first, count)], r_sem.at[index, step])
        for slot in range(first, first + count):
            kept = sums[step][slot, pl.ds(side[step] * half, half)].astype(F32)
            total = kept + received[step][slot].astype(F32)
            if step == bits - 1:
                total = total * grad_factor
            sums[step + 1][slot] = total.astype(BF16)
        if step < bits - 1:
            send_half(item, step + 1)
            return
        sent.append((part.at[pl.ds(first, count), pl.ds(0, frame_groups - 1)], rs_sem.at[index]))
        done = sums[bits]
        for slot in range(first, first + count):
            for peer_column in column_peers():
                push(
                    done.at[slot, 0, peer_column],
                    result(slot, column_at),
                    x_sem.at[0, slot],
                    x_sem.at[1, slot],
                    {"dp": clip(row_at, peer_column)},
                )
            result(slot, column_at)[...] = done[slot, 0, column_at]
            others = done.at[slot, 0, pl.ds(0, column_groups - 1)]
            sent.append((others, x_sem.at[0, slot]))

    def settle(item):
        first, count, _ = item
        for slot in range(first, first + count):
            drain(sums[bits].at[slot, 0, pl.ds(0, column_groups - 1)], x_sem.at[1, slot])

    outputs = [(temporalout_ref, 0)]
    outputs += [(temporalin_ref, i * width) for i in (2, 1, 0)]
    outputs += [(spatialout_ref, 0)]
    outputs += [(spatialin_ref, i * width) for i in (2, 1, 0)]

    def result(slot, column):
        out, start = outputs[slot]
        return out.at[:, pl.ds(pl.multiple_of(start + column * block, block), block)]

    with jax.named_scope("a01_norm"):
        loads["frames"].wait()
        loads["bottle"].wait()
        tokens[:patches] = frames_ref[...].astype(F32)
        tokens[patches:] = jnp.zeros((rows - patches, model), F32)
        tokens[patches : patches + bottles] = bottle_ref[...].astype(F32)
        normed, s_inverse = normalize(tokens[...])
        s_normed[...] = normed
        s_low = normed.astype(BF16)
        loads["se"].wait()
        load("og", output_grad_hbm, og_send)
        load("te", temporal_entry_hbm, te_ref)
        load("to", temporal_exit_hbm, to_ref)
        load("joined", joined_hbm, joined_ref)
    columns = lax.broadcasted_iota(jnp.int32, (HEADS * rows, rows), 1)
    attended, s_saved = attend(s_low, se_ref, columns < patches + bottles)
    with jax.named_scope("a02_states"):
        loads["so"].wait()
        states = (tokens[:patches] + dot(attended[:patches], so_ref[...], 1, 1)).astype(BF16)
        st_send[...] = states.astype(F32).reshape(frame_groups, group, model).astype(BF16)
    with jax.named_scope("a03_enter"):
        pl.semaphore_wait(barrier, frame_groups + data_groups - 2)
        exchange_frames(st_send, st_recv, 0)
        loads["og"].wait()
        exchange_frames(og_send, og_recv, 1)
        s_nl_shared = share(s_nl_send, s_nl, s_low, True, 0)
        s_att_shared = share(s_att_send, s_att, attended, False, 1)

    t_rows = frame_groups * group
    with jax.named_scope("a05_waitst"):
        arrive_frames(st_recv, 0)
    with jax.named_scope("a06_tempfwd"):
        normed, t_inverse = normalize(st_recv[...].astype(F32).reshape(t_rows, model))
        t_normed[...] = normed
        t_low = normed.astype(BF16)
        relay(s_nl_shared)
        relay(s_att_shared)
        t_nl_shared = share(t_nl_send, t_nl, t_low, True, 2)
        loads["te"].wait()
        shape = (HEADS * t_rows, t_rows)
        row_patch = lax.broadcasted_iota(jnp.int32, shape, 0) & (group - 1)
        column_patch = lax.broadcasted_iota(jnp.int32, shape, 1) & (group - 1)
        attended, t_saved = attend(t_low, te_ref, row_patch == column_patch)
        t_att_shared = share(t_att_send, t_att, attended, False, 3)
    with jax.named_scope("a06_waitog"):
        arrive_frames(og_recv, 1)
    t_cot = og_recv[...].astype(F32).reshape(t_rows, model)
    t_cot_low = t_cot.astype(BF16)
    t_c_shared = share(t_c_send, t_c, t_cot_low, True, 4)
    t_shared = {}

    def keep_temporal(i, value):
        t_shared[i] = share(t_mg_send.at[i], t_mg.at[i], value, False, 5 + i)

    with jax.named_scope("a07_tempbwd"):
        loads["to"].wait()
        mixture_grad = backward_mixture(t_cot_low, to_ref, t_saved, keep_temporal)
        state_grads = backward_inputs(mixture_grad, te_ref, t_cot, t_normed[...], t_inverse)
        sg_send[...] = state_grads.reshape(frame_groups, group, model).astype(BF16)
        exchange_frames(sg_send, sg_recv, 2)

    with jax.named_scope("a08_relays"):
        relay(t_nl_shared)
        relay(t_att_shared)
        relay(t_c_shared)
        cot_ref[patches:] = jnp.zeros((rows - patches, model), F32)
        loads["joined"].wait()
        cot_ref[patches : patches + bottles] = (
            (joined_ref[...].astype(F32) / frame_groups).astype(BF16).astype(F32)
        )
        for i in (2, 1, 0):
            relay(t_shared[i])
    temporal_exit_item, temporal_item = (0, 1, 0), (1, 3, 1)
    with jax.named_scope("a09_waitsg"):
        arrive_frames(sg_recv, 2)
    cot_ref[:patches] = sg_recv[...].astype(F32).reshape(patches, model)
    s_cot_low = cot_ref[...].astype(BF16)
    s_c_shared = share_direct(s_c_send, s_c, s_cot_low, True, 8)
    s_shared = {}

    def keep_spatial(i, value):
        s_shared[i] = share_direct(s_mg_send.at[i], s_mg.at[i], value, False, 9 + i)
        if i == 2:
            with jax.named_scope("b1_w"):
                finish(t_att_shared)
                finish(t_c_shared)
            with jax.named_scope("b1_exit"):
                gradient(0, t_c, t_att)
                send_half(temporal_exit_item, 0)
        if i == 1:
            halve(temporal_exit_item, 0)
        if i == 0:
            with jax.named_scope("b2_w"):
                finish(t_nl_shared)
                for n in (2, 1, 0):
                    finish(t_shared[n])
            with jax.named_scope("b2_entry"):
                for slot in (1, 2, 3):
                    gradient(slot, t_nl, t_mg.at[3 - slot])
                send_half(temporal_item, 0)

    with jax.named_scope("b0_spatbwd"):
        mixture_grad = backward_mixture(s_cot_low, so_ref, s_saved, keep_spatial)
        halve(temporal_item, 0)
        tokens_grad = backward_inputs(mixture_grad, se_ref, cot_ref[...], s_normed[...], s_inverse)
        frames_delta_ref[...] = tokens_grad[:patches].astype(BF16)
        bot_sum[0] = tokens_grad[patches : patches + bottles]

    stores = []

    def store(src, dst):
        copy = pltpu.make_async_copy(src, dst, out_sem.at[len(stores)])
        copy.start()
        stores.append(copy)

    store(frames_delta_ref, frames_delta_hbm)

    bottle_copies = []

    def send_bottles(step):
        bottle_copies.append(
            push(
                bot_sum.at[step],
                bot_recv.at[step],
                b_sem.at[0, step],
                b_sem.at[1, step],
                {"frame": across(1 << step)},
            )
        )

    def add_bottles(step):
        bottle_copies[step].wait_recv()
        total = bot_sum[step] + bot_recv[step]
        if step < bits - 1:
            bot_sum[step + 1] = total
            send_bottles(step + 1)
        else:
            bottle_delta_ref[...] = total.astype(BF16)
            store(bottle_delta_ref, bottle_delta_hbm)

    send_bottles(0)
    spatial_a, spatial_b, spatial_c = (4, 2, 2), (6, 1, 3), (7, 1, 4)
    finish(s_nl_shared)
    finish(s_att_shared)
    with jax.named_scope("c1_w"):
        finish_direct(s_c_shared)
        finish_direct(s_shared[2])
    with jax.named_scope("c1_mm"):
        gradient(4, s_c, s_att)
        gradient(5, s_nl, s_mg.at[2])
        send_half(spatial_a, 0)
    with jax.named_scope("c3_w"):
        finish_direct(s_shared[1])
    with jax.named_scope("c3_mm"):
        gradient(6, s_nl, s_mg.at[1])
        send_half(spatial_b, 0)
        halve(spatial_a, 0)
    with jax.named_scope("c4_w"):
        finish_direct(s_shared[0])
    with jax.named_scope("c4_mm"):
        gradient(7, s_nl, s_mg.at[0])
        send_half(spatial_c, 0)
        halve(spatial_b, 0)
    with jax.named_scope("c5_halve"):
        halve(temporal_exit_item, 1)
        halve(spatial_c, 0)
    for step in range(1, bits + 1):
        with jax.named_scope("d%d_t" % step):
            if step > 1 and step < bits:
                halve(temporal_exit_item, step)
            if step < bits:
                halve(temporal_item, step)
        if step < bits:
            with jax.named_scope("d%d_a" % step):
                add_bottles(step - 1)
                halve(spatial_a, step)
            with jax.named_scope("d%d_b" % step):
                halve(spatial_b, step)
            with jax.named_scope("d%d_c" % step):
                halve(spatial_c, step)
    add_bottles(bits - 1)
    with jax.named_scope("e1_settle"):
        settle(temporal_exit_item)
        store(temporalout_ref, temporalout_hbm)
        settle(temporal_item)
        store(temporalin_ref, temporalin_hbm)
        settle(spatial_a)
        store(spatialout_ref, spatialout_hbm)
        settle(spatial_b)
        settle(spatial_c)
        store(spatialin_ref, spatialin_hbm)
    with jax.named_scope("e2_drain"):
        for view, sem in sent:
            drain(view, sem)
        for copy in bottle_copies:
            copy.wait_send()
        for copy in stores:
            copy.wait()


def hand_over(*refs):
    count = len(refs) // 2
    for source, target in zip(refs[:count], refs[count:]):
        target[...] = source[...]


def per_device(
    frames_in,
    bottleneck,
    spatial_entry,
    spatial_exit,
    temporal_entry,
    temporal_exit,
    output_grad,
    joined_grad,
):
    clip_count, frames_local, patches, model = frames_in.shape
    bottles = bottleneck.shape[1]
    frame_groups = lax.axis_size("frame")
    data_groups = lax.axis_size("dp")
    assert clip_count == 1 and frames_local == 1
    entry_width = spatial_entry.shape[1]
    exit_width = spatial_exit.shape[1]
    group = patches // frame_groups
    assert group & (group - 1) == 0
    assert frame_groups & (frame_groups - 1) == 0 and data_groups & (data_groups - 1) == 0
    assert entry_width == 3 * exit_width
    bits = frame_groups.bit_length() - 1
    row_groups = 1 << ((data_groups.bit_length() - 1) // 2)
    column_groups = data_groups // row_groups
    rows = -(-(patches + bottles) // 16) * 16
    sent_rows = -(-(patches + bottles) // 8) * 8
    t_rows = patches
    wide = model // row_groups
    block = exit_width // column_groups
    owned = model // data_groups // frame_groups
    grad_factor = 1.0 / math.sqrt(patches * data_groups * frame_groups)

    def gather_set(count):
        return [
            pltpu.VMEM((row_groups, count, wide), BF16),
            pltpu.VMEM((data_groups, count, wide), BF16),
            pltpu.VMEM((column_groups, count, block), BF16),
            pltpu.VMEM((data_groups, count, block), BF16),
            pltpu.VMEM((row_groups, count, wide), BF16),
            pltpu.VMEM((data_groups, count, wide), BF16),
            pltpu.VMEM((3, column_groups, count, block), BF16),
            pltpu.VMEM((3, data_groups, count, block), BF16),
        ]

    moved = pltpu.VMEM((frame_groups, group, model), BF16)
    hbm = pl.BlockSpec(memory_space=pl.ANY)
    vmem = pl.BlockSpec(memory_space=pltpu.VMEM)
    out_shape = (
        jax.ShapeDtypeStruct((patches, model), BF16),
        jax.ShapeDtypeStruct((bottles, model), BF16),
        jax.ShapeDtypeStruct((owned, entry_width), BF16),
        jax.ShapeDtypeStruct((owned, exit_width), BF16),
        jax.ShapeDtypeStruct((owned, entry_width), BF16),
        jax.ShapeDtypeStruct((owned, exit_width), BF16),
    )
    outs = pl.pallas_call(
        functools.partial(kernel, frame_groups, row_groups, column_groups, grad_factor),
        out_shape=out_shape,
        in_specs=[hbm] * 8,
        out_specs=[hbm] * 6,
        scratch_shapes=[
            pltpu.VMEM((patches, model), BF16),
            pltpu.VMEM((bottles, model), BF16),
            moved,
            pltpu.VMEM((bottles, model), BF16),
            pltpu.VMEM(spatial_entry.shape, BF16),
            pltpu.VMEM(spatial_exit.shape, BF16),
            pltpu.VMEM(temporal_entry.shape, BF16),
            pltpu.VMEM(temporal_exit.shape, BF16),
            *[pltpu.VMEM(out.shape, BF16) for out in out_shape],
            pltpu.VMEM((rows, model), F32),
            pltpu.VMEM((rows, model), F32),
            pltpu.VMEM((rows, model), F32),
            pltpu.VMEM((t_rows, model), F32),
            moved,
            moved,
            moved,
            moved,
            moved,
            pltpu.VMEM((bits, bottles, model), F32),
            pltpu.VMEM((bits, bottles, model), F32),
            *gather_set(sent_rows),
            *gather_set(t_rows),
            pltpu.VMEM((8, frame_groups, column_groups, owned, block), BF16),
            *[
                pltpu.VMEM((8, frame_groups >> s, column_groups, owned, block), BF16)
                for s in range(1, bits + 1)
            ]
            * 2,
            pltpu.SemaphoreType.DMA((8,)),
            pltpu.SemaphoreType.DMA((6,)),
            pltpu.SemaphoreType.DMA((2, 3)),
            pltpu.SemaphoreType.DMA((3, 12)),
            pltpu.SemaphoreType.DMA((5, bits)),
            pltpu.SemaphoreType.DMA((5,)),
            pltpu.SemaphoreType.DMA((2, 8)),
            pltpu.SemaphoreType.DMA((2, bits)),
        ],
        compiler_params=pltpu.CompilerParams(
            collective_id=0, has_side_effects=True, vmem_limit_bytes=61 * 1024 * 1024
        ),
    )(
        frames_in.reshape(patches, model),
        bottleneck.reshape(bottles, model),
        output_grad.reshape(frame_groups, group, model),
        joined_grad.reshape(bottles, model),
        spatial_entry,
        spatial_exit,
        temporal_entry,
        temporal_exit,
    )
    outs = pl.pallas_call(
        hand_over,
        out_shape=[jax.ShapeDtypeStruct(out.shape, out.dtype) for out in outs],
        in_specs=[vmem] * len(outs),
        out_specs=[vmem] * len(outs),
        compiler_params=pltpu.CompilerParams(vmem_limit_bytes=61 * 1024 * 1024),
    )(*outs)
    return (outs[0].reshape(frames_in.shape), outs[1].reshape(bottleneck.shape), *outs[2:])


def solution(mesh):
    return jax.shard_map(
        per_device,
        mesh=mesh,
        in_specs=(
            P("dp", "frame", None, None),
            P("dp", None, None),
            P(),
            P(),
            P(),
            P(),
            P("dp", "frame", None, None),
            P("dp", None, None),
        ),
        out_specs=(
            P("dp", "frame", None, None),
            P("dp", None, None),
            P(("dp", "frame"), None),
            P(("dp", "frame"), None),
            P(("dp", "frame"), None),
            P(("dp", "frame"), None),
        ),
        check_vma=False,
    )
```

```python
import functools
import math

import jax
import jax.numpy as jnp
from jax import lax
from jax.experimental import pallas as pl
from jax.experimental.pallas import tpu as pltpu
from jax.sharding import PartitionSpec as P

HEADS = 8
EPSILON = 1e-05
MESH = pl.DeviceIdType.MESH
F32 = jnp.float32
BF16 = jnp.bfloat16


def dot(left, right, left_dim=1, right_dim=0):
    return lax.dot_general(
        left, right, (((left_dim,), (right_dim,)), ((), ())), preferred_element_type=F32
    )


def normalize(widened):
    centred = widened - jnp.mean(widened, axis=-1, keepdims=True)
    inverse = lax.rsqrt(jnp.mean(centred * centred, axis=-1, keepdims=True) + EPSILON)
    return centred * inverse, inverse


def head_masks(width, dtype):
    lanes = lax.broadcasted_iota(jnp.int32, (1, width), 1)
    size = width // HEADS
    return [
        jnp.where((lanes >= h * size) & (lanes < (h + 1) * size), 1.0, 0.0).astype(dtype)
        for h in range(HEADS)
    ]


def stack_heads(rows):
    return jnp.concatenate([rows * m for m in head_masks(rows.shape[1], rows.dtype)], axis=0)


def merge_heads(stacked):
    count = stacked.shape[0] // HEADS
    masks = head_masks(stacked.shape[1], stacked.dtype)
    total = stacked[:count] * masks[0]
    for h in range(1, HEADS):
        total = total + stacked[h * count : (h + 1) * count] * masks[h]
    return total


def attend(normed_low, entry_ref, mask, ready=lambda i: None):
    width = entry_ref.shape[1] // 3
    parts = []
    for i in range(3):
        ready(i)
        parts.append(dot(normed_low, entry_ref[:, i * width : (i + 1) * width]).astype(BF16))
    queries, key_rows, values = parts
    factor = 1.0 / math.sqrt(width // HEADS)
    query_stack = stack_heads(queries)
    scores = dot(query_stack, key_rows, 1, 1) * factor
    scores = jnp.where(mask, scores, -1e30)
    scores = scores - jnp.max(scores, axis=-1, keepdims=True)
    expon = jnp.where(mask, jnp.exp(scores), 0.0)
    weights = expon / jnp.sum(expon, axis=-1, keepdims=True)
    weights_low = weights.astype(BF16)
    attended = merge_heads(dot(weights_low, values)).astype(BF16)
    return attended, (query_stack, key_rows, values, weights, weights_low)


def backward_mixture(cotangent, exit_ref, saved, emit):
    query_stack, key_rows, values, weights, weights_low = saved
    factor = 1.0 / math.sqrt(values.shape[1] // HEADS)
    attended_grad = dot(cotangent, exit_ref[...]).astype(BF16)
    grad_stack = stack_heads(attended_grad)
    values_grad = dot(weights_low, grad_stack, 0, 0).astype(BF16)
    emit(2, values_grad)
    softmax_grad = dot(grad_stack, values, 1, 1)
    centre = jnp.sum(weights * softmax_grad, axis=-1, keepdims=True)
    scores_grad = (weights * (softmax_grad - centre) * factor).astype(BF16)
    keys_grad = dot(scores_grad, query_stack, 0, 0).astype(BF16)
    emit(1, keys_grad)
    queries_grad = merge_heads(dot(scores_grad, key_rows)).astype(BF16)
    emit(0, queries_grad)
    return jnp.concatenate([queries_grad, keys_grad, values_grad], axis=1)


def backward_inputs(mixture_grad, turned_ref, cotangent, normed, inverse):
    normed_grad = dot(mixture_grad, turned_ref[...])
    inner = (
        normed_grad
        - jnp.mean(normed_grad, axis=-1, keepdims=True)
        - normed * jnp.mean(normed_grad * normed, axis=-1, keepdims=True)
    )
    return cotangent + inverse * inner


def kernel(
    frame_groups,
    row_groups,
    column_groups,
    grad_factor,
    frames_hbm,
    bottle_hbm,
    output_grad_hbm,
    joined_hbm,
    spatial_entry_hbm,
    spatial_exit_hbm,
    temporal_entry_hbm,
    temporal_exit_hbm,
    frames_delta_hbm,
    bottle_delta_hbm,
    spatialin_hbm,
    spatialout_hbm,
    temporalin_hbm,
    temporalout_hbm,
    frames_ref,
    bottle_ref,
    og_send,
    joined_ref,
    se_ref,
    so_ref,
    te_ref,
    to_ref,
    turned_se,
    turned_te,
    frames_delta_ref,
    bottle_delta_ref,
    spatialin_ref,
    spatialout_ref,
    temporalin_ref,
    temporalout_ref,
    tokens,
    cot_ref,
    s_normed,
    t_normed,
    og_recv,
    st_send,
    st_recv,
    sg_send,
    sg_recv,
    bot_sum,
    bot_recv,
    s_nl_send,
    s_nl,
    s_att_send,
    s_att,
    s_c_send,
    s_c,
    s_mg_send,
    s_mg,
    t_nl_send,
    t_nl,
    t_att_send,
    t_att,
    t_c_send,
    t_c,
    t_mg_send,
    t_mg,
    *tail,
):
    bits = frame_groups.bit_length() - 1
    part, final = tail[:2]
    received = tail[2 : 1 + bits]
    sums = (part,) + tuple(tail[1 + bits : 2 * bits])
    (
        load_sem,
        out_sem,
        f_sem,
        d_sem,
        r_sem,
        rs_sem,
        x_sem,
        b_sem,
    ) = tail[2 * bits :]
    frame = lax.axis_index("frame")
    data = lax.axis_index("dp")
    row_at = data // column_groups
    column_at = lax.rem(data, column_groups)
    data_groups = row_groups * column_groups
    patches, model = frames_ref.shape
    bottles = bottle_ref.shape[0]
    rows = tokens.shape[0]
    group = og_send.shape[1]
    width = to_ref.shape[1]
    block = width // column_groups
    owned = part.shape[3]
    side = [lax.rem(frame // (1 << s), 2) for s in range(bits)]

    loads = {}

    def load(name, src, dst):
        loads[name] = pltpu.make_async_copy(src, dst, load_sem.at[len(loads)])
        loads[name].start()

    load("frames", frames_hbm, frames_ref)
    load("bottle", bottle_hbm, bottle_ref)
    parts = [pl.ds(i * width, width) for i in range(3)]
    for i in range(3):
        load(i, spatial_entry_hbm.at[:, parts[i]], se_ref.at[:, parts[i]])

    barrier = pltpu.get_barrier_semaphore()
    for k in range(1, frame_groups):
        pl.semaphore_signal(
            barrier,
            inc=1,
            device_id={"frame": lax.rem(frame + k, frame_groups)},
            device_id_type=MESH,
        )
    for k in range(1, data_groups):
        pl.semaphore_signal(
            barrier, inc=1, device_id={"dp": lax.rem(data + k, data_groups)}, device_id_type=MESH
        )

    sent = []

    def push(src, dst, send_sem, recv_sem, device):
        copy = pltpu.make_async_remote_copy(
            src_ref=src,
            dst_ref=dst,
            send_sem=send_sem,
            recv_sem=recv_sem,
            device_id=device,
            device_id_type=MESH,
        )
        copy.start()
        return copy

    def drain(view, sem):
        pltpu.make_async_copy(view, view, sem).wait()

    def across(k):
        peer = frame
        for s in range(bits):
            if k >> s & 1:
                peer = peer + (1 << s) * (1 - 2 * side[s])
        return peer

    def exchange_frames(send, dst, phase):
        for k in reversed(range(1, frame_groups)):
            peer = across(k)
            push(
                send.at[peer],
                dst.at[frame],
                f_sem.at[0, phase],
                f_sem.at[1, phase],
                {"frame": peer},
            )
        dst[frame] = send[frame]
        sent.append((dst.at[pl.ds(0, frame_groups - 1)], f_sem.at[0, phase]))

    def arrive_frames(dst, phase):
        drain(dst.at[pl.ds(0, frame_groups - 1)], f_sem.at[1, phase])

    def clip(row, column):
        return row * column_groups + column

    def row_peers():
        return [lax.rem(row_at + k, row_groups) for k in range(1, row_groups)]

    def column_peers():
        return [lax.rem(column_at + k, column_groups) for k in range(1, column_groups)]

    def put_blocks(dst, value):
        count, kept, size = dst.shape
        for i in range(count):
            dst[i] = value[:kept, i * size : (i + 1) * size]

    def share(send, dst, value, by_row, phase):
        put_blocks(send, value)
        mine = row_at if by_row else column_at
        for peer_row in row_peers():
            push(
                send.at[peer_row if by_row else column_at],
                dst.at[data],
                d_sem.at[0, phase],
                d_sem.at[1 if by_row else 2, phase],
                {"dp": clip(peer_row, column_at)},
            )
        for peer_column in column_peers():
            push(
                send.at[row_at if by_row else peer_column],
                dst.at[data],
                d_sem.at[0, phase],
                d_sem.at[2 if by_row else 1, phase],
                {"dp": clip(row_at, peer_column)},
            )
        dst[data] = send[mine]
        sent.append((dst.at[pl.ds(0, data_groups - 1)], d_sem.at[0, phase]))
        return dst, by_row, phase

    def relay(shared):
        dst, by_row, phase = shared
        first = (row_groups if by_row else column_groups) - 1
        drain(dst.at[pl.ds(0, first)], d_sem.at[1, phase])
        for peer_row in row_peers():
            for peer_column in column_peers():
                source = clip(peer_row, column_at) if by_row else clip(row_at, peer_column)
                target = clip(row_at, peer_column) if by_row else clip(peer_row, column_at)
                push(
                    dst.at[source],
                    dst.at[source],
                    d_sem.at[0, phase],
                    d_sem.at[2, phase],
                    {"dp": target},
                )

    def finish(shared):
        dst, by_row, phase = shared
        first = (row_groups if by_row else column_groups) - 1
        drain(dst.at[pl.ds(0, data_groups - 1 - first)], d_sem.at[2, phase])

    def share_direct(send, dst, value, by_row, phase):
        put_blocks(send, value)
        for k in reversed(range(1, data_groups)):
            peer_row = lax.rem(row_at + k // column_groups, row_groups)
            peer_column = lax.rem(column_at + k % column_groups, column_groups)
            push(
                send.at[peer_row if by_row else peer_column],
                dst.at[data],
                d_sem.at[0, phase],
                d_sem.at[1, phase],
                {"dp": clip(peer_row, peer_column)},
            )
        dst[data] = send[row_at if by_row else column_at]
        sent.append((dst.at[pl.ds(0, data_groups - 1)], d_sem.at[0, phase]))
        return dst, by_row, phase

    def finish_direct(shared):
        dst, _, phase = shared
        drain(dst.at[pl.ds(0, data_groups - 1)], d_sem.at[1, phase])

    def gradient(slot, left, right):
        def product_of(low, high):
            count = (high - low) * data_groups
            pieces = [ref[:, low:high] for ref in (left, right)]
            if (high - low) % 16:
                pieces = [p.astype(F32) for p in pieces]
            pieces = [p.reshape(count, p.shape[2]).astype(BF16) for p in pieces]
            return dot(pieces[0], pieces[1], 0, 0)

        product = product_of(0, patches)
        if left.shape[1] > patches:
            product = product + product_of(patches, left.shape[1])
        for f in range(frame_groups):
            place = sum((f >> s & 1) << (bits - 1 - s) for s in range(bits))
            for c in range(column_groups):
                start = (c * frame_groups + f) * owned
                part[slot, place, c] = product[start : start + owned].astype(BF16)

    def send_half(item, step):
        first, count, index = item
        half = frame_groups >> (step + 1)
        slots = pl.ds(first, count)
        push(
            sums[step].at[slots, pl.ds((1 - side[step]) * half, half)],
            received[step].at[slots],
            rs_sem.at[index],
            r_sem.at[index, step],
            {"frame": across(1 << step)},
        )

    def send_owners(item):
        first, count, index = item
        step = bits - 1
        slots = pl.ds(first, count)
        for k in reversed(range(column_groups)):
            owner = lax.rem(column_at + k, column_groups)
            for far in (1, 0) if k else (1,):
                frame_to = across(1 << step) if far else frame
                choice = 1 - side[step] if far else side[step]
                push(
                    sums[step].at[slots, choice, owner],
                    final.at[slots, far * column_groups + column_at],
                    x_sem.at[0, index],
                    x_sem.at[1, index],
                    {"dp": clip(row_at, owner), "frame": frame_to},
                )
        for slot in range(first, first + count):
            final[slot, column_at] = sums[step][slot, side[step], column_at]
        sent.append((final.at[slots, pl.ds(0, 2 * column_groups - 1)], x_sem.at[0, index]))

    def halve(item, step):
        first, count, index = item
        half = frame_groups >> (step + 1)
        drain(received[step].at[pl.ds(first, count)], r_sem.at[index, step])
        for slot in range(first, first + count):
            kept = sums[step][slot, pl.ds(side[step] * half, half)].astype(F32)
            total = kept + received[step][slot].astype(F32)
            sums[step + 1][slot] = total.astype(BF16)
        if step < bits - 2:
            send_half(item, step + 1)
            return
        sent.append((part.at[pl.ds(first, count), pl.ds(0, frame_groups - 2)], rs_sem.at[index]))
        send_owners(item)

    def settle(item):
        first, count, index = item
        drain(final.at[pl.ds(first, count), pl.ds(0, 2 * column_groups - 1)], x_sem.at[1, index])
        for slot in range(first, first + count):
            out, start = outputs[slot]
            for c in range(column_groups):
                near, far = final[slot, c], final[slot, column_groups + c]
                total = (near.astype(F32) + far.astype(F32)) * grad_factor
                out[:, start + c * block : start + (c + 1) * block] = total.astype(BF16)

    outputs = [(temporalout_ref, 0)]
    outputs += [(temporalin_ref, i * width) for i in (2, 1, 0)]
    outputs += [(spatialout_ref, 0)]
    outputs += [(spatialin_ref, i * width) for i in (2, 1, 0)]

    with jax.named_scope("a01_norm"):
        loads["frames"].wait()
        loads["bottle"].wait()
        tokens[:patches] = frames_ref[...].astype(F32)
        tokens[patches:] = jnp.zeros((rows - patches, model), F32)
        tokens[patches : patches + bottles] = bottle_ref[...].astype(F32)
        normed, s_inverse = normalize(tokens[...])
        s_normed[...] = normed
        s_low = normed.astype(BF16)
        load("so", spatial_exit_hbm, so_ref)
        load("og", output_grad_hbm, og_send)
        load("te", temporal_entry_hbm, te_ref)
        load("to", temporal_exit_hbm, to_ref)
        load("joined", joined_hbm, joined_ref)
    columns = lax.broadcasted_iota(jnp.int32, (HEADS * rows, rows), 1)
    def enter(i):
        loads[i].wait()


    attended, s_saved = attend(s_low, se_ref, columns < patches + bottles, enter)
    with jax.named_scope("a02_states"):
        loads["so"].wait()
        states = (tokens[:patches] + dot(attended[:patches], so_ref[...], 1, 1)).astype(BF16)
        st_send[...] = states.astype(F32).reshape(frame_groups, group, model).astype(BF16)
        pl.semaphore_wait(barrier, frame_groups + data_groups - 2)
    with jax.named_scope("a03_enter"):
        exchange_frames(st_send, st_recv, 0)
        loads["og"].wait()
        exchange_frames(og_send, og_recv, 1)
        s_nl_shared = share(s_nl_send, s_nl, s_low, True, 0)
        s_att_shared = share(s_att_send, s_att, attended, False, 1)

    t_rows = frame_groups * group
    with jax.named_scope("a04_turn"):
        loads["te"].wait()
        turned_te[...] = te_ref[...].T
        turned_se[...] = se_ref[...].T
    with jax.named_scope("a04_relays"):
        relay(s_nl_shared)
        relay(s_att_shared)
    with jax.named_scope("a05_waitst"):
        arrive_frames(st_recv, 0)
    with jax.named_scope("a06_tempfwd"):
        normed, t_inverse = normalize(st_recv[...].astype(F32).reshape(t_rows, model))
        t_normed[...] = normed
        t_low = normed.astype(BF16)
        t_nl_shared = share(t_nl_send, t_nl, t_low, True, 2)
        shape = (HEADS * t_rows, t_rows)
        row_patch = lax.broadcasted_iota(jnp.int32, shape, 0) & (group - 1)
        column_patch = lax.broadcasted_iota(jnp.int32, shape, 1) & (group - 1)
        attended, t_saved = attend(t_low, te_ref, row_patch == column_patch)
        t_att_shared = share(t_att_send, t_att, attended, False, 3)
    with jax.named_scope("a06_waitog"):
        arrive_frames(og_recv, 1)
    t_cot = og_recv[...].astype(F32).reshape(t_rows, model)
    t_cot_low = t_cot.astype(BF16)
    t_c_shared = share(t_c_send, t_c, t_cot_low, True, 4)
    t_shared = {}

    def keep_temporal(i, value):
        t_shared[i] = share(t_mg_send.at[i], t_mg.at[i], value, False, 5 + i)

    with jax.named_scope("a07_tempbwd"):
        loads["to"].wait()
        mixture_grad = backward_mixture(t_cot_low, to_ref, t_saved, keep_temporal)
        state_grads = backward_inputs(mixture_grad, turned_te, t_cot, t_normed[...], t_inverse)
        sg_send[...] = state_grads.reshape(frame_groups, group, model).astype(BF16)
        exchange_frames(sg_send, sg_recv, 2)

    with jax.named_scope("a08_relays"):
        relay(t_nl_shared)
        relay(t_att_shared)
        relay(t_c_shared)
        cot_ref[patches:] = jnp.zeros((rows - patches, model), F32)
        loads["joined"].wait()
        cot_ref[patches : patches + bottles] = (
            (joined_ref[...].astype(F32) / frame_groups).astype(BF16).astype(F32)
        )
        for i in (2, 1, 0):
            relay(t_shared[i])
    temporal = [(slot, 1, slot) for slot in range(4)]
    spatial = [(4 + slot, 1, 4 + slot) for slot in range(4)]
    with jax.named_scope("a09_waitsg"):
        arrive_frames(sg_recv, 2)
    cot_ref[:patches] = sg_recv[...].astype(F32).reshape(patches, model)
    s_cot_low = cot_ref[...].astype(BF16)
    s_c_shared = share_direct(s_c_send, s_c, s_cot_low, True, 8)
    s_shared = {}

    def keep_spatial(i, value):
        s_shared[i] = share_direct(s_mg_send.at[i], s_mg.at[i], value, False, 9 + i)
        if i == 2:
            with jax.named_scope("b1_w"):
                finish(t_att_shared)
                finish(t_c_shared)
            with jax.named_scope("b1_exit"):
                gradient(0, t_c, t_att)
                send_half(temporal[0], 0)
        if i == 0:
            with jax.named_scope("b2_w"):
                finish(t_nl_shared)
            with jax.named_scope("b2_entry"):
                for slot in (1, 2, 3):
                    finish(t_shared[3 - slot])
                    gradient(slot, t_nl, t_mg.at[3 - slot])
                    send_half(temporal[slot], 0)
                    if slot == 1:
                        halve(temporal[0], 0)

    with jax.named_scope("b3_spatbwd"):
        mixture_grad = backward_mixture(s_cot_low, so_ref, s_saved, keep_spatial)
    with jax.named_scope("b4_inputs"):
        tokens_grad = backward_inputs(mixture_grad, turned_se, cot_ref[...], s_normed[...], s_inverse)
        frames_delta_ref[...] = tokens_grad[:patches].astype(BF16)
        bot_sum[0] = tokens_grad[patches : patches + bottles]

    stores = []

    def store(src, dst):
        copy = pltpu.make_async_copy(src, dst, out_sem.at[len(stores)])
        copy.start()
        stores.append(copy)

    store(frames_delta_ref, frames_delta_hbm)

    bottle_copies = []

    def send_bottles(step):
        bottle_copies.append(
            push(
                bot_sum.at[step],
                bot_recv.at[step],
                b_sem.at[0, step],
                b_sem.at[1, step],
                {"frame": across(1 << step)},
            )
        )

    def add_bottles(step):
        bottle_copies[step].wait_recv()
        total = bot_sum[step] + bot_recv[step]
        if step < bits - 1:
            bot_sum[step + 1] = total
            send_bottles(step + 1)
        else:
            bottle_delta_ref[...] = total.astype(BF16)
            store(bottle_delta_ref, bottle_delta_hbm)

    send_bottles(0)
    with jax.named_scope("b5_halve"):
        for slot in (1, 2, 3):
            halve(temporal[slot], 0)
    finish(s_nl_shared)
    finish(s_att_shared)
    with jax.named_scope("c0_w"):
        finish_direct(s_c_shared)
    with jax.named_scope("c0_mm"):
        gradient(4, s_c, s_att)
        send_half(spatial[0], 0)
        add_bottles(0)
    for n, i in enumerate((2, 1, 0)):
        with jax.named_scope("c%d_w" % (n + 1)):
            finish_direct(s_shared[i])
        with jax.named_scope("c%d_mm" % (n + 1)):
            gradient(5 + n, s_nl, s_mg.at[i])
            send_half(spatial[n + 1], 0)
        with jax.named_scope("c%d_halve" % (n + 1)):
            halve(spatial[n], 0)
    with jax.named_scope("c4_halve"):
        halve(spatial[3], 0)
    for step in range(1, bits - 1):
        with jax.named_scope("d%d_t" % step):
            add_bottles(step)
            for it in temporal:
                halve(it, step)
        for n, it in enumerate(spatial):
            with jax.named_scope("d%d_s%d" % (step, n)):
                halve(it, step)
    with jax.named_scope("e1_t"):
        add_bottles(bits - 1)
        for it in temporal:
            settle(it)
        store(temporalout_ref, temporalout_hbm)
        store(temporalin_ref, temporalin_hbm)
    for n, it in enumerate(spatial):
        with jax.named_scope("e2_s%d" % n):
            settle(it)
    store(spatialout_ref, spatialout_hbm)
    store(spatialin_ref, spatialin_hbm)
    with jax.named_scope("e3_drain"):
        for view, sem in sent:
            drain(view, sem)
        for copy in bottle_copies:
            copy.wait_send()
        for copy in stores:
            copy.wait()


def hand_over(*refs):
    count = len(refs) // 2
    for source, target in zip(refs[:count], refs[count:]):
        target[...] = source[...]


def per_device(
    frames_in,
    bottleneck,
    spatial_entry,
    spatial_exit,
    temporal_entry,
    temporal_exit,
    output_grad,
    joined_grad,
):
    clip_count, frames_local, patches, model = frames_in.shape
    bottles = bottleneck.shape[1]
    frame_groups = lax.axis_size("frame")
    data_groups = lax.axis_size("dp")
    assert clip_count == 1 and frames_local == 1
    entry_width = spatial_entry.shape[1]
    exit_width = spatial_exit.shape[1]
    group = patches // frame_groups
    assert group & (group - 1) == 0
    assert frame_groups & (frame_groups - 1) == 0 and data_groups & (data_groups - 1) == 0
    assert entry_width == 3 * exit_width and frame_groups >= 4
    bits = frame_groups.bit_length() - 1
    row_groups = 1 << ((data_groups.bit_length() - 1) // 2)
    column_groups = data_groups // row_groups
    rows = -(-(patches + bottles) // 16) * 16
    sent_rows = -(-(patches + bottles) // 8) * 8
    t_rows = patches
    wide = model // row_groups
    block = exit_width // column_groups
    owned = model // data_groups // frame_groups
    grad_factor = 1.0 / math.sqrt(patches * data_groups * frame_groups)

    def gather_set(count):
        return [
            pltpu.VMEM((row_groups, count, wide), BF16),
            pltpu.VMEM((data_groups, count, wide), BF16),
            pltpu.VMEM((column_groups, count, block), BF16),
            pltpu.VMEM((data_groups, count, block), BF16),
            pltpu.VMEM((row_groups, count, wide), BF16),
            pltpu.VMEM((data_groups, count, wide), BF16),
            pltpu.VMEM((3, column_groups, count, block), BF16),
            pltpu.VMEM((3, data_groups, count, block), BF16),
        ]

    moved = pltpu.VMEM((frame_groups, group, model), BF16)
    hbm = pl.BlockSpec(memory_space=pl.ANY)
    vmem = pl.BlockSpec(memory_space=pltpu.VMEM)
    out_shape = (
        jax.ShapeDtypeStruct((patches, model), BF16),
        jax.ShapeDtypeStruct((bottles, model), BF16),
        jax.ShapeDtypeStruct((owned, entry_width), BF16),
        jax.ShapeDtypeStruct((owned, exit_width), BF16),
        jax.ShapeDtypeStruct((owned, entry_width), BF16),
        jax.ShapeDtypeStruct((owned, exit_width), BF16),
    )
    outs = pl.pallas_call(
        functools.partial(kernel, frame_groups, row_groups, column_groups, grad_factor),
        out_shape=out_shape,
        in_specs=[hbm] * 8,
        out_specs=[hbm] * 6,
        scratch_shapes=[
            pltpu.VMEM((patches, model), BF16),
            pltpu.VMEM((bottles, model), BF16),
            moved,
            pltpu.VMEM((bottles, model), BF16),
            pltpu.VMEM(spatial_entry.shape, BF16),
            pltpu.VMEM(spatial_exit.shape, BF16),
            pltpu.VMEM(temporal_entry.shape, BF16),
            pltpu.VMEM(temporal_exit.shape, BF16),
            pltpu.VMEM(spatial_entry.shape[::-1], BF16),
            pltpu.VMEM(temporal_entry.shape[::-1], BF16),
            *[pltpu.VMEM(out.shape, BF16) for out in out_shape],
            pltpu.VMEM((rows, model), F32),
            pltpu.VMEM((rows, model), F32),
            pltpu.VMEM((rows, model), F32),
            pltpu.VMEM((t_rows, model), F32),
            moved,
            moved,
            moved,
            moved,
            moved,
            pltpu.VMEM((bits, bottles, model), F32),
            pltpu.VMEM((bits, bottles, model), F32),
            *gather_set(sent_rows),
            *gather_set(t_rows),
            pltpu.VMEM((8, frame_groups, column_groups, owned, block), BF16),
            pltpu.VMEM((8, 2 * column_groups, owned, block), BF16),
            *[
                pltpu.VMEM((8, frame_groups >> s, column_groups, owned, block), BF16)
                for s in range(1, bits)
            ]
            * 2,
            pltpu.SemaphoreType.DMA((10,)),
            pltpu.SemaphoreType.DMA((6,)),
            pltpu.SemaphoreType.DMA((2, 3)),
            pltpu.SemaphoreType.DMA((3, 12)),
            pltpu.SemaphoreType.DMA((8, bits - 1)),
            pltpu.SemaphoreType.DMA((8,)),
            pltpu.SemaphoreType.DMA((2, 8)),
            pltpu.SemaphoreType.DMA((2, bits)),
        ],
        compiler_params=pltpu.CompilerParams(
            collective_id=0, has_side_effects=True, vmem_limit_bytes=61 * 1024 * 1024
        ),
    )(
        frames_in.reshape(patches, model),
        bottleneck.reshape(bottles, model),
        output_grad.reshape(frame_groups, group, model),
        joined_grad.reshape(bottles, model),
        spatial_entry,
        spatial_exit,
        temporal_entry,
        temporal_exit,
    )
    outs = pl.pallas_call(
        hand_over,
        out_shape=[jax.ShapeDtypeStruct(out.shape, out.dtype) for out in outs],
        in_specs=[vmem] * len(outs),
        out_specs=[vmem] * len(outs),
        compiler_params=pltpu.CompilerParams(vmem_limit_bytes=61 * 1024 * 1024),
    )(*outs)
    return (outs[0].reshape(frames_in.shape), outs[1].reshape(bottleneck.shape), *outs[2:])


def solution(mesh):
    return jax.shard_map(
        per_device,
        mesh=mesh,
        in_specs=(
            P("dp", "frame", None, None),
            P("dp", None, None),
            P(),
            P(),
            P(),
            P(),
            P("dp", "frame", None, None),
            P("dp", None, None),
        ),
        out_specs=(
            P("dp", "frame", None, None),
            P("dp", None, None),
            P(("dp", "frame"), None),
            P(("dp", "frame"), None),
            P(("dp", "frame"), None),
            P(("dp", "frame"), None),
        ),
        check_vma=False,
    )
```

```python
import functools
import math

import jax
import jax.numpy as jnp
from jax import lax
from jax.experimental import pallas as pl
from jax.experimental.pallas import tpu as pltpu
from jax.sharding import PartitionSpec as P

HEADS = 8
LANES = 128
EPSILON = 1e-05
MESH = pl.DeviceIdType.MESH
F32 = jnp.float32
BF16 = jnp.bfloat16


def dot(left, right, left_dim=1, right_dim=0):
    return lax.dot_general(
        left, right, (((left_dim,), (right_dim,)), ((), ())), preferred_element_type=F32
    )


def normalize(widened):
    centred = widened - jnp.mean(widened, axis=-1, keepdims=True)
    inverse = lax.rsqrt(jnp.mean(centred * centred, axis=-1, keepdims=True) + EPSILON)
    return centred * inverse, inverse


def head_masks(heads, width, dtype):
    lanes = lax.broadcasted_iota(jnp.int32, (1, width), 1)
    size = width // heads
    return [
        jnp.where((lanes >= h * size) & (lanes < (h + 1) * size), 1.0, 0.0).astype(dtype)
        for h in range(heads)
    ]


def split(rows):
    width = rows.shape[1]
    lanes = max(LANES, width // HEADS)
    return [rows[:, i : i + lanes] for i in range(0, width, lanes)]


def stack_heads(rows, heads):
    return jnp.concatenate([rows * m for m in head_masks(heads, rows.shape[1], rows.dtype)], axis=0)


def merge_heads(stacked, heads):
    count = stacked.shape[0] // heads
    masks = head_masks(heads, stacked.shape[1], stacked.dtype)
    total = stacked[:count] * masks[0]
    for h in range(1, heads):
        total = total + stacked[h * count : (h + 1) * count] * masks[h]
    return total


def attend(normed_low, entry_ref, mask, ready=lambda i: None):
    width = entry_ref.shape[1] // 3
    parts = []
    for i in range(3):
        ready(i)
        parts.append(dot(normed_low, entry_ref[:, i * width : (i + 1) * width]).astype(BF16))
    factor = 1.0 / math.sqrt(width // HEADS)
    saved, attended = [], []
    for queries, key_rows, values in zip(*map(split, parts)):
        heads = HEADS * queries.shape[1] // width
        query_stack = stack_heads(queries, heads)
        scores = dot(query_stack, key_rows, 1, 1) * factor
        here = mask(scores.shape)
        scores = jnp.where(here, scores, -1e30)
        scores = scores - jnp.max(scores, axis=-1, keepdims=True)
        expon = jnp.where(here, jnp.exp(scores), 0.0)
        weights = expon / jnp.sum(expon, axis=-1, keepdims=True)
        weights_low = weights.astype(BF16)
        attended.append(merge_heads(dot(weights_low, values), heads).astype(BF16))
        saved.append((query_stack, key_rows, values, weights, weights_low))
    return jnp.concatenate(attended, axis=1), saved


def backward_mixture(cotangent, exit_ref, saved, emit):
    width = exit_ref.shape[1]
    factor = 1.0 / math.sqrt(width // HEADS)
    attended_grad = split(dot(cotangent, exit_ref[...]).astype(BF16))
    heads = HEADS * attended_grad[0].shape[1] // width
    grad_stacks = [stack_heads(g, heads) for g in attended_grad]
    values_grad = jnp.concatenate(
        [dot(s[4], g, 0, 0).astype(BF16) for s, g in zip(saved, grad_stacks)], axis=1
    )
    emit(2, values_grad)
    scores_grads = []
    for (_, _, values, weights, _), grad_stack in zip(saved, grad_stacks):
        softmax_grad = dot(grad_stack, values, 1, 1)
        centre = jnp.sum(weights * softmax_grad, axis=-1, keepdims=True)
        scores_grads.append((weights * (softmax_grad - centre) * factor).astype(BF16))
    keys_grad = jnp.concatenate(
        [dot(g, s[0], 0, 0).astype(BF16) for s, g in zip(saved, scores_grads)], axis=1
    )
    emit(1, keys_grad)
    queries_grad = jnp.concatenate(
        [merge_heads(dot(g, s[1]), heads).astype(BF16) for s, g in zip(saved, scores_grads)], axis=1
    )
    emit(0, queries_grad)
    return jnp.concatenate([queries_grad, keys_grad, values_grad], axis=1)


def backward_inputs(mixture_grad, turned_ref, cotangent, normed, inverse):
    normed_grad = dot(mixture_grad, turned_ref[...])
    inner = (
        normed_grad
        - jnp.mean(normed_grad, axis=-1, keepdims=True)
        - normed * jnp.mean(normed_grad * normed, axis=-1, keepdims=True)
    )
    return cotangent + inverse * inner


def kernel(
    frame_groups,
    row_groups,
    column_groups,
    grad_factor,
    frames_hbm,
    bottle_hbm,
    output_grad_hbm,
    joined_hbm,
    spatial_entry_hbm,
    spatial_exit_hbm,
    temporal_entry_hbm,
    temporal_exit_hbm,
    frames_delta_ref,
    bottle_delta_ref,
    spatialin_ref,
    spatialout_ref,
    temporalin_ref,
    temporalout_ref,
    frames_ref,
    bottle_ref,
    og_send,
    joined_ref,
    se_ref,
    so_ref,
    te_ref,
    to_ref,
    turned_se,
    turned_te,
    tokens,
    cot_ref,
    s_normed,
    t_normed,
    og_recv,
    st_send,
    st_recv,
    sg_send,
    sg_recv,
    at_send,
    at_recv,
    bot_sum,
    bot_recv,
    s_nl_send,
    s_nl,
    s_att_send,
    s_att,
    s_c_send,
    s_c,
    s_mg_send,
    s_mg,
    t_nl_send,
    t_nl,
    t_att_send,
    t_att,
    t_c_send,
    t_c,
    t_mg_send,
    t_mg,
    *tail,
):
    bits = frame_groups.bit_length() - 1
    part, final = tail[:2]
    received = tail[2 : 1 + bits]
    sums = (part,) + tuple(tail[1 + bits : 2 * bits])
    (
        load_sem,
        f_sem,
        d_sem,
        r_sem,
        rs_sem,
        x_sem,
        b_sem,
    ) = tail[2 * bits :]
    frame = lax.axis_index("frame")
    data = lax.axis_index("dp")
    row_at = data // column_groups
    column_at = lax.rem(data, column_groups)
    data_groups = row_groups * column_groups
    patches, model = frames_ref.shape
    bottles = bottle_ref.shape[0]
    rows = tokens.shape[0]
    group = og_send.shape[1]
    width = to_ref.shape[1]
    block = width // column_groups
    owned = part.shape[3]
    side = [lax.rem(frame // (1 << s), 2) for s in range(bits)]

    loads = {}

    def load(name, src, dst):
        loads[name] = pltpu.make_async_copy(src, dst, load_sem.at[len(loads)])
        loads[name].start()

    load("frames", frames_hbm, frames_ref)
    load("bottle", bottle_hbm, bottle_ref)
    parts = [pl.ds(i * width, width) for i in range(3)]
    for i in range(3):
        load(i, spatial_entry_hbm.at[:, parts[i]], se_ref.at[:, parts[i]])

    barrier = pltpu.get_barrier_semaphore()
    for k in range(1, frame_groups):
        pl.semaphore_signal(
            barrier,
            inc=1,
            device_id={"frame": lax.rem(frame + k, frame_groups)},
            device_id_type=MESH,
        )
    for k in range(1, data_groups):
        pl.semaphore_signal(
            barrier, inc=1, device_id={"dp": lax.rem(data + k, data_groups)}, device_id_type=MESH
        )

    sent = []

    def push(src, dst, send_sem, recv_sem, device):
        copy = pltpu.make_async_remote_copy(
            src_ref=src,
            dst_ref=dst,
            send_sem=send_sem,
            recv_sem=recv_sem,
            device_id=device,
            device_id_type=MESH,
        )
        copy.start()
        return copy

    def drain(view, sem):
        pltpu.make_async_copy(view, view, sem).wait()

    def across(k):
        peer = frame
        for s in range(bits):
            if k >> s & 1:
                peer = peer + (1 << s) * (1 - 2 * side[s])
        return peer

    def exchange_frames(send, dst, phase):
        for k in reversed(range(1, frame_groups)):
            peer = across(k)
            push(
                send.at[peer],
                dst.at[frame],
                f_sem.at[0, phase],
                f_sem.at[1, phase],
                {"frame": peer},
            )
        dst[frame] = send[frame]
        sent.append((dst.at[pl.ds(0, frame_groups - 1)], f_sem.at[0, phase]))

    def arrive_frames(dst, phase):
        drain(dst.at[pl.ds(0, frame_groups - 1)], f_sem.at[1, phase])

    def clip(row, column):
        return row * column_groups + column

    def row_peers():
        return [lax.rem(row_at + k, row_groups) for k in range(1, row_groups)]

    def column_peers():
        return [lax.rem(column_at + k, column_groups) for k in range(1, column_groups)]

    def put_blocks(dst, value):
        count, kept, size = dst.shape
        for i in range(count):
            dst[i] = value[:kept, i * size : (i + 1) * size]

    def share(send, dst, value, by_row, phase):
        put_blocks(send, value)
        mine = row_at if by_row else column_at
        for peer_row in row_peers():
            push(
                send.at[peer_row if by_row else column_at],
                dst.at[data],
                d_sem.at[0, phase],
                d_sem.at[1 if by_row else 2, phase],
                {"dp": clip(peer_row, column_at)},
            )
        for peer_column in column_peers():
            push(
                send.at[row_at if by_row else peer_column],
                dst.at[data],
                d_sem.at[0, phase],
                d_sem.at[2 if by_row else 1, phase],
                {"dp": clip(row_at, peer_column)},
            )
        dst[data] = send[mine]
        sent.append((dst.at[pl.ds(0, data_groups - 1)], d_sem.at[0, phase]))
        return dst, by_row, phase

    def relay(shared):
        dst, by_row, phase = shared
        first = (row_groups if by_row else column_groups) - 1
        drain(dst.at[pl.ds(0, first)], d_sem.at[1, phase])
        for peer_row in row_peers():
            for peer_column in column_peers():
                source = clip(peer_row, column_at) if by_row else clip(row_at, peer_column)
                target = clip(row_at, peer_column) if by_row else clip(peer_row, column_at)
                push(
                    dst.at[source],
                    dst.at[source],
                    d_sem.at[0, phase],
                    d_sem.at[2, phase],
                    {"dp": target},
                )

    def finish(shared):
        dst, by_row, phase = shared
        first = (row_groups if by_row else column_groups) - 1
        drain(dst.at[pl.ds(0, data_groups - 1 - first)], d_sem.at[2, phase])

    def share_direct(send, dst, value, by_row, phase):
        put_blocks(send, value)
        for k in reversed(range(1, data_groups)):
            peer_row = lax.rem(row_at + k // column_groups, row_groups)
            peer_column = lax.rem(column_at + k % column_groups, column_groups)
            push(
                send.at[peer_row if by_row else peer_column],
                dst.at[data],
                d_sem.at[0, phase],
                d_sem.at[1, phase],
                {"dp": clip(peer_row, peer_column)},
            )
        dst[data] = send[row_at if by_row else column_at]
        sent.append((dst.at[pl.ds(0, data_groups - 1)], d_sem.at[0, phase]))
        return dst, by_row, phase

    def finish_direct(shared):
        dst, _, phase = shared
        drain(dst.at[pl.ds(0, data_groups - 1)], d_sem.at[1, phase])

    def gradient(slot, left, right):
        def product_of(low, high):
            count = (high - low) * data_groups
            pieces = [ref[:, low:high] for ref in (left, right)]
            if (high - low) % 16:
                pieces = [p.astype(F32) for p in pieces]
            pieces = [p.reshape(count, p.shape[2]).astype(BF16) for p in pieces]
            return dot(pieces[0], pieces[1], 0, 0)

        product = product_of(0, patches)
        if left.shape[1] > patches:
            product = product + product_of(patches, left.shape[1])
        for f in range(frame_groups):
            place = sum((f >> s & 1) << (bits - 1 - s) for s in range(bits))
            for c in range(column_groups):
                start = (c * frame_groups + f) * owned
                part[slot, place, c] = product[start : start + owned].astype(BF16)

    def send_half(item, step):
        first, count, index = item
        half = frame_groups >> (step + 1)
        slots = pl.ds(first, count)
        push(
            sums[step].at[slots, pl.ds((1 - side[step]) * half, half)],
            received[step].at[slots],
            rs_sem.at[index],
            r_sem.at[index, step],
            {"frame": across(1 << step)},
        )

    def send_owners(item):
        first, count, index = item
        step = bits - 1
        slots = pl.ds(first, count)
        for k in reversed(range(column_groups)):
            owner = lax.rem(column_at + k, column_groups)
            for far in (1, 0) if k else (1,):
                frame_to = across(1 << step) if far else frame
                choice = 1 - side[step] if far else side[step]
                push(
                    sums[step].at[slots, choice, owner],
                    final.at[slots, far * column_groups + column_at],
                    x_sem.at[0, index],
                    x_sem.at[1, index],
                    {"dp": clip(row_at, owner), "frame": frame_to},
                )
        for slot in range(first, first + count):
            final[slot, column_at] = sums[step][slot, side[step], column_at]
        sent.append((final.at[slots, pl.ds(0, 2 * column_groups - 1)], x_sem.at[0, index]))

    def halve(item, step):
        first, count, index = item
        half = frame_groups >> (step + 1)
        drain(received[step].at[pl.ds(first, count)], r_sem.at[index, step])
        for slot in range(first, first + count):
            kept = sums[step][slot, pl.ds(side[step] * half, half)].astype(F32)
            total = kept + received[step][slot].astype(F32)
            sums[step + 1][slot] = total.astype(BF16)
        if step < bits - 2:
            send_half(item, step + 1)
            return
        sent.append((part.at[pl.ds(first, count), pl.ds(0, frame_groups - 2)], rs_sem.at[index]))
        send_owners(item)

    def settle(item):
        first, count, index = item
        drain(final.at[pl.ds(first, count), pl.ds(0, 2 * column_groups - 1)], x_sem.at[1, index])
        for slot in range(first, first + count):
            out, start = outputs[slot]
            for c in range(column_groups):
                near, far = final[slot, c], final[slot, column_groups + c]
                total = (near.astype(F32) + far.astype(F32)) * grad_factor
                out[:, start + c * block : start + (c + 1) * block] = total.astype(BF16)

    def flat(ref, count):
        return ref[...].astype(F32).reshape(count, ref.shape[2]).astype(BF16)

    outputs = [(temporalout_ref, 0)]
    outputs += [(temporalin_ref, i * width) for i in (2, 1, 0)]
    outputs += [(spatialout_ref, 0)]
    outputs += [(spatialin_ref, i * width) for i in (2, 1, 0)]

    with jax.named_scope("a01_norm"):
        loads["frames"].wait()
        loads["bottle"].wait()
        tokens[:patches] = frames_ref[...].astype(F32)
        tokens[patches:] = jnp.zeros((rows - patches, model), F32)
        tokens[patches : patches + bottles] = bottle_ref[...].astype(F32)
        normed, s_inverse = normalize(tokens[...])
        s_normed[...] = normed
        s_low = normed.astype(BF16)
        load("so", spatial_exit_hbm, so_ref)
        load("og", output_grad_hbm, og_send)
        load("te", temporal_entry_hbm, te_ref)
        load("to", temporal_exit_hbm, to_ref)
        load("joined", joined_hbm, joined_ref)
    def real_rows(shape):
        return lax.broadcasted_iota(jnp.int32, shape, 1) < patches + bottles

    def enter(i):
        loads[i].wait()


    attended, s_saved = attend(s_low, se_ref, real_rows, enter)
    with jax.named_scope("a02_states"):
        loads["so"].wait()
        states = (tokens[:patches] + dot(attended[:patches], so_ref[...], 1, 1)).astype(BF16)
        st_send[...] = states.astype(F32).reshape(frame_groups, group, model).astype(BF16)
        pl.semaphore_wait(barrier, frame_groups + data_groups - 2)
    with jax.named_scope("a03_enter"):
        exchange_frames(st_send, st_recv, 0)
        loads["og"].wait()
        exchange_frames(og_send, og_recv, 1)
        t_c_shared = share(t_c_send, t_c, flat(og_send, patches), True, 4)
        s_nl_shared = share(s_nl_send, s_nl, s_low, True, 0)
        s_att_shared = share(s_att_send, s_att, attended, False, 1)

    t_rows = frame_groups * group
    with jax.named_scope("a04_turn"):
        loads["te"].wait()
        turned_te[...] = te_ref[...].T
        turned_se[...] = se_ref[...].T
    with jax.named_scope("a04_relays"):
        relay(t_c_shared)
    def same_patch(shape):
        row_patch = lax.broadcasted_iota(jnp.int32, shape, 0) & (group - 1)
        column_patch = lax.broadcasted_iota(jnp.int32, shape, 1) & (group - 1)
        return row_patch == column_patch

    with jax.named_scope("a05_waitst"):
        arrive_frames(st_recv, 0)
    with jax.named_scope("a06_tempfwd"):
        normed, t_inverse = normalize(st_recv[...].astype(F32).reshape(t_rows, model))
        t_normed[...] = normed
        t_low = normed.astype(BF16)
        t_nl_shared = share_direct(t_nl_send, t_nl, t_low, True, 2)
        attended, t_saved = attend(t_low, te_ref, same_patch)
        at_send[...] = attended.astype(F32).reshape(at_send.shape).astype(BF16)
        exchange_frames(at_send, at_recv, 3)
    with jax.named_scope("a06_waitog"):
        arrive_frames(og_recv, 1)
    t_cot = og_recv[...].astype(F32).reshape(t_rows, model)
    t_cot_low = t_cot.astype(BF16)
    t_shared = {}

    def keep_temporal(i, value):
        t_shared[i] = share_direct(t_mg_send.at[i], t_mg.at[i], value, False, 5 + i)

    with jax.named_scope("a07_tempbwd"):
        loads["to"].wait()
        mixture_grad = backward_mixture(t_cot_low, to_ref, t_saved, keep_temporal)
        state_grads = backward_inputs(mixture_grad, turned_te, t_cot, t_normed[...], t_inverse)
        sg_send[...] = state_grads.reshape(frame_groups, group, model).astype(BF16)
        exchange_frames(sg_send, sg_recv, 2)

    with jax.named_scope("a08_relays"):
        relay(s_nl_shared)
        relay(s_att_shared)
        arrive_frames(at_recv, 3)
        t_att_shared = share_direct(t_att_send, t_att, flat(at_recv, patches), False, 3)
        cot_ref[patches:] = jnp.zeros((rows - patches, model), F32)
        loads["joined"].wait()
        cot_ref[patches : patches + bottles] = (
            (joined_ref[...].astype(F32) / frame_groups).astype(BF16).astype(F32)
        )
    temporal = [(slot, 1, slot) for slot in range(4)]
    spatial = [(4 + slot, 1, 4 + slot) for slot in range(4)]
    with jax.named_scope("a09_waitsg"):
        arrive_frames(sg_recv, 2)
    cot_ref[:patches] = sg_recv[...].astype(F32).reshape(patches, model)
    s_cot_low = cot_ref[...].astype(BF16)
    s_c_shared = share_direct(s_c_send, s_c, s_cot_low, True, 8)
    s_shared = {}

    def keep_spatial(i, value):
        s_shared[i] = share_direct(s_mg_send.at[i], s_mg.at[i], value, False, 9 + i)
        if i == 0:
            with jax.named_scope("b1_w"):
                finish_direct(t_nl_shared)
                finish_direct(t_shared[2])
            with jax.named_scope("b1_entry"):
                for slot in (1, 2, 3):
                    if slot > 1:
                        finish_direct(t_shared[3 - slot])
                    gradient(slot, t_nl, t_mg.at[3 - slot])
                    send_half(temporal[slot], 0)

    with jax.named_scope("b3_spatbwd"):
        mixture_grad = backward_mixture(s_cot_low, so_ref, s_saved, keep_spatial)
    with jax.named_scope("b4_inputs"):
        tokens_grad = backward_inputs(mixture_grad, turned_se, cot_ref[...], s_normed[...], s_inverse)
        frames_delta_ref[...] = tokens_grad[:patches].astype(BF16)
        bot_sum[0] = tokens_grad[patches : patches + bottles]

    bottle_copies = []

    def send_bottles(step):
        bottle_copies.append(
            push(
                bot_sum.at[step],
                bot_recv.at[step],
                b_sem.at[0, step],
                b_sem.at[1, step],
                {"frame": across(1 << step)},
            )
        )

    def add_bottles(step):
        bottle_copies[step].wait_recv()
        total = bot_sum[step] + bot_recv[step]
        if step < bits - 1:
            bot_sum[step + 1] = total
            send_bottles(step + 1)
        else:
            bottle_delta_ref[...] = total.astype(BF16)

    send_bottles(0)
    with jax.named_scope("b5_halve"):
        for slot in (1, 2, 3):
            halve(temporal[slot], 0)
    with jax.named_scope("b6_w"):
        finish(t_c_shared)
        finish_direct(t_att_shared)
    with jax.named_scope("b6_exit"):
        gradient(0, t_c, t_att)
        send_half(temporal[0], 0)
    with jax.named_scope("b7_halve"):
        add_bottles(0)
        halve(temporal[1], 1)
        halve(temporal[0], 0)
        halve(temporal[2], 1)
    finish(s_nl_shared)
    finish(s_att_shared)
    with jax.named_scope("c0_w"):
        finish_direct(s_c_shared)
    with jax.named_scope("c0_mm"):
        gradient(4, s_c, s_att)
        send_half(spatial[0], 0)
    for n, i in enumerate((2, 1, 0)):
        with jax.named_scope("c%d_w" % (n + 1)):
            finish_direct(s_shared[i])
        with jax.named_scope("c%d_mm" % (n + 1)):
            gradient(5 + n, s_nl, s_mg.at[i])
            send_half(spatial[n + 1], 0)
        with jax.named_scope("c%d_halve" % (n + 1)):
            halve(spatial[n], 0)
            if n == 1:
                halve(temporal[3], 1)
    with jax.named_scope("c4_halve"):
        halve(spatial[3], 0)
        halve(temporal[0], 1)
    for step in range(1, bits - 1):
        with jax.named_scope("d%d_t" % step):
            add_bottles(step)
            if step > 1:
                for it in temporal:
                    halve(it, step)
        for n, it in enumerate(spatial):
            with jax.named_scope("d%d_s%d" % (step, n)):
                halve(it, step)
    with jax.named_scope("e1_t"):
        add_bottles(bits - 1)
        for it in temporal[1:] + temporal[:1]:
            settle(it)
    for n, it in enumerate(spatial):
        with jax.named_scope("e2_s%d" % n):
            settle(it)
    with jax.named_scope("e3_drain"):
        for view, sem in sent:
            drain(view, sem)
        for copy in bottle_copies:
            copy.wait_send()


def hand_over(*refs):
    count = len(refs) // 2
    for source, target in zip(refs[:count], refs[count:]):
        target[...] = source[...]


def per_device(
    frames_in,
    bottleneck,
    spatial_entry,
    spatial_exit,
    temporal_entry,
    temporal_exit,
    output_grad,
    joined_grad,
):
    clip_count, frames_local, patches, model = frames_in.shape
    bottles = bottleneck.shape[1]
    frame_groups = lax.axis_size("frame")
    data_groups = lax.axis_size("dp")
    assert clip_count == 1 and frames_local == 1
    entry_width = spatial_entry.shape[1]
    exit_width = spatial_exit.shape[1]
    group = patches // frame_groups
    assert group & (group - 1) == 0
    assert frame_groups & (frame_groups - 1) == 0 and data_groups & (data_groups - 1) == 0
    assert entry_width == 3 * exit_width and frame_groups >= 4
    bits = frame_groups.bit_length() - 1
    row_groups = 1 << ((data_groups.bit_length() - 1) // 2)
    column_groups = data_groups // row_groups
    rows = -(-(patches + bottles) // 16) * 16
    sent_rows = -(-(patches + bottles) // 8) * 8
    t_rows = patches
    wide = model // row_groups
    block = exit_width // column_groups
    owned = model // data_groups // frame_groups
    grad_factor = 1.0 / math.sqrt(patches * data_groups * frame_groups)

    def gather_set(count):
        return [
            pltpu.VMEM((row_groups, count, wide), BF16),
            pltpu.VMEM((data_groups, count, wide), BF16),
            pltpu.VMEM((column_groups, count, block), BF16),
            pltpu.VMEM((data_groups, count, block), BF16),
            pltpu.VMEM((row_groups, count, wide), BF16),
            pltpu.VMEM((data_groups, count, wide), BF16),
            pltpu.VMEM((3, column_groups, count, block), BF16),
            pltpu.VMEM((3, data_groups, count, block), BF16),
        ]

    moved = pltpu.VMEM((frame_groups, group, model), BF16)
    hbm = pl.BlockSpec(memory_space=pltpu.HBM)
    vmem = pl.BlockSpec(memory_space=pltpu.VMEM)
    out_shape = (
        jax.ShapeDtypeStruct((patches, model), BF16),
        jax.ShapeDtypeStruct((bottles, model), BF16),
        jax.ShapeDtypeStruct((owned, entry_width), BF16),
        jax.ShapeDtypeStruct((owned, exit_width), BF16),
        jax.ShapeDtypeStruct((owned, entry_width), BF16),
        jax.ShapeDtypeStruct((owned, exit_width), BF16),
    )
    outs = pl.pallas_call(
        functools.partial(kernel, frame_groups, row_groups, column_groups, grad_factor),
        out_shape=out_shape,
        in_specs=[hbm] * 8,
        out_specs=[vmem] * 6,
        scratch_shapes=[
            pltpu.VMEM((patches, model), BF16),
            pltpu.VMEM((bottles, model), BF16),
            moved,
            pltpu.VMEM((bottles, model), BF16),
            pltpu.VMEM(spatial_entry.shape, BF16),
            pltpu.VMEM(spatial_exit.shape, BF16),
            pltpu.VMEM(temporal_entry.shape, BF16),
            pltpu.VMEM(temporal_exit.shape, BF16),
            pltpu.VMEM(spatial_entry.shape[::-1], BF16),
            pltpu.VMEM(temporal_entry.shape[::-1], BF16),
            pltpu.VMEM((rows, model), F32),
            pltpu.VMEM((rows, model), F32),
            pltpu.VMEM((rows, model), F32),
            pltpu.VMEM((t_rows, model), F32),
            moved,
            moved,
            moved,
            moved,
            moved,
            *[pltpu.VMEM((frame_groups, group, exit_width), BF16)] * 2,
            pltpu.VMEM((bits, bottles, model), F32),
            pltpu.VMEM((bits, bottles, model), F32),
            *gather_set(sent_rows),
            *gather_set(t_rows),
            pltpu.VMEM((8, frame_groups, column_groups, owned, block), BF16),
            pltpu.VMEM((8, 2 * column_groups, owned, block), BF16),
            *[
                pltpu.VMEM((8, frame_groups >> s, column_groups, owned, block), BF16)
                for s in range(1, bits)
            ]
            * 2,
            pltpu.SemaphoreType.DMA((10,)),
            pltpu.SemaphoreType.DMA((2, 4)),
            pltpu.SemaphoreType.DMA((3, 12)),
            pltpu.SemaphoreType.DMA((8, bits - 1)),
            pltpu.SemaphoreType.DMA((8,)),
            pltpu.SemaphoreType.DMA((2, 8)),
            pltpu.SemaphoreType.DMA((2, bits)),
        ],
        compiler_params=pltpu.CompilerParams(
            collective_id=0, has_side_effects=True, vmem_limit_bytes=40 * 1024 * 1024
        ),
    )(
        *[
            pltpu.with_memory_space_constraint(x, pltpu.HBM)
            for x in (
                frames_in.reshape(patches, model),
                bottleneck.reshape(bottles, model),
                output_grad.reshape(frame_groups, group, model),
                joined_grad.reshape(bottles, model),
                spatial_entry,
                spatial_exit,
                temporal_entry,
                temporal_exit,
            )
        ]
    )
    outs = pl.pallas_call(
        hand_over,
        out_shape=[jax.ShapeDtypeStruct(out.shape, out.dtype) for out in outs],
        in_specs=[vmem] * len(outs),
        out_specs=[vmem] * len(outs),
        compiler_params=pltpu.CompilerParams(vmem_limit_bytes=40 * 1024 * 1024),
    )(*outs)
    return (outs[0].reshape(frames_in.shape), outs[1].reshape(bottleneck.shape), *outs[2:])


def solution(mesh):
    return jax.shard_map(
        per_device,
        mesh=mesh,
        in_specs=(
            P("dp", "frame", None, None),
            P("dp", None, None),
            P(),
            P(),
            P(),
            P(),
            P("dp", "frame", None, None),
            P("dp", None, None),
        ),
        out_specs=(
            P("dp", "frame", None, None),
            P("dp", None, None),
            P(("dp", "frame"), None),
            P(("dp", "frame"), None),
            P(("dp", "frame"), None),
            P(("dp", "frame"), None),
        ),
        check_vma=False,
    )
```

```python
import functools
import math

import jax
import jax.numpy as jnp
from jax import lax
from jax.experimental import pallas as pl
from jax.experimental.pallas import tpu as pltpu
from jax.sharding import PartitionSpec as P

HEADS = 8
LANES = 128
EPSILON = 1e-05
MESH = pl.DeviceIdType.MESH
F32 = jnp.float32
BF16 = jnp.bfloat16


def dot(left, right, left_dim=1, right_dim=0):
    return lax.dot_general(
        left, right, (((left_dim,), (right_dim,)), ((), ())), preferred_element_type=F32
    )


def normalize(widened):
    centred = widened - jnp.mean(widened, axis=-1, keepdims=True)
    inverse = lax.rsqrt(jnp.mean(centred * centred, axis=-1, keepdims=True) + EPSILON)
    return centred * inverse, inverse


def head_masks(heads, width, dtype):
    lanes = lax.broadcasted_iota(jnp.int32, (1, width), 1)
    size = width // heads
    return [
        jnp.where((lanes >= h * size) & (lanes < (h + 1) * size), 1.0, 0.0).astype(dtype)
        for h in range(heads)
    ]


def split(rows):
    width = rows.shape[1]
    lanes = max(LANES, width // HEADS)
    return [rows[:, i : i + lanes] for i in range(0, width, lanes)]


def stack_heads(rows, heads):
    return jnp.concatenate([rows * m for m in head_masks(heads, rows.shape[1], rows.dtype)], axis=0)


def merge_heads(stacked, heads):
    count = stacked.shape[0] // heads
    masks = head_masks(heads, stacked.shape[1], stacked.dtype)
    total = stacked[:count] * masks[0]
    for h in range(1, heads):
        total = total + stacked[h * count : (h + 1) * count] * masks[h]
    return total


def attend(normed_low, entry_ref, mask, ready=lambda i: None):
    width = entry_ref.shape[1] // 3
    parts = []
    for i in range(3):
        ready(i)
        parts.append(dot(normed_low, entry_ref[:, i * width : (i + 1) * width]).astype(BF16))
    factor = 1.0 / math.sqrt(width // HEADS)
    saved, attended = [], []
    for queries, key_rows, values in zip(*map(split, parts)):
        heads = HEADS * queries.shape[1] // width
        query_stack = stack_heads(queries, heads)
        scores = dot(query_stack, key_rows, 1, 1) * factor
        here = mask(scores.shape)
        scores = jnp.where(here, scores, -1e30)
        scores = scores - jnp.max(scores, axis=-1, keepdims=True)
        expon = jnp.where(here, jnp.exp(scores), 0.0)
        weights = expon / jnp.sum(expon, axis=-1, keepdims=True)
        weights_low = weights.astype(BF16)
        attended.append(merge_heads(dot(weights_low, values), heads).astype(BF16))
        saved.append((query_stack, key_rows, values, weights, weights_low))
    return jnp.concatenate(attended, axis=1), saved


def backward_mixture(cotangent, exit_ref, saved, emit):
    width = exit_ref.shape[1]
    factor = 1.0 / math.sqrt(width // HEADS)
    attended_grad = split(dot(cotangent, exit_ref[...]).astype(BF16))
    heads = HEADS * attended_grad[0].shape[1] // width
    grad_stacks = [stack_heads(g, heads) for g in attended_grad]
    values_grad = jnp.concatenate(
        [dot(s[4], g, 0, 0).astype(BF16) for s, g in zip(saved, grad_stacks)], axis=1
    )
    emit(2, values_grad)
    scores_grads = []
    for (_, _, values, weights, _), grad_stack in zip(saved, grad_stacks):
        softmax_grad = dot(grad_stack, values, 1, 1)
        centre = jnp.sum(weights * softmax_grad, axis=-1, keepdims=True)
        scores_grads.append((weights * (softmax_grad - centre) * factor).astype(BF16))
    keys_grad = jnp.concatenate(
        [dot(g, s[0], 0, 0).astype(BF16) for s, g in zip(saved, scores_grads)], axis=1
    )
    emit(1, keys_grad)
    queries_grad = jnp.concatenate(
        [merge_heads(dot(g, s[1]), heads).astype(BF16) for s, g in zip(saved, scores_grads)], axis=1
    )
    emit(0, queries_grad)
    return jnp.concatenate([queries_grad, keys_grad, values_grad], axis=1)


def backward_inputs(mixture_grad, turned_ref, cotangent, normed, inverse):
    normed_grad = dot(mixture_grad, turned_ref[...])
    inner = (
        normed_grad
        - jnp.mean(normed_grad, axis=-1, keepdims=True)
        - normed * jnp.mean(normed_grad * normed, axis=-1, keepdims=True)
    )
    return cotangent + inverse * inner


def kernel(
    frame_groups,
    row_groups,
    column_groups,
    grad_factor,
    frames_hbm,
    bottle_hbm,
    output_grad_hbm,
    joined_hbm,
    spatial_entry_hbm,
    spatial_exit_hbm,
    temporal_entry_hbm,
    temporal_exit_hbm,
    frames_delta_ref,
    bottle_delta_ref,
    spatialin_ref,
    spatialout_ref,
    temporalin_ref,
    temporalout_ref,
    frames_ref,
    bottle_ref,
    og_send,
    joined_ref,
    se_ref,
    so_ref,
    te_ref,
    to_ref,
    turned_se,
    turned_te,
    tokens,
    cot_ref,
    s_normed,
    t_normed,
    og_recv,
    st_send,
    st_recv,
    sg_send,
    sg_recv,
    at_send,
    at_recv,
    bot_sum,
    bot_recv,
    s_nl_send,
    s_nl,
    s_att_send,
    s_att,
    s_c_send,
    s_c,
    s_mg_send,
    s_mg,
    t_nl_send,
    t_nl,
    t_att_send,
    t_att,
    t_c_send,
    t_c,
    t_mg_send,
    t_mg,
    *tail,
):
    bits = frame_groups.bit_length() - 1
    part, final = tail[:2]
    received = tail[2 : 1 + bits]
    sums = (part,) + tuple(tail[1 + bits : 2 * bits])
    (
        load_sem,
        f_sem,
        d_sem,
        dr_sem,
        r_sem,
        rs_sem,
        x_sem,
        xs_sem,
        b_sem,
    ) = tail[2 * bits :]
    frame = lax.axis_index("frame")
    data = lax.axis_index("dp")
    row_at = data // column_groups
    column_at = lax.rem(data, column_groups)
    data_groups = row_groups * column_groups
    patches, model = frames_ref.shape
    bottles = bottle_ref.shape[0]
    rows = tokens.shape[0]
    group = og_send.shape[1]
    width = to_ref.shape[1]
    block = width // column_groups
    owned = part.shape[3]
    side = [lax.rem(frame // (1 << s), 2) for s in range(bits)]

    loads = {}

    def load(name, src, dst):
        loads[name] = pltpu.make_async_copy(src, dst, load_sem.at[len(loads)])
        loads[name].start()

    load("frames", frames_hbm, frames_ref)
    load("bottle", bottle_hbm, bottle_ref)
    parts = [pl.ds(i * width, width) for i in range(3)]
    for i in range(3):
        load(i, spatial_entry_hbm.at[:, parts[i]], se_ref.at[:, parts[i]])

    barrier = pltpu.get_barrier_semaphore()
    for k in range(1, frame_groups):
        pl.semaphore_signal(
            barrier,
            inc=1,
            device_id={"frame": lax.rem(frame + k, frame_groups)},
            device_id_type=MESH,
        )
    for k in range(1, data_groups):
        pl.semaphore_signal(
            barrier, inc=1, device_id={"dp": lax.rem(data + k, data_groups)}, device_id_type=MESH
        )

    sent = []

    def push(src, dst, send_sem, recv_sem, device):
        copy = pltpu.make_async_remote_copy(
            src_ref=src,
            dst_ref=dst,
            send_sem=send_sem,
            recv_sem=recv_sem,
            device_id=device,
            device_id_type=MESH,
        )
        copy.start()
        return copy

    def drain(view, sem):
        pltpu.make_async_copy(view, view, sem).wait()

    def across(k):
        peer = frame
        for s in range(bits):
            if k >> s & 1:
                peer = peer + (1 << s) * (1 - 2 * side[s])
        return peer

    def exchange_frames(send, dst, phase, far_first=True):
        order = range(1, frame_groups)
        for k in reversed(order) if far_first else order:
            peer = across(k)
            push(
                send.at[peer],
                dst.at[frame],
                f_sem.at[0, phase],
                f_sem.at[1, phase],
                {"frame": peer},
            )
        dst[frame] = send[frame]
        sent.append((dst.at[pl.ds(0, frame_groups - 1)], f_sem.at[0, phase]))

    def arrive_frames(dst, phase):
        drain(dst.at[pl.ds(0, frame_groups - 1)], f_sem.at[1, phase])

    def clip(row, column):
        return row * column_groups + column

    def row_peers():
        return [lax.rem(row_at + k, row_groups) for k in range(1, row_groups)]

    def column_peers():
        return [lax.rem(column_at + k, column_groups) for k in range(1, column_groups)]

    def put_blocks(dst, value):
        count, kept, size = dst.shape
        for i in range(count):
            dst[i] = value[:kept, i * size : (i + 1) * size]

    def send_slot(phase):
        return phase if phase < 5 else 5 if phase < 8 else 6 if phase == 8 else 7

    def share(send, dst, value, by_row, phase):
        put_blocks(send, value)
        mine = row_at if by_row else column_at
        for peer_row in row_peers():
            push(
                send.at[peer_row if by_row else column_at],
                dst.at[data],
                d_sem.at[send_slot(phase)],
                dr_sem.at[phase if by_row else 12 + min(phase, 2)],
                {"dp": clip(peer_row, column_at)},
            )
        for peer_column in column_peers():
            push(
                send.at[row_at if by_row else peer_column],
                dst.at[data],
                d_sem.at[send_slot(phase)],
                dr_sem.at[12 + min(phase, 2) if by_row else phase],
                {"dp": clip(row_at, peer_column)},
            )
        dst[data] = send[mine]
        sent.append((dst.at[pl.ds(0, data_groups - 1)], d_sem.at[send_slot(phase)]))
        return dst, by_row, phase

    def relay(shared):
        dst, by_row, phase = shared
        first = (row_groups if by_row else column_groups) - 1
        drain(dst.at[pl.ds(0, first)], dr_sem.at[phase])
        for peer_row in row_peers():
            for peer_column in column_peers():
                source = clip(peer_row, column_at) if by_row else clip(row_at, peer_column)
                target = clip(row_at, peer_column) if by_row else clip(peer_row, column_at)
                push(
                    dst.at[source],
                    dst.at[source],
                    d_sem.at[send_slot(phase)],
                    dr_sem.at[12 + min(phase, 2)],
                    {"dp": target},
                )

    def finish(shared):
        dst, by_row, phase = shared
        first = (row_groups if by_row else column_groups) - 1
        drain(dst.at[pl.ds(0, data_groups - 1 - first)], dr_sem.at[12 + min(phase, 2)])

    def share_direct(send, dst, value, by_row, phase):
        put_blocks(send, value)
        for k in reversed(range(1, data_groups)):
            peer_row = lax.rem(row_at + k // column_groups, row_groups)
            peer_column = lax.rem(column_at + k % column_groups, column_groups)
            push(
                send.at[peer_row if by_row else peer_column],
                dst.at[data],
                d_sem.at[send_slot(phase)],
                dr_sem.at[phase],
                {"dp": clip(peer_row, peer_column)},
            )
        dst[data] = send[row_at if by_row else column_at]
        if send_slot(phase) not in (5, 7):
            sent.append((dst.at[pl.ds(0, data_groups - 1)], d_sem.at[send_slot(phase)]))
        return dst, by_row, phase

    def finish_direct(shared):
        dst, _, phase = shared
        drain(dst.at[pl.ds(0, data_groups - 1)], dr_sem.at[phase])

    def gradient(slot, left, right):
        def product_of(low, high):
            count = (high - low) * data_groups
            pieces = [ref[:, low:high] for ref in (left, right)]
            if (high - low) % 16:
                pieces = [p.astype(F32) for p in pieces]
            pieces = [p.reshape(count, p.shape[2]).astype(BF16) for p in pieces]
            return dot(pieces[0], pieces[1], 0, 0)

        product = product_of(0, patches)
        if left.shape[1] > patches:
            product = product + product_of(patches, left.shape[1])
        for f in range(frame_groups):
            place = sum((f >> s & 1) << (bits - 1 - s) for s in range(bits))
            for c in range(column_groups):
                start = (c * frame_groups + f) * owned
                part[slot, place, c] = product[start : start + owned].astype(BF16)

    def send_half(item, step):
        first, count, index = item
        half = frame_groups >> (step + 1)
        slots = pl.ds(first, count)
        push(
            sums[step].at[slots, pl.ds((1 - side[step]) * half, half)],
            received[step].at[slots],
            rs_sem,
            r_sem.at[index, step],
            {"frame": across(1 << step)},
        )

    def send_owners(item):
        first, count, index = item
        step = bits - 1
        slots = pl.ds(first, count)
        for k in reversed(range(column_groups)):
            owner = lax.rem(column_at + k, column_groups)
            for far in (1, 0) if k else (1,):
                frame_to = across(1 << step) if far else frame
                choice = 1 - side[step] if far else side[step]
                push(
                    sums[step].at[slots, choice, owner],
                    final.at[slots, far * column_groups + column_at],
                    xs_sem,
                    x_sem.at[index],
                    {"dp": clip(row_at, owner), "frame": frame_to},
                )
        for slot in range(first, first + count):
            final[slot, column_at] = sums[step][slot, side[step], column_at]

    def halve(item, step):
        first, count, index = item
        half = frame_groups >> (step + 1)
        drain(received[step].at[pl.ds(first, count)], r_sem.at[index, step])
        for slot in range(first, first + count):
            kept = sums[step][slot, pl.ds(side[step] * half, half)].astype(F32)
            total = kept + received[step][slot].astype(F32)
            sums[step + 1][slot] = total.astype(BF16)
        if step < bits - 2:
            send_half(item, step + 1)
            return
        send_owners(item)

    def settle(item):
        first, count, index = item
        drain(final.at[pl.ds(first, count), pl.ds(0, 2 * column_groups - 1)], x_sem.at[index])
        for slot in range(first, first + count):
            out, start = outputs[slot]
            for c in range(column_groups):
                near, far = final[slot, c], final[slot, column_groups + c]
                total = (near.astype(F32) + far.astype(F32)) * grad_factor
                out[:, start + c * block : start + (c + 1) * block] = total.astype(BF16)

    def flat(ref, count):
        return ref[...].astype(F32).reshape(count, ref.shape[2]).astype(BF16)

    outputs = [(temporalout_ref, 0)]
    outputs += [(temporalin_ref, i * width) for i in (2, 1, 0)]
    outputs += [(spatialout_ref, 0)]
    outputs += [(spatialin_ref, i * width) for i in (2, 1, 0)]

    with jax.named_scope("a01_norm"):
        loads["frames"].wait()
        loads["bottle"].wait()
        tokens[:patches] = frames_ref[...].astype(F32)
        tokens[patches:] = jnp.zeros((rows - patches, model), F32)
        tokens[patches : patches + bottles] = bottle_ref[...].astype(F32)
        normed, s_inverse = normalize(tokens[...])
        s_normed[...] = normed
        s_low = normed.astype(BF16)
        load("so", spatial_exit_hbm, so_ref)
        load("og", output_grad_hbm, og_send)
        load("te", temporal_entry_hbm, te_ref)
        load("to", temporal_exit_hbm, to_ref)
        load("joined", joined_hbm, joined_ref)
    def real_rows(shape):
        return lax.broadcasted_iota(jnp.int32, shape, 1) < patches + bottles

    def enter(i):
        loads[i].wait()


    attended, s_saved = attend(s_low, se_ref, real_rows, enter)
    with jax.named_scope("a02_states"):
        loads["so"].wait()
        states = (tokens[:patches] + dot(attended[:patches], so_ref[...], 1, 1)).astype(BF16)
        st_send[...] = states.astype(F32).reshape(frame_groups, group, model).astype(BF16)
        pl.semaphore_wait(barrier, frame_groups + data_groups - 2)
    with jax.named_scope("a03_enter"):
        exchange_frames(st_send, st_recv, 0)
        loads["og"].wait()
        exchange_frames(og_send, og_recv, 1, far_first=False)
        t_c_shared = share(t_c_send, t_c, flat(og_send, patches), True, 4)
        s_nl_shared = share(s_nl_send, s_nl, s_low, True, 0)
        s_att_shared = share(s_att_send, s_att, attended, False, 1)

    t_rows = frame_groups * group
    with jax.named_scope("a04_turn"):
        loads["te"].wait()
        turned_te[...] = te_ref[...].T
        turned_se[...] = se_ref[...].T
    with jax.named_scope("a04_relays"):
        relay(t_c_shared)
    def same_patch(shape):
        row_patch = lax.broadcasted_iota(jnp.int32, shape, 0) & (group - 1)
        column_patch = lax.broadcasted_iota(jnp.int32, shape, 1) & (group - 1)
        return row_patch == column_patch

    with jax.named_scope("a05_waitst"):
        arrive_frames(st_recv, 0)
    with jax.named_scope("a06_tempfwd"):
        normed, t_inverse = normalize(st_recv[...].astype(F32).reshape(t_rows, model))
        t_normed[...] = normed
        t_low = normed.astype(BF16)
        t_nl_shared = share_direct(t_nl_send, t_nl, t_low, True, 2)
        attended, t_saved = attend(t_low, te_ref, same_patch)
        at_send[...] = attended.astype(F32).reshape(at_send.shape).astype(BF16)
        exchange_frames(at_send, at_recv, 3)
    with jax.named_scope("a06_waitog"):
        arrive_frames(og_recv, 1)
    t_cot = og_recv[...].astype(F32).reshape(t_rows, model)
    t_cot_low = t_cot.astype(BF16)
    t_shared = {}

    def keep_temporal(i, value):
        t_shared[i] = share_direct(t_mg_send.at[i], t_mg.at[i], value, False, 5 + i)

    with jax.named_scope("a07_tempbwd"):
        loads["to"].wait()
        mixture_grad = backward_mixture(t_cot_low, to_ref, t_saved, keep_temporal)
        state_grads = backward_inputs(mixture_grad, turned_te, t_cot, t_normed[...], t_inverse)
        sg_send[...] = state_grads.reshape(frame_groups, group, model).astype(BF16)
        exchange_frames(sg_send, sg_recv, 2)

    with jax.named_scope("a08_relays"):
        relay(s_nl_shared)
        relay(s_att_shared)
        arrive_frames(at_recv, 3)
        t_att_shared = share_direct(t_att_send, t_att, flat(at_recv, patches), False, 3)
        cot_ref[patches:] = jnp.zeros((rows - patches, model), F32)
        loads["joined"].wait()
        cot_ref[patches : patches + bottles] = (
            (joined_ref[...].astype(F32) / frame_groups).astype(BF16).astype(F32)
        )
    temporal = [(slot, 1, slot) for slot in range(4)]
    spatial = [(4 + slot, 1, 4 + slot) for slot in range(4)]
    def reduce_entry(slot):
        finish_direct(t_shared[3 - slot])
        gradient(slot, t_nl, t_mg.at[3 - slot])
        send_half(temporal[slot], 0)

    with jax.named_scope("b1_first"):
        finish_direct(t_nl_shared)
        reduce_entry(1)
    with jax.named_scope("a09_waitsg"):
        arrive_frames(sg_recv, 2)
    cot_ref[:patches] = sg_recv[...].astype(F32).reshape(patches, model)
    s_cot_low = cot_ref[...].astype(BF16)
    s_c_shared = share_direct(s_c_send, s_c, s_cot_low, True, 8)
    s_shared = {}

    def keep_spatial(i, value):
        s_shared[i] = share_direct(s_mg_send.at[i], s_mg.at[i], value, False, 9 + i)
        if i == 2:
            with jax.named_scope("b3_third"):
                halve(temporal[2], 0)
                reduce_entry(3)
        if i == 0:
            halve(temporal[3], 0)

    with jax.named_scope("b2_second"):
        halve(temporal[1], 0)
        reduce_entry(2)
    with jax.named_scope("b3_spatbwd"):
        mixture_grad = backward_mixture(s_cot_low, so_ref, s_saved, keep_spatial)
    with jax.named_scope("b4_inputs"):
        tokens_grad = backward_inputs(mixture_grad, turned_se, cot_ref[...], s_normed[...], s_inverse)
        frames_delta_ref[...] = tokens_grad[:patches].astype(BF16)
        bot_sum[0] = tokens_grad[patches : patches + bottles]

    bottle_copies = []

    def send_bottles(step):
        bottle_copies.append(
            push(
                bot_sum.at[step],
                bot_recv.at[step],
                b_sem.at[0, step],
                b_sem.at[1, step],
                {"frame": across(1 << step)},
            )
        )

    def add_bottles(step):
        bottle_copies[step].wait_recv()
        total = bot_sum[step] + bot_recv[step]
        if step < bits - 1:
            bot_sum[step + 1] = total
            send_bottles(step + 1)
        else:
            bottle_delta_ref[...] = total.astype(BF16)

    send_bottles(0)
    with jax.named_scope("b6_w"):
        finish(t_c_shared)
        finish_direct(t_att_shared)
    with jax.named_scope("b6_exit"):
        gradient(0, t_c, t_att)
        send_half(temporal[0], 0)
    with jax.named_scope("b7_halve"):
        add_bottles(0)
        halve(temporal[1], 1)
        halve(temporal[0], 0)
    finish(s_nl_shared)
    finish(s_att_shared)
    with jax.named_scope("c0_w"):
        finish_direct(s_c_shared)
    with jax.named_scope("c0_mm"):
        gradient(4, s_c, s_att)
        send_half(spatial[0], 0)
        halve(temporal[2], 1)
    for n, i in enumerate((2, 1, 0)):
        with jax.named_scope("c%d_w" % (n + 1)):
            finish_direct(s_shared[i])
        with jax.named_scope("c%d_mm" % (n + 1)):
            gradient(5 + n, s_nl, s_mg.at[i])
            send_half(spatial[n + 1], 0)
        with jax.named_scope("c%d_halve" % (n + 1)):
            halve(spatial[n], 0)
            if n < 2:
                halve(temporal[3 - 3 * n], 1)
    with jax.named_scope("c4_halve"):
        halve(spatial[3], 0)
    for step in range(1, bits - 1):
        with jax.named_scope("d%d_t" % step):
            add_bottles(step)
            if step > 1:
                for it in temporal:
                    halve(it, step)
        for n, it in enumerate(spatial):
            with jax.named_scope("d%d_s%d" % (step, n)):
                halve(it, step)
    with jax.named_scope("e1_t"):
        add_bottles(bits - 1)
        for it in temporal[1:] + temporal[:1]:
            settle(it)
    for n, it in enumerate(spatial):
        with jax.named_scope("e2_s%d" % n):
            settle(it)
    with jax.named_scope("e3_drain"):
        sent.append((t_mg.at[:, pl.ds(0, data_groups - 1)], d_sem.at[5]))
        sent.append((s_mg.at[:, pl.ds(0, data_groups - 1)], d_sem.at[7]))
        sent.append((part.at[:, pl.ds(0, frame_groups - 2)], rs_sem))
        sent.append((final.at[:, pl.ds(0, 2 * column_groups - 1)], xs_sem))
        for view, sem in sent:
            drain(view, sem)
        for copy in bottle_copies:
            copy.wait_send()


def hand_over(*refs):
    count = len(refs) // 2
    for source, target in zip(refs[:count], refs[count:]):
        target[...] = source[...]


def per_device(
    frames_in,
    bottleneck,
    spatial_entry,
    spatial_exit,
    temporal_entry,
    temporal_exit,
    output_grad,
    joined_grad,
):
    clip_count, frames_local, patches, model = frames_in.shape
    bottles = bottleneck.shape[1]
    frame_groups = lax.axis_size("frame")
    data_groups = lax.axis_size("dp")
    assert clip_count == 1 and frames_local == 1
    entry_width = spatial_entry.shape[1]
    exit_width = spatial_exit.shape[1]
    group = patches // frame_groups
    assert group & (group - 1) == 0
    assert frame_groups & (frame_groups - 1) == 0 and data_groups & (data_groups - 1) == 0
    assert entry_width == 3 * exit_width and frame_groups >= 4
    bits = frame_groups.bit_length() - 1
    row_groups = 1 << ((data_groups.bit_length() - 1) // 2)
    column_groups = data_groups // row_groups
    rows = -(-(patches + bottles) // 16) * 16
    sent_rows = -(-(patches + bottles) // 8) * 8
    t_rows = patches
    wide = model // row_groups
    block = exit_width // column_groups
    owned = model // data_groups // frame_groups
    grad_factor = 1.0 / math.sqrt(patches * data_groups * frame_groups)

    def gather_set(count):
        return [
            pltpu.VMEM((row_groups, count, wide), BF16),
            pltpu.VMEM((data_groups, count, wide), BF16),
            pltpu.VMEM((column_groups, count, block), BF16),
            pltpu.VMEM((data_groups, count, block), BF16),
            pltpu.VMEM((row_groups, count, wide), BF16),
            pltpu.VMEM((data_groups, count, wide), BF16),
            pltpu.VMEM((3, column_groups, count, block), BF16),
            pltpu.VMEM((3, data_groups, count, block), BF16),
        ]

    moved = pltpu.VMEM((frame_groups, group, model), BF16)
    hbm = pl.BlockSpec(memory_space=pltpu.HBM)
    vmem = pl.BlockSpec(memory_space=pltpu.VMEM)
    out_shape = (
        jax.ShapeDtypeStruct((patches, model), BF16),
        jax.ShapeDtypeStruct((bottles, model), BF16),
        jax.ShapeDtypeStruct((owned, entry_width), BF16),
        jax.ShapeDtypeStruct((owned, exit_width), BF16),
        jax.ShapeDtypeStruct((owned, entry_width), BF16),
        jax.ShapeDtypeStruct((owned, exit_width), BF16),
    )
    outs = pl.pallas_call(
        functools.partial(kernel, frame_groups, row_groups, column_groups, grad_factor),
        out_shape=out_shape,
        in_specs=[hbm] * 8,
        out_specs=[vmem] * 6,
        scratch_shapes=[
            pltpu.VMEM((patches, model), BF16),
            pltpu.VMEM((bottles, model), BF16),
            moved,
            pltpu.VMEM((bottles, model), BF16),
            pltpu.VMEM(spatial_entry.shape, BF16),
            pltpu.VMEM(spatial_exit.shape, BF16),
            pltpu.VMEM(temporal_entry.shape, BF16),
            pltpu.VMEM(temporal_exit.shape, BF16),
            pltpu.VMEM(spatial_entry.shape[::-1], BF16),
            pltpu.VMEM(temporal_entry.shape[::-1], BF16),
            pltpu.VMEM((rows, model), F32),
            pltpu.VMEM((rows, model), F32),
            pltpu.VMEM((rows, model), F32),
            pltpu.VMEM((t_rows, model), F32),
            moved,
            moved,
            moved,
            moved,
            moved,
            *[pltpu.VMEM((frame_groups, group, exit_width), BF16)] * 2,
            pltpu.VMEM((bits, bottles, model), F32),
            pltpu.VMEM((bits, bottles, model), F32),
            *gather_set(sent_rows),
            *gather_set(t_rows),
            pltpu.VMEM((8, frame_groups, column_groups, owned, block), BF16),
            pltpu.VMEM((8, 2 * column_groups, owned, block), BF16),
            *[
                pltpu.VMEM((8, frame_groups >> s, column_groups, owned, block), BF16)
                for s in range(1, bits)
            ]
            * 2,
            pltpu.SemaphoreType.DMA((10,)),
            pltpu.SemaphoreType.DMA((2, 4)),
            pltpu.SemaphoreType.DMA((8,)),
            pltpu.SemaphoreType.DMA((15,)),
            pltpu.SemaphoreType.DMA((8, bits - 1)),
            pltpu.SemaphoreType.DMA,
            pltpu.SemaphoreType.DMA((8,)),
            pltpu.SemaphoreType.DMA,
            pltpu.SemaphoreType.DMA((2, bits)),
        ],
        compiler_params=pltpu.CompilerParams(
            collective_id=0, has_side_effects=True, vmem_limit_bytes=40 * 1024 * 1024
        ),
    )(
        *[
            pltpu.with_memory_space_constraint(x, pltpu.HBM)
            for x in (
                frames_in.reshape(patches, model),
                bottleneck.reshape(bottles, model),
                output_grad.reshape(frame_groups, group, model),
                joined_grad.reshape(bottles, model),
                spatial_entry,
                spatial_exit,
                temporal_entry,
                temporal_exit,
            )
        ]
    )
    outs = pl.pallas_call(
        hand_over,
        out_shape=[jax.ShapeDtypeStruct(out.shape, out.dtype) for out in outs],
        in_specs=[vmem] * len(outs),
        out_specs=[vmem] * len(outs),
        compiler_params=pltpu.CompilerParams(vmem_limit_bytes=40 * 1024 * 1024),
    )(*outs)
    return (outs[0].reshape(frames_in.shape), outs[1].reshape(bottleneck.shape), *outs[2:])


def solution(mesh):
    return jax.shard_map(
        per_device,
        mesh=mesh,
        in_specs=(
            P("dp", "frame", None, None),
            P("dp", None, None),
            P(),
            P(),
            P(),
            P(),
            P("dp", "frame", None, None),
            P("dp", None, None),
        ),
        out_specs=(
            P("dp", "frame", None, None),
            P("dp", None, None),
            P(("dp", "frame"), None),
            P(("dp", "frame"), None),
            P(("dp", "frame"), None),
            P(("dp", "frame"), None),
        ),
        check_vma=False,
    )
```

```python
import functools
import math

import jax
import jax.numpy as jnp
from jax import lax
from jax.experimental import pallas as pl
from jax.experimental.pallas import tpu as pltpu
from jax.sharding import PartitionSpec as P

HEADS = 8
LANES = 128
PIECES = (4, 5, 6, 7)
EPSILON = 1e-05
MESH = pl.DeviceIdType.MESH
F32 = jnp.float32
BF16 = jnp.bfloat16


def dot(left, right, left_dim=1, right_dim=0):
    return lax.dot_general(
        left, right, (((left_dim,), (right_dim,)), ((), ())), preferred_element_type=F32
    )


def normalize(widened):
    centred = widened - jnp.mean(widened, axis=-1, keepdims=True)
    inverse = lax.rsqrt(jnp.mean(centred * centred, axis=-1, keepdims=True) + EPSILON)
    return centred * inverse, inverse


def head_masks(heads, width, dtype):
    lanes = lax.broadcasted_iota(jnp.int32, (1, width), 1)
    size = width // heads
    return [
        jnp.where((lanes >= h * size) & (lanes < (h + 1) * size), 1.0, 0.0).astype(dtype)
        for h in range(heads)
    ]


def split(rows):
    width = rows.shape[1]
    lanes = max(LANES, width // HEADS)
    return [rows[:, i : i + lanes] for i in range(0, width, lanes)]


def stack_heads(rows, heads):
    return jnp.concatenate([rows * m for m in head_masks(heads, rows.shape[1], rows.dtype)], axis=0)


def merge_heads(stacked, heads):
    count = stacked.shape[0] // heads
    masks = head_masks(heads, stacked.shape[1], stacked.dtype)
    total = stacked[:count] * masks[0]
    for h in range(1, heads):
        total = total + stacked[h * count : (h + 1) * count] * masks[h]
    return total


def attend(normed_low, entry_ref, mask, ready=lambda i: None):
    width = entry_ref.shape[1] // 3
    parts = []
    for i in range(3):
        ready(i)
        parts.append(dot(normed_low, entry_ref[:, i * width : (i + 1) * width]).astype(BF16))
    factor = 1.0 / math.sqrt(width // HEADS)
    saved, attended = [], []
    for queries, key_rows, values in zip(*map(split, parts)):
        heads = HEADS * queries.shape[1] // width
        query_stack = stack_heads(queries, heads)
        scores = dot(query_stack, key_rows, 1, 1) * factor
        here = mask(scores.shape)
        scores = jnp.where(here, scores, -1e30)
        scores = scores - jnp.max(scores, axis=-1, keepdims=True)
        expon = jnp.where(here, jnp.exp(scores), 0.0)
        weights = expon / jnp.sum(expon, axis=-1, keepdims=True)
        weights_low = weights.astype(BF16)
        attended.append(merge_heads(dot(weights_low, values), heads).astype(BF16))
        saved.append((query_stack, key_rows, values, weights, weights_low))
    return jnp.concatenate(attended, axis=1), saved


def backward_mixture(cotangent, exit_ref, saved, emit):
    width = exit_ref.shape[1]
    factor = 1.0 / math.sqrt(width // HEADS)
    attended_grad = split(dot(cotangent, exit_ref[...]).astype(BF16))
    heads = HEADS * attended_grad[0].shape[1] // width
    grad_stacks = [stack_heads(g, heads) for g in attended_grad]
    values_grad = jnp.concatenate(
        [dot(s[4], g, 0, 0).astype(BF16) for s, g in zip(saved, grad_stacks)], axis=1
    )
    emit(2, values_grad)
    scores_grads = []
    for (_, _, values, weights, _), grad_stack in zip(saved, grad_stacks):
        softmax_grad = dot(grad_stack, values, 1, 1)
        centre = jnp.sum(weights * softmax_grad, axis=-1, keepdims=True)
        scores_grads.append((weights * (softmax_grad - centre) * factor).astype(BF16))
    keys_grad = jnp.concatenate(
        [dot(g, s[0], 0, 0).astype(BF16) for s, g in zip(saved, scores_grads)], axis=1
    )
    emit(1, keys_grad)
    queries_grad = jnp.concatenate(
        [merge_heads(dot(g, s[1]), heads).astype(BF16) for s, g in zip(saved, scores_grads)], axis=1
    )
    emit(0, queries_grad)
    return jnp.concatenate([queries_grad, keys_grad, values_grad], axis=1)


def backward_inputs(mixture_grad, turned_ref, cotangent, normed, inverse):
    normed_grad = dot(mixture_grad, turned_ref[...])
    inner = (
        normed_grad
        - jnp.mean(normed_grad, axis=-1, keepdims=True)
        - normed * jnp.mean(normed_grad * normed, axis=-1, keepdims=True)
    )
    return cotangent + inverse * inner


def kernel(
    frame_groups,
    row_groups,
    column_groups,
    grad_factor,
    frames_hbm,
    bottle_hbm,
    output_grad_hbm,
    joined_hbm,
    spatial_entry_hbm,
    spatial_exit_hbm,
    temporal_entry_hbm,
    temporal_exit_hbm,
    frames_delta_ref,
    bottle_delta_ref,
    spatialin_ref,
    spatialout_ref,
    temporalin_ref,
    temporalout_ref,
    frames_ref,
    bottle_ref,
    og_send,
    joined_ref,
    se_ref,
    so_ref,
    te_ref,
    to_ref,
    turned_se,
    turned_te,
    tokens,
    cot_ref,
    s_normed,
    t_normed,
    og_recv,
    st_send,
    st_recv,
    sg_send,
    sg_recv,
    at_send,
    at_recv,
    bot_sum,
    bot_recv,
    s_nl_send,
    s_nl,
    s_att_send,
    s_att,
    s_c_send,
    s_c,
    s_mg_send,
    s_mg,
    t_nl_send,
    t_nl,
    t_att_send,
    t_att,
    t_c_send,
    t_c,
    t_mg_send,
    t_mg,
    *tail,
):
    bits = frame_groups.bit_length() - 1
    part, final = tail[:2]
    received = tail[2 : 1 + bits]
    sums = (part,) + tuple(tail[1 + bits : 2 * bits])
    (
        load_sem,
        f_sem,
        d_sem,
        dr_sem,
        r_sem,
        rs_sem,
        p_sem,
        x_sem,
        xs_sem,
        b_sem,
    ) = tail[2 * bits :]
    frame = lax.axis_index("frame")
    data = lax.axis_index("dp")
    row_at = data // column_groups
    column_at = lax.rem(data, column_groups)
    data_groups = row_groups * column_groups
    patches, model = frames_ref.shape
    bottles = bottle_ref.shape[0]
    rows = tokens.shape[0]
    group = og_send.shape[1]
    width = to_ref.shape[1]
    block = width // column_groups
    owned = part.shape[3]
    side = [lax.rem(frame // (1 << s), 2) for s in range(bits)]

    loads = {}

    def load(name, src, dst):
        loads[name] = pltpu.make_async_copy(src, dst, load_sem.at[len(loads)])
        loads[name].start()

    load("frames", frames_hbm, frames_ref)
    load("bottle", bottle_hbm, bottle_ref)
    parts = [pl.ds(i * width, width) for i in range(3)]
    for i in range(3):
        load(i, spatial_entry_hbm.at[:, parts[i]], se_ref.at[:, parts[i]])

    barrier = pltpu.get_barrier_semaphore()
    for k in range(1, frame_groups):
        pl.semaphore_signal(
            barrier,
            inc=1,
            device_id={"frame": lax.rem(frame + k, frame_groups)},
            device_id_type=MESH,
        )
    for k in range(1, data_groups):
        pl.semaphore_signal(
            barrier, inc=1, device_id={"dp": lax.rem(data + k, data_groups)}, device_id_type=MESH
        )

    sent = []

    def push(src, dst, send_sem, recv_sem, device):
        copy = pltpu.make_async_remote_copy(
            src_ref=src,
            dst_ref=dst,
            send_sem=send_sem,
            recv_sem=recv_sem,
            device_id=device,
            device_id_type=MESH,
        )
        copy.start()
        return copy

    def drain(view, sem):
        pltpu.make_async_copy(view, view, sem).wait()

    def across(k):
        peer = frame
        for s in range(bits):
            if k >> s & 1:
                peer = peer + (1 << s) * (1 - 2 * side[s])
        return peer

    def exchange_frames(send, dst, phase, far_first=True):
        order = range(1, frame_groups)
        for k in reversed(order) if far_first else order:
            peer = across(k)
            push(
                send.at[peer],
                dst.at[frame],
                f_sem.at[0, phase],
                f_sem.at[1, phase],
                {"frame": peer},
            )
        dst[frame] = send[frame]
        sent.append((dst.at[pl.ds(0, frame_groups - 1)], f_sem.at[0, phase]))

    def arrive_frames(dst, phase):
        drain(dst.at[pl.ds(0, frame_groups - 1)], f_sem.at[1, phase])

    def clip(row, column):
        return row * column_groups + column

    def row_peers():
        return [lax.rem(row_at + k, row_groups) for k in range(1, row_groups)]

    def column_peers():
        return [lax.rem(column_at + k, column_groups) for k in range(1, column_groups)]

    def put_blocks(dst, value):
        count, kept, size = dst.shape
        for i in range(count):
            dst[i] = value[:kept, i * size : (i + 1) * size]

    def send_slot(phase):
        return phase if phase < 5 else 5 if phase < 8 else 6 if phase == 8 else 7

    def share(send, dst, value, by_row, phase):
        put_blocks(send, value)
        mine = row_at if by_row else column_at
        for peer_row in row_peers():
            push(
                send.at[peer_row if by_row else column_at],
                dst.at[data],
                d_sem.at[send_slot(phase)],
                dr_sem.at[phase if by_row else 12 + min(phase, 2)],
                {"dp": clip(peer_row, column_at)},
            )
        for peer_column in column_peers():
            push(
                send.at[row_at if by_row else peer_column],
                dst.at[data],
                d_sem.at[send_slot(phase)],
                dr_sem.at[12 + min(phase, 2) if by_row else phase],
                {"dp": clip(row_at, peer_column)},
            )
        dst[data] = send[mine]
        sent.append((dst.at[pl.ds(0, data_groups - 1)], d_sem.at[send_slot(phase)]))
        return dst, by_row, phase

    def relay(shared):
        dst, by_row, phase = shared
        first = (row_groups if by_row else column_groups) - 1
        drain(dst.at[pl.ds(0, first)], dr_sem.at[phase])
        for peer_row in row_peers():
            for peer_column in column_peers():
                source = clip(peer_row, column_at) if by_row else clip(row_at, peer_column)
                target = clip(row_at, peer_column) if by_row else clip(peer_row, column_at)
                push(
                    dst.at[source],
                    dst.at[source],
                    d_sem.at[send_slot(phase)],
                    dr_sem.at[12 + min(phase, 2)],
                    {"dp": target},
                )

    def finish(shared):
        dst, by_row, phase = shared
        first = (row_groups if by_row else column_groups) - 1
        drain(dst.at[pl.ds(0, data_groups - 1 - first)], dr_sem.at[12 + min(phase, 2)])

    def share_direct(send, dst, value, by_row, phase):
        put_blocks(send, value)
        for k in reversed(range(1, data_groups)):
            peer_row = lax.rem(row_at + k // column_groups, row_groups)
            peer_column = lax.rem(column_at + k % column_groups, column_groups)
            push(
                send.at[peer_row if by_row else peer_column],
                dst.at[data],
                d_sem.at[send_slot(phase)],
                dr_sem.at[phase],
                {"dp": clip(peer_row, peer_column)},
            )
        dst[data] = send[row_at if by_row else column_at]
        if send_slot(phase) not in (5, 7):
            sent.append((dst.at[pl.ds(0, data_groups - 1)], d_sem.at[send_slot(phase)]))
        return dst, by_row, phase

    def finish_direct(shared):
        dst, _, phase = shared
        drain(dst.at[pl.ds(0, data_groups - 1)], dr_sem.at[phase])

    def gradient(slot, left, right):
        def product_of(low, high):
            count = (high - low) * data_groups
            pieces = [ref[:, low:high] for ref in (left, right)]
            if (high - low) % 16:
                pieces = [p.astype(F32) for p in pieces]
            pieces = [p.reshape(count, p.shape[2]).astype(BF16) for p in pieces]
            return dot(pieces[0], pieces[1], 0, 0)

        product = product_of(0, patches)
        if left.shape[1] > patches:
            product = product + product_of(patches, left.shape[1])
        for f in range(frame_groups):
            place = sum((f >> s & 1) << (bits - 1 - s) for s in range(bits))
            for c in range(column_groups):
                start = (c * frame_groups + f) * owned
                part[slot, place, c] = product[start : start + owned].astype(BF16)

    def send_half(item, step):
        first, count, index = item
        half = frame_groups >> (step + 1)
        slots = pl.ds(first, count)
        away = pl.ds((1 - side[step]) * half, half)
        if step == bits - 2 and index in PIECES:
            for k in reversed(range(column_groups)):
                column = lax.rem(column_at + k, column_groups)
                push(
                    sums[step].at[slots, away, column],
                    received[step].at[slots, :, column],
                    rs_sem,
                    p_sem.at[PIECES.index(index), k],
                    {"frame": across(1 << step)},
                )
            return
        push(
            sums[step].at[slots, away],
            received[step].at[slots],
            rs_sem,
            r_sem.at[index, step],
            {"frame": across(1 << step)},
        )

    def send_owner(item, k):
        first, count, index = item
        step = bits - 1
        slots = pl.ds(first, count)
        owner = lax.rem(column_at + k, column_groups)
        for far in (1, 0) if k else (1,):
            push(
                sums[step].at[slots, 1 - side[step] if far else side[step], owner],
                final.at[slots, far * column_groups + column_at],
                xs_sem,
                x_sem.at[index],
                {"dp": clip(row_at, owner), "frame": across(1 << step) if far else frame},
            )
        if not k:
            for slot in range(first, first + count):
                final[slot, column_at] = sums[step][slot, side[step], column_at]

    def halve(item, step):
        first, count, index = item
        half = frame_groups >> (step + 1)
        near = pl.ds(side[step] * half, half)
        if step == bits - 2 and index in PIECES:
            for k in reversed(range(column_groups)):
                column = lax.rem(column_at + k, column_groups)
                view = received[step].at[pl.ds(first, count), :, column]
                drain(view, p_sem.at[PIECES.index(index), k])
                for slot in range(first, first + count):
                    kept = sums[step][slot, near, column].astype(F32)
                    total = kept + received[step][slot, :, column].astype(F32)
                    sums[step + 1][slot, :, column] = total.astype(BF16)
                send_owner(item, k)
            return
        drain(received[step].at[pl.ds(first, count)], r_sem.at[index, step])
        for slot in range(first, first + count):
            kept = sums[step][slot, near].astype(F32)
            total = kept + received[step][slot].astype(F32)
            sums[step + 1][slot] = total.astype(BF16)
        if step < bits - 2:
            send_half(item, step + 1)
            return
        for k in reversed(range(column_groups)):
            send_owner(item, k)

    def settle(item):
        first, count, index = item
        drain(final.at[pl.ds(first, count), pl.ds(0, 2 * column_groups - 1)], x_sem.at[index])
        for slot in range(first, first + count):
            out, start = outputs[slot]
            for c in range(column_groups):
                near, far = final[slot, c], final[slot, column_groups + c]
                total = (near.astype(F32) + far.astype(F32)) * grad_factor
                out[:, start + c * block : start + (c + 1) * block] = total.astype(BF16)

    def flat(ref, count):
        return ref[...].astype(F32).reshape(count, ref.shape[2]).astype(BF16)

    outputs = [(temporalout_ref, 0)]
    outputs += [(temporalin_ref, i * width) for i in (2, 1, 0)]
    outputs += [(spatialout_ref, 0)]
    outputs += [(spatialin_ref, i * width) for i in (2, 1, 0)]

    with jax.named_scope("a01_norm"):
        loads["frames"].wait()
        loads["bottle"].wait()
        tokens[:patches] = frames_ref[...].astype(F32)
        tokens[patches:] = jnp.zeros((rows - patches, model), F32)
        tokens[patches : patches + bottles] = bottle_ref[...].astype(F32)
        normed, s_inverse = normalize(tokens[...])
        s_normed[...] = normed
        s_low = normed.astype(BF16)
        load("so", spatial_exit_hbm, so_ref)
        load("og", output_grad_hbm, og_send)
        load("te", temporal_entry_hbm, te_ref)
        load("to", temporal_exit_hbm, to_ref)
        load("joined", joined_hbm, joined_ref)
    def real_rows(shape):
        return lax.broadcasted_iota(jnp.int32, shape, 1) < patches + bottles

    def enter(i):
        loads[i].wait()


    attended, s_saved = attend(s_low, se_ref, real_rows, enter)
    with jax.named_scope("a02_enter"):
        loads["og"].wait()
        pl.semaphore_wait(barrier, frame_groups + data_groups - 2)
        t_c_shared = share(t_c_send, t_c, flat(og_send, patches), True, 4)
        s_nl_shared = share(s_nl_send, s_nl, s_low, True, 0)
    with jax.named_scope("a02_states"):
        loads["so"].wait()
        states = (tokens[:patches] + dot(attended[:patches], so_ref[...], 1, 1)).astype(BF16)
        st_send[...] = states.astype(F32).reshape(frame_groups, group, model).astype(BF16)
    with jax.named_scope("a03_enter"):
        exchange_frames(st_send, st_recv, 0)
        exchange_frames(og_send, og_recv, 1, far_first=False)
        s_att_shared = share(s_att_send, s_att, attended, False, 1)

    t_rows = frame_groups * group
    with jax.named_scope("a04_turn"):
        loads["te"].wait()
        turned_te[...] = te_ref[...].T
        turned_se[...] = se_ref[...].T
    with jax.named_scope("a04_relays"):
        relay(t_c_shared)
        relay(s_nl_shared)
    def same_patch(shape):
        row_patch = lax.broadcasted_iota(jnp.int32, shape, 0) & (group - 1)
        column_patch = lax.broadcasted_iota(jnp.int32, shape, 1) & (group - 1)
        return row_patch == column_patch

    with jax.named_scope("a05_waitst"):
        arrive_frames(st_recv, 0)
    with jax.named_scope("a06_tempfwd"):
        normed, t_inverse = normalize(st_recv[...].astype(F32).reshape(t_rows, model))
        t_normed[...] = normed
        t_low = normed.astype(BF16)
        t_nl_shared = share_direct(t_nl_send, t_nl, t_low, True, 2)
        attended, t_saved = attend(t_low, te_ref, same_patch)
        at_send[...] = attended.astype(F32).reshape(at_send.shape).astype(BF16)
        exchange_frames(at_send, at_recv, 3)
    with jax.named_scope("a06_waitog"):
        arrive_frames(og_recv, 1)
    t_cot = og_recv[...].astype(F32).reshape(t_rows, model)
    t_cot_low = t_cot.astype(BF16)
    t_shared = {}

    def keep_temporal(i, value):
        t_shared[i] = share_direct(t_mg_send.at[i], t_mg.at[i], value, False, 5 + i)

    with jax.named_scope("a07_tempbwd"):
        loads["to"].wait()
        mixture_grad = backward_mixture(t_cot_low, to_ref, t_saved, keep_temporal)
        state_grads = backward_inputs(mixture_grad, turned_te, t_cot, t_normed[...], t_inverse)
        sg_send[...] = state_grads.reshape(frame_groups, group, model).astype(BF16)
        exchange_frames(sg_send, sg_recv, 2)

    with jax.named_scope("a08_relays"):
        relay(s_att_shared)
        arrive_frames(at_recv, 3)
        t_att_shared = share_direct(t_att_send, t_att, flat(at_recv, patches), False, 3)
        cot_ref[patches:] = jnp.zeros((rows - patches, model), F32)
        loads["joined"].wait()
        cot_ref[patches : patches + bottles] = (
            (joined_ref[...].astype(F32) / frame_groups).astype(BF16).astype(F32)
        )
    temporal = [(slot, 1, slot) for slot in range(4)]
    spatial = [(4 + slot, 1, 4 + slot) for slot in range(4)]
    def reduce_entry(slot):
        finish_direct(t_shared[3 - slot])
        gradient(slot, t_nl, t_mg.at[3 - slot])
        send_half(temporal[slot], 0)

    with jax.named_scope("b1_first"):
        finish_direct(t_nl_shared)
        reduce_entry(1)
    with jax.named_scope("a09_waitsg"):
        arrive_frames(sg_recv, 2)
    cot_ref[:patches] = sg_recv[...].astype(F32).reshape(patches, model)
    s_cot_low = cot_ref[...].astype(BF16)
    s_c_shared = share_direct(s_c_send, s_c, s_cot_low, True, 8)
    s_shared = {}

    def keep_spatial(i, value):
        s_shared[i] = share_direct(s_mg_send.at[i], s_mg.at[i], value, False, 9 + i)
        if i == 2:
            with jax.named_scope("b3_third"):
                halve(temporal[2], 0)
                reduce_entry(3)
        if i == 0:
            halve(temporal[3], 0)

    with jax.named_scope("b2_second"):
        halve(temporal[1], 0)
        reduce_entry(2)
    with jax.named_scope("b3_spatbwd"):
        mixture_grad = backward_mixture(s_cot_low, so_ref, s_saved, keep_spatial)
    with jax.named_scope("b4_inputs"):
        tokens_grad = backward_inputs(mixture_grad, turned_se, cot_ref[...], s_normed[...], s_inverse)
        frames_delta_ref[...] = tokens_grad[:patches].astype(BF16)
        bot_sum[0] = tokens_grad[patches : patches + bottles]

    bottle_copies = []

    def send_bottles(step):
        bottle_copies.append(
            push(
                bot_sum.at[step],
                bot_recv.at[step],
                b_sem.at[0, step],
                b_sem.at[1, step],
                {"frame": across(1 << step)},
            )
        )

    def add_bottles(step):
        bottle_copies[step].wait_recv()
        total = bot_sum[step] + bot_recv[step]
        if step < bits - 1:
            bot_sum[step + 1] = total
            send_bottles(step + 1)
        else:
            bottle_delta_ref[...] = total.astype(BF16)

    send_bottles(0)
    with jax.named_scope("b6_w"):
        finish(t_c_shared)
        finish_direct(t_att_shared)
    with jax.named_scope("b6_exit"):
        gradient(0, t_c, t_att)
        send_half(temporal[0], 0)
    with jax.named_scope("b7_halve"):
        add_bottles(0)
        halve(temporal[1], 1)
        halve(temporal[0], 0)
    finish(s_nl_shared)
    finish(s_att_shared)
    with jax.named_scope("c0_w"):
        finish_direct(s_c_shared)
    with jax.named_scope("c0_mm"):
        gradient(4, s_c, s_att)
        send_half(spatial[0], 0)
        halve(temporal[2], 1)
    for n, i in enumerate((2, 1, 0)):
        with jax.named_scope("c%d_w" % (n + 1)):
            finish_direct(s_shared[i])
        with jax.named_scope("c%d_mm" % (n + 1)):
            gradient(5 + n, s_nl, s_mg.at[i])
            send_half(spatial[n + 1], 0)
        with jax.named_scope("c%d_halve" % (n + 1)):
            halve(spatial[n], 0)
            if n < 2:
                halve(temporal[3 - 3 * n], 1)
    with jax.named_scope("c4_halve"):
        halve(spatial[3], 0)
    for step in range(1, bits - 1):
        with jax.named_scope("d%d_t" % step):
            add_bottles(step)
            if step > 1:
                for it in temporal:
                    halve(it, step)
        for n, it in enumerate(spatial):
            with jax.named_scope("d%d_s%d" % (step, n)):
                halve(it, step)
    with jax.named_scope("e1_t"):
        add_bottles(bits - 1)
        for it in temporal[1:] + temporal[:1]:
            settle(it)
    for n, it in enumerate(spatial):
        with jax.named_scope("e2_s%d" % n):
            settle(it)
    with jax.named_scope("e3_drain"):
        sent.append((t_mg.at[:, pl.ds(0, data_groups - 1)], d_sem.at[5]))
        sent.append((s_mg.at[:, pl.ds(0, data_groups - 1)], d_sem.at[7]))
        sent.append((part.at[:, pl.ds(0, frame_groups - 2)], rs_sem))
        sent.append((final.at[:, pl.ds(0, 2 * column_groups - 1)], xs_sem))
        for view, sem in sent:
            drain(view, sem)
        for copy in bottle_copies:
            copy.wait_send()


def hand_over(*refs):
    count = len(refs) // 2
    for source, target in zip(refs[:count], refs[count:]):
        target[...] = source[...]


def per_device(
    frames_in,
    bottleneck,
    spatial_entry,
    spatial_exit,
    temporal_entry,
    temporal_exit,
    output_grad,
    joined_grad,
):
    clip_count, frames_local, patches, model = frames_in.shape
    bottles = bottleneck.shape[1]
    frame_groups = lax.axis_size("frame")
    data_groups = lax.axis_size("dp")
    assert clip_count == 1 and frames_local == 1
    entry_width = spatial_entry.shape[1]
    exit_width = spatial_exit.shape[1]
    group = patches // frame_groups
    assert group & (group - 1) == 0
    assert frame_groups & (frame_groups - 1) == 0 and data_groups & (data_groups - 1) == 0
    assert entry_width == 3 * exit_width and frame_groups >= 4
    bits = frame_groups.bit_length() - 1
    row_groups = 1 << ((data_groups.bit_length() - 1) // 2)
    column_groups = data_groups // row_groups
    rows = -(-(patches + bottles) // 16) * 16
    sent_rows = -(-(patches + bottles) // 8) * 8
    t_rows = patches
    wide = model // row_groups
    block = exit_width // column_groups
    owned = model // data_groups // frame_groups
    grad_factor = 1.0 / math.sqrt(patches * data_groups * frame_groups)

    def gather_set(count):
        return [
            pltpu.VMEM((row_groups, count, wide), BF16),
            pltpu.VMEM((data_groups, count, wide), BF16),
            pltpu.VMEM((column_groups, count, block), BF16),
            pltpu.VMEM((data_groups, count, block), BF16),
            pltpu.VMEM((row_groups, count, wide), BF16),
            pltpu.VMEM((data_groups, count, wide), BF16),
            pltpu.VMEM((3, column_groups, count, block), BF16),
            pltpu.VMEM((3, data_groups, count, block), BF16),
        ]

    moved = pltpu.VMEM((frame_groups, group, model), BF16)
    hbm = pl.BlockSpec(memory_space=pltpu.HBM)
    vmem = pl.BlockSpec(memory_space=pltpu.VMEM)
    out_shape = (
        jax.ShapeDtypeStruct((patches, model), BF16),
        jax.ShapeDtypeStruct((bottles, model), BF16),
        jax.ShapeDtypeStruct((owned, entry_width), BF16),
        jax.ShapeDtypeStruct((owned, exit_width), BF16),
        jax.ShapeDtypeStruct((owned, entry_width), BF16),
        jax.ShapeDtypeStruct((owned, exit_width), BF16),
    )
    outs = pl.pallas_call(
        functools.partial(kernel, frame_groups, row_groups, column_groups, grad_factor),
        out_shape=out_shape,
        in_specs=[hbm] * 8,
        out_specs=[vmem] * 6,
        scratch_shapes=[
            pltpu.VMEM((patches, model), BF16),
            pltpu.VMEM((bottles, model), BF16),
            moved,
            pltpu.VMEM((bottles, model), BF16),
            pltpu.VMEM(spatial_entry.shape, BF16),
            pltpu.VMEM(spatial_exit.shape, BF16),
            pltpu.VMEM(temporal_entry.shape, BF16),
            pltpu.VMEM(temporal_exit.shape, BF16),
            pltpu.VMEM(spatial_entry.shape[::-1], BF16),
            pltpu.VMEM(temporal_entry.shape[::-1], BF16),
            pltpu.VMEM((rows, model), F32),
            pltpu.VMEM((rows, model), F32),
            pltpu.VMEM((rows, model), F32),
            pltpu.VMEM((t_rows, model), F32),
            moved,
            moved,
            moved,
            moved,
            moved,
            *[pltpu.VMEM((frame_groups, group, exit_width), BF16)] * 2,
            pltpu.VMEM((bits, bottles, model), F32),
            pltpu.VMEM((bits, bottles, model), F32),
            *gather_set(sent_rows),
            *gather_set(t_rows),
            pltpu.VMEM((8, frame_groups, column_groups, owned, block), BF16),
            pltpu.VMEM((8, 2 * column_groups, owned, block), BF16),
            *[
                pltpu.VMEM((8, frame_groups >> s, column_groups, owned, block), BF16)
                for s in range(1, bits)
            ]
            * 2,
            pltpu.SemaphoreType.DMA((10,)),
            pltpu.SemaphoreType.DMA((2, 4)),
            pltpu.SemaphoreType.DMA((8,)),
            pltpu.SemaphoreType.DMA((15,)),
            pltpu.SemaphoreType.DMA((8, bits - 1)),
            pltpu.SemaphoreType.DMA,
            pltpu.SemaphoreType.DMA((len(PIECES), column_groups)),
            pltpu.SemaphoreType.DMA((8,)),
            pltpu.SemaphoreType.DMA,
            pltpu.SemaphoreType.DMA((2, bits)),
        ],
        compiler_params=pltpu.CompilerParams(
            collective_id=0, has_side_effects=True, vmem_limit_bytes=40 * 1024 * 1024
        ),
    )(
        *[
            pltpu.with_memory_space_constraint(x, pltpu.HBM)
            for x in (
                frames_in.reshape(patches, model),
                bottleneck.reshape(bottles, model),
                output_grad.reshape(frame_groups, group, model),
                joined_grad.reshape(bottles, model),
                spatial_entry,
                spatial_exit,
                temporal_entry,
                temporal_exit,
            )
        ]
    )
    outs = pl.pallas_call(
        hand_over,
        out_shape=[jax.ShapeDtypeStruct(out.shape, out.dtype) for out in outs],
        in_specs=[vmem] * len(outs),
        out_specs=[vmem] * len(outs),
        compiler_params=pltpu.CompilerParams(vmem_limit_bytes=40 * 1024 * 1024),
    )(*outs)
    return (outs[0].reshape(frames_in.shape), outs[1].reshape(bottleneck.shape), *outs[2:])


def solution(mesh):
    return jax.shard_map(
        per_device,
        mesh=mesh,
        in_specs=(
            P("dp", "frame", None, None),
            P("dp", None, None),
            P(),
            P(),
            P(),
            P(),
            P("dp", "frame", None, None),
            P("dp", None, None),
        ),
        out_specs=(
            P("dp", "frame", None, None),
            P("dp", None, None),
            P(("dp", "frame"), None),
            P(("dp", "frame"), None),
            P(("dp", "frame"), None),
            P(("dp", "frame"), None),
        ),
        check_vma=False,
    )
```

```python
import functools
import math

import jax
import jax.numpy as jnp
from jax import lax
from jax.experimental import pallas as pl
from jax.experimental.pallas import tpu as pltpu
from jax.sharding import PartitionSpec as P

HEADS = 8
LANES = 128
PIECES = (5, 6, 7)
EPSILON = 1e-05
MESH = pl.DeviceIdType.MESH
F32 = jnp.float32
BF16 = jnp.bfloat16


def dot(left, right, left_dim=1, right_dim=0):
    return lax.dot_general(
        left, right, (((left_dim,), (right_dim,)), ((), ())), preferred_element_type=F32
    )


def normalize(widened):
    centred = widened - jnp.mean(widened, axis=-1, keepdims=True)
    inverse = lax.rsqrt(jnp.mean(centred * centred, axis=-1, keepdims=True) + EPSILON)
    return centred * inverse, inverse


def head_masks(heads, width, dtype):
    lanes = lax.broadcasted_iota(jnp.int32, (1, width), 1)
    size = width // heads
    return [
        jnp.where((lanes >= h * size) & (lanes < (h + 1) * size), 1.0, 0.0).astype(dtype)
        for h in range(heads)
    ]


def split(rows):
    width = rows.shape[1]
    lanes = max(LANES, width // HEADS)
    return [rows[:, i : i + lanes] for i in range(0, width, lanes)]


def stack_heads(rows, heads):
    return jnp.concatenate([rows * m for m in head_masks(heads, rows.shape[1], rows.dtype)], axis=0)


def merge_heads(stacked, heads):
    count = stacked.shape[0] // heads
    masks = head_masks(heads, stacked.shape[1], stacked.dtype)
    total = stacked[:count] * masks[0]
    for h in range(1, heads):
        total = total + stacked[h * count : (h + 1) * count] * masks[h]
    return total


def attend(normed_low, entry_ref, mask, ready=lambda i: None):
    width = entry_ref.shape[1] // 3
    parts = []
    for i in range(3):
        ready(i)
        parts.append(dot(normed_low, entry_ref[:, i * width : (i + 1) * width]).astype(BF16))
    factor = 1.0 / math.sqrt(width // HEADS)
    saved, attended = [], []
    for queries, key_rows, values in zip(*map(split, parts)):
        heads = HEADS * queries.shape[1] // width
        query_stack = stack_heads(queries, heads)
        scores = dot(query_stack, key_rows, 1, 1) * factor
        here = mask(scores.shape)
        scores = jnp.where(here, scores, -1e30)
        scores = scores - jnp.max(scores, axis=-1, keepdims=True)
        expon = jnp.where(here, jnp.exp(scores), 0.0)
        weights = expon / jnp.sum(expon, axis=-1, keepdims=True)
        weights_low = weights.astype(BF16)
        attended.append(merge_heads(dot(weights_low, values), heads).astype(BF16))
        saved.append((query_stack, key_rows, values, weights, weights_low))
    return jnp.concatenate(attended, axis=1), saved


def backward_mixture(cotangent, exit_ref, saved, emit):
    width = exit_ref.shape[1]
    factor = 1.0 / math.sqrt(width // HEADS)
    attended_grad = split(dot(cotangent, exit_ref[...]).astype(BF16))
    heads = HEADS * attended_grad[0].shape[1] // width
    grad_stacks = [stack_heads(g, heads) for g in attended_grad]
    values_grad = jnp.concatenate(
        [dot(s[4], g, 0, 0).astype(BF16) for s, g in zip(saved, grad_stacks)], axis=1
    )
    emit(2, values_grad)
    scores_grads = []
    for (_, _, values, weights, _), grad_stack in zip(saved, grad_stacks):
        softmax_grad = dot(grad_stack, values, 1, 1)
        centre = jnp.sum(weights * softmax_grad, axis=-1, keepdims=True)
        scores_grads.append((weights * (softmax_grad - centre) * factor).astype(BF16))
    keys_grad = jnp.concatenate(
        [dot(g, s[0], 0, 0).astype(BF16) for s, g in zip(saved, scores_grads)], axis=1
    )
    emit(1, keys_grad)
    queries_grad = jnp.concatenate(
        [merge_heads(dot(g, s[1]), heads).astype(BF16) for s, g in zip(saved, scores_grads)], axis=1
    )
    emit(0, queries_grad)
    return jnp.concatenate([queries_grad, keys_grad, values_grad], axis=1)


def backward_inputs(mixture_grad, turned_ref, cotangent, normed, inverse):
    normed_grad = dot(mixture_grad, turned_ref[...])
    inner = (
        normed_grad
        - jnp.mean(normed_grad, axis=-1, keepdims=True)
        - normed * jnp.mean(normed_grad * normed, axis=-1, keepdims=True)
    )
    return cotangent + inverse * inner


def kernel(
    frame_groups,
    row_groups,
    column_groups,
    grad_factor,
    frames_hbm,
    bottle_hbm,
    output_grad_hbm,
    joined_hbm,
    spatial_entry_hbm,
    spatial_exit_hbm,
    temporal_entry_hbm,
    temporal_exit_hbm,
    frames_delta_ref,
    bottle_delta_ref,
    spatialin_ref,
    spatialout_ref,
    temporalin_ref,
    temporalout_ref,
    frames_ref,
    bottle_ref,
    og_send,
    joined_ref,
    se_ref,
    so_ref,
    te_ref,
    to_ref,
    turned_se,
    turned_te,
    tokens,
    cot_ref,
    s_normed,
    t_normed,
    og_recv,
    st_send,
    st_recv,
    sg_send,
    sg_recv,
    at_send,
    at_recv,
    bot_sum,
    bot_recv,
    s_nl_send,
    s_nl,
    s_att_send,
    s_att,
    s_c_send,
    s_c,
    s_mg_send,
    s_mg,
    t_nl_send,
    t_nl,
    t_att_send,
    t_att,
    t_c_send,
    t_c,
    t_mg_send,
    t_mg,
    *tail,
):
    bits = frame_groups.bit_length() - 1
    part, final = tail[:2]
    received = tail[2 : 1 + bits]
    sums = (part,) + tuple(tail[1 + bits : 2 * bits])
    (
        load_sem,
        f_sem,
        d_sem,
        dr_sem,
        r_sem,
        rs_sem,
        p_sem,
        x_sem,
        xs_sem,
        b_sem,
    ) = tail[2 * bits :]
    frame = lax.axis_index("frame")
    data = lax.axis_index("dp")
    row_at = data // column_groups
    column_at = lax.rem(data, column_groups)
    data_groups = row_groups * column_groups
    patches, model = frames_ref.shape
    bottles = bottle_ref.shape[0]
    rows = tokens.shape[0]
    group = og_send.shape[1]
    width = to_ref.shape[1]
    block = width // column_groups
    owned = part.shape[3]
    side = [lax.rem(frame // (1 << s), 2) for s in range(bits)]

    loads = {}

    def load(name, src, dst):
        loads[name] = pltpu.make_async_copy(src, dst, load_sem.at[len(loads)])
        loads[name].start()

    load("frames", frames_hbm, frames_ref)
    load("bottle", bottle_hbm, bottle_ref)
    parts = [pl.ds(i * width, width) for i in range(3)]
    for i in range(3):
        load(i, spatial_entry_hbm.at[:, parts[i]], se_ref.at[:, parts[i]])

    barrier = pltpu.get_barrier_semaphore()
    for k in range(1, frame_groups):
        pl.semaphore_signal(
            barrier,
            inc=1,
            device_id={"frame": lax.rem(frame + k, frame_groups)},
            device_id_type=MESH,
        )
    for k in range(1, data_groups):
        pl.semaphore_signal(
            barrier, inc=1, device_id={"dp": lax.rem(data + k, data_groups)}, device_id_type=MESH
        )

    sent = []

    def push(src, dst, send_sem, recv_sem, device):
        copy = pltpu.make_async_remote_copy(
            src_ref=src,
            dst_ref=dst,
            send_sem=send_sem,
            recv_sem=recv_sem,
            device_id=device,
            device_id_type=MESH,
        )
        copy.start()
        return copy

    def drain(view, sem):
        pltpu.make_async_copy(view, view, sem).wait()

    def across(k):
        peer = frame
        for s in range(bits):
            if k >> s & 1:
                peer = peer + (1 << s) * (1 - 2 * side[s])
        return peer

    near = list(range(1, frame_groups))

    def exchange_frames(send, dst, phase, order):
        for k in order:
            peer = across(k)
            push(
                send.at[peer],
                dst.at[frame],
                f_sem.at[0, phase],
                f_sem.at[1, phase],
                {"frame": peer},
            )
        dst[frame] = send[frame]
        sent.append((dst.at[pl.ds(0, frame_groups - 1)], f_sem.at[0, phase]))

    def arrive_frames(dst, phase):
        drain(dst.at[pl.ds(0, frame_groups - 1)], f_sem.at[1, phase])

    def clip(row, column):
        return row * column_groups + column

    def row_peers():
        return [lax.rem(row_at + k, row_groups) for k in range(1, row_groups)]

    def column_peers():
        return [lax.rem(column_at + k, column_groups) for k in range(1, column_groups)]

    def put_blocks(dst, value):
        count, kept, size = dst.shape
        for i in range(count):
            dst[i] = value[:kept, i * size : (i + 1) * size]

    def send_slot(phase):
        return phase if phase < 5 else 5 if phase < 8 else 6 if phase == 8 else 7

    def share(send, dst, value, by_row, phase):
        put_blocks(send, value)
        mine = row_at if by_row else column_at
        for peer_row in row_peers():
            push(
                send.at[peer_row if by_row else column_at],
                dst.at[data],
                d_sem.at[send_slot(phase)],
                dr_sem.at[phase if by_row else 12 + min(phase, 2)],
                {"dp": clip(peer_row, column_at)},
            )
        for peer_column in column_peers():
            push(
                send.at[row_at if by_row else peer_column],
                dst.at[data],
                d_sem.at[send_slot(phase)],
                dr_sem.at[12 + min(phase, 2) if by_row else phase],
                {"dp": clip(row_at, peer_column)},
            )
        dst[data] = send[mine]
        sent.append((dst.at[pl.ds(0, data_groups - 1)], d_sem.at[send_slot(phase)]))
        return dst, by_row, phase

    def relay(shared):
        dst, by_row, phase = shared
        first = (row_groups if by_row else column_groups) - 1
        drain(dst.at[pl.ds(0, first)], dr_sem.at[phase])
        for peer_row in row_peers():
            for peer_column in column_peers():
                source = clip(peer_row, column_at) if by_row else clip(row_at, peer_column)
                target = clip(row_at, peer_column) if by_row else clip(peer_row, column_at)
                push(
                    dst.at[source],
                    dst.at[source],
                    d_sem.at[send_slot(phase)],
                    dr_sem.at[12 + min(phase, 2)],
                    {"dp": target},
                )

    def finish(shared):
        dst, by_row, phase = shared
        first = (row_groups if by_row else column_groups) - 1
        drain(dst.at[pl.ds(0, data_groups - 1 - first)], dr_sem.at[12 + min(phase, 2)])

    def share_direct(send, dst, value, by_row, phase):
        put_blocks(send, value)
        for k in reversed(range(1, data_groups)):
            peer_row = lax.rem(row_at + k // column_groups, row_groups)
            peer_column = lax.rem(column_at + k % column_groups, column_groups)
            push(
                send.at[peer_row if by_row else peer_column],
                dst.at[data],
                d_sem.at[send_slot(phase)],
                dr_sem.at[phase],
                {"dp": clip(peer_row, peer_column)},
            )
        dst[data] = send[row_at if by_row else column_at]
        if send_slot(phase) not in (5, 7):
            sent.append((dst.at[pl.ds(0, data_groups - 1)], d_sem.at[send_slot(phase)]))
        return dst, by_row, phase

    def finish_direct(shared):
        dst, _, phase = shared
        drain(dst.at[pl.ds(0, data_groups - 1)], dr_sem.at[phase])

    def gradient(slot, left, right):
        def product_of(low, high):
            count = (high - low) * data_groups
            pieces = [ref[:, low:high] for ref in (left, right)]
            if (high - low) % 16:
                pieces = [p.astype(F32) for p in pieces]
            pieces = [p.reshape(count, p.shape[2]).astype(BF16) for p in pieces]
            return dot(pieces[0], pieces[1], 0, 0)

        product = product_of(0, patches)
        if left.shape[1] > patches:
            product = product + product_of(patches, left.shape[1])
        for f in range(frame_groups):
            place = sum((f >> s & 1) << (bits - 1 - s) for s in range(bits))
            for c in range(column_groups):
                start = (c * frame_groups + f) * owned
                part[slot, place, c] = product[start : start + owned].astype(BF16)

    def send_half(item, step):
        first, count, index = item
        half = frame_groups >> (step + 1)
        slots = pl.ds(first, count)
        away = pl.ds((1 - side[step]) * half, half)
        if step == bits - 2 and index in PIECES:
            for k in reversed(range(column_groups)):
                column = lax.rem(column_at + k, column_groups)
                push(
                    sums[step].at[slots, away, column],
                    received[step].at[slots, :, column],
                    rs_sem,
                    p_sem.at[PIECES.index(index), k],
                    {"frame": across(1 << step)},
                )
            return
        push(
            sums[step].at[slots, away],
            received[step].at[slots],
            rs_sem,
            r_sem.at[index, step],
            {"frame": across(1 << step)},
        )

    def send_owner(item, k):
        first, count, index = item
        step = bits - 1
        slots = pl.ds(first, count)
        owner = lax.rem(column_at + k, column_groups)
        for far in (1, 0) if k else (1,):
            push(
                sums[step].at[slots, 1 - side[step] if far else side[step], owner],
                final.at[slots, far * column_groups + column_at],
                xs_sem,
                x_sem.at[index],
                {"dp": clip(row_at, owner), "frame": across(1 << step) if far else frame},
            )
        if not k:
            for slot in range(first, first + count):
                final[slot, column_at] = sums[step][slot, side[step], column_at]

    def halve(item, step):
        first, count, index = item
        half = frame_groups >> (step + 1)
        near = pl.ds(side[step] * half, half)
        if step == bits - 2 and index in PIECES:
            for k in reversed(range(column_groups)):
                column = lax.rem(column_at + k, column_groups)
                view = received[step].at[pl.ds(first, count), :, column]
                drain(view, p_sem.at[PIECES.index(index), k])
                for slot in range(first, first + count):
                    kept = sums[step][slot, near, column].astype(F32)
                    total = kept + received[step][slot, :, column].astype(F32)
                    sums[step + 1][slot, :, column] = total.astype(BF16)
                send_owner(item, k)
            return
        drain(received[step].at[pl.ds(first, count)], r_sem.at[index, step])
        for slot in range(first, first + count):
            kept = sums[step][slot, near].astype(F32)
            total = kept + received[step][slot].astype(F32)
            sums[step + 1][slot] = total.astype(BF16)
        if step < bits - 2:
            send_half(item, step + 1)
            return
        for k in reversed(range(column_groups)):
            send_owner(item, k)

    def settle(item):
        first, count, index = item
        drain(final.at[pl.ds(first, count), pl.ds(0, 2 * column_groups - 1)], x_sem.at[index])
        for slot in range(first, first + count):
            out, start = outputs[slot]
            for c in range(column_groups):
                near, far = final[slot, c], final[slot, column_groups + c]
                total = (near.astype(F32) + far.astype(F32)) * grad_factor
                out[:, start + c * block : start + (c + 1) * block] = total.astype(BF16)

    def flat(ref, count):
        return ref[...].astype(F32).reshape(count, ref.shape[2]).astype(BF16)

    outputs = [(temporalout_ref, 0)]
    outputs += [(temporalin_ref, i * width) for i in (2, 1, 0)]
    outputs += [(spatialout_ref, 0)]
    outputs += [(spatialin_ref, i * width) for i in (2, 1, 0)]

    with jax.named_scope("a01_norm"):
        loads["frames"].wait()
        loads["bottle"].wait()
        tokens[:patches] = frames_ref[...].astype(F32)
        tokens[patches:] = jnp.zeros((rows - patches, model), F32)
        tokens[patches : patches + bottles] = bottle_ref[...].astype(F32)
        normed, s_inverse = normalize(tokens[...])
        s_normed[...] = normed
        s_low = normed.astype(BF16)
        load("so", spatial_exit_hbm, so_ref)
        load("og", output_grad_hbm, og_send)
        load("te", temporal_entry_hbm, te_ref)
        load("to", temporal_exit_hbm, to_ref)
        load("joined", joined_hbm, joined_ref)
    def real_rows(shape):
        return lax.broadcasted_iota(jnp.int32, shape, 1) < patches + bottles

    def enter(i):
        loads[i].wait()


    attended, s_saved = attend(s_low, se_ref, real_rows, enter)
    with jax.named_scope("a02_enter"):
        loads["og"].wait()
        pl.semaphore_wait(barrier, frame_groups + data_groups - 2)
        t_c_shared = share(t_c_send, t_c, flat(og_send, patches), True, 4)
        s_nl_shared = share(s_nl_send, s_nl, s_low, True, 0)
    with jax.named_scope("a02_states"):
        loads["so"].wait()
        states = (tokens[:patches] + dot(attended[:patches], so_ref[...], 1, 1)).astype(BF16)
        st_send[...] = states.astype(F32).reshape(frame_groups, group, model).astype(BF16)
    with jax.named_scope("a03_enter"):
        exchange_frames(st_send, st_recv, 0, near[::-1])
        exchange_frames(og_send, og_recv, 1, near)
        s_att_shared = share(s_att_send, s_att, attended, False, 1)

    t_rows = frame_groups * group
    with jax.named_scope("a04_turn"):
        loads["te"].wait()
        turned_te[...] = te_ref[...].T
        turned_se[...] = se_ref[...].T
    with jax.named_scope("a04_relays"):
        relay(t_c_shared)
        relay(s_nl_shared)
    def same_patch(shape):
        row_patch = lax.broadcasted_iota(jnp.int32, shape, 0) & (group - 1)
        column_patch = lax.broadcasted_iota(jnp.int32, shape, 1) & (group - 1)
        return row_patch == column_patch

    with jax.named_scope("a05_waitst"):
        arrive_frames(st_recv, 0)
    with jax.named_scope("a06_tempfwd"):
        normed, t_inverse = normalize(st_recv[...].astype(F32).reshape(t_rows, model))
        t_normed[...] = normed
        t_low = normed.astype(BF16)
        t_nl_shared = share_direct(t_nl_send, t_nl, t_low, True, 2)
        attended, t_saved = attend(t_low, te_ref, same_patch)
        at_send[...] = attended.astype(F32).reshape(at_send.shape).astype(BF16)
        exchange_frames(at_send, at_recv, 3, near)
    with jax.named_scope("a06_waitog"):
        arrive_frames(og_recv, 1)
    t_cot = og_recv[...].astype(F32).reshape(t_rows, model)
    t_cot_low = t_cot.astype(BF16)
    t_shared = {}

    def keep_temporal(i, value):
        t_shared[i] = share_direct(t_mg_send.at[i], t_mg.at[i], value, False, 5 + i)

    with jax.named_scope("a07_tempbwd"):
        loads["to"].wait()
        mixture_grad = backward_mixture(t_cot_low, to_ref, t_saved, keep_temporal)
        state_grads = backward_inputs(mixture_grad, turned_te, t_cot, t_normed[...], t_inverse)
        sg_send[...] = state_grads.reshape(frame_groups, group, model).astype(BF16)
        exchange_frames(sg_send, sg_recv, 2, near[::-1])

    with jax.named_scope("a08_relays"):
        relay(s_att_shared)
        arrive_frames(at_recv, 3)
        t_att_shared = share_direct(t_att_send, t_att, flat(at_recv, patches), False, 3)
        cot_ref[patches:] = jnp.zeros((rows - patches, model), F32)
        loads["joined"].wait()
        cot_ref[patches : patches + bottles] = (
            (joined_ref[...].astype(F32) / frame_groups).astype(BF16).astype(F32)
        )
    temporal = [(slot, 1, slot) for slot in range(4)]
    spatial = [(4 + slot, 1, 4 + slot) for slot in range(4)]
    def reduce_entry(slot):
        finish_direct(t_shared[3 - slot])
        gradient(slot, t_nl, t_mg.at[3 - slot])
        send_half(temporal[slot], 0)

    with jax.named_scope("b1_first"):
        finish_direct(t_nl_shared)
        reduce_entry(1)
    with jax.named_scope("a09_waitsg"):
        arrive_frames(sg_recv, 2)
    cot_ref[:patches] = sg_recv[...].astype(F32).reshape(patches, model)
    s_cot_low = cot_ref[...].astype(BF16)
    s_c_shared = share_direct(s_c_send, s_c, s_cot_low, True, 8)
    s_shared = {}

    def keep_spatial(i, value):
        s_shared[i] = share_direct(s_mg_send.at[i], s_mg.at[i], value, False, 9 + i)
        if i == 2:
            with jax.named_scope("b3_third"):
                halve(temporal[2], 0)
                reduce_entry(3)
        if i == 0:
            halve(temporal[3], 0)

    with jax.named_scope("b2_second"):
        halve(temporal[1], 0)
        reduce_entry(2)
    with jax.named_scope("b3_spatbwd"):
        mixture_grad = backward_mixture(s_cot_low, so_ref, s_saved, keep_spatial)
    with jax.named_scope("b4_inputs"):
        tokens_grad = backward_inputs(mixture_grad, turned_se, cot_ref[...], s_normed[...], s_inverse)
        frames_delta_ref[...] = tokens_grad[:patches].astype(BF16)
        bot_sum[0] = tokens_grad[patches : patches + bottles]

    bottle_copies = []

    def send_bottles(step):
        bottle_copies.append(
            push(
                bot_sum.at[step],
                bot_recv.at[step],
                b_sem.at[0, step],
                b_sem.at[1, step],
                {"frame": across(1 << step)},
            )
        )

    def add_bottles(step):
        bottle_copies[step].wait_recv()
        total = bot_sum[step] + bot_recv[step]
        if step < bits - 1:
            bot_sum[step + 1] = total
            send_bottles(step + 1)
        else:
            bottle_delta_ref[...] = total.astype(BF16)

    send_bottles(0)
    with jax.named_scope("b6_w"):
        finish(t_c_shared)
        finish_direct(t_att_shared)
    with jax.named_scope("b6_exit"):
        gradient(0, t_c, t_att)
        send_half(temporal[0], 0)
    with jax.named_scope("b7_halve"):
        add_bottles(0)
        halve(temporal[1], 1)
        halve(temporal[0], 0)
    finish(s_nl_shared)
    finish(s_att_shared)
    with jax.named_scope("c0_w"):
        finish_direct(s_c_shared)
    with jax.named_scope("c0_mm"):
        gradient(4, s_c, s_att)
        send_half(spatial[0], 0)
        halve(temporal[2], 1)
    for n, i in enumerate((2, 1, 0)):
        with jax.named_scope("c%d_w" % (n + 1)):
            finish_direct(s_shared[i])
        with jax.named_scope("c%d_mm" % (n + 1)):
            gradient(5 + n, s_nl, s_mg.at[i])
            send_half(spatial[n + 1], 0)
        with jax.named_scope("c%d_halve" % (n + 1)):
            halve(spatial[n], 0)
            if n < 2:
                halve(temporal[3 - 3 * n], 1)
            else:
                halve(spatial[0], 1)
    with jax.named_scope("c4_halve"):
        halve(spatial[3], 0)
    for step in range(1, bits - 1):
        with jax.named_scope("d%d_t" % step):
            add_bottles(step)
            if step > 1:
                for it in temporal:
                    halve(it, step)
        for n, it in enumerate(spatial):
            with jax.named_scope("d%d_s%d" % (step, n)):
                if n or step > 1:
                    halve(it, step)
    with jax.named_scope("e1_t"):
        add_bottles(bits - 1)
        for it in temporal[1:] + temporal[:1]:
            settle(it)
    for n, it in enumerate(spatial):
        with jax.named_scope("e2_s%d" % n):
            settle(it)
    with jax.named_scope("e3_drain"):
        sent.append((t_mg.at[:, pl.ds(0, data_groups - 1)], d_sem.at[5]))
        sent.append((s_mg.at[:, pl.ds(0, data_groups - 1)], d_sem.at[7]))
        sent.append((part.at[:, pl.ds(0, frame_groups - 2)], rs_sem))
        sent.append((final.at[:, pl.ds(0, 2 * column_groups - 1)], xs_sem))
        for view, sem in sent:
            drain(view, sem)
        for copy in bottle_copies:
            copy.wait_send()


def hand_over(*refs):
    count = len(refs) // 2
    for source, target in zip(refs[:count], refs[count:]):
        target[...] = source[...]


def per_device(
    frames_in,
    bottleneck,
    spatial_entry,
    spatial_exit,
    temporal_entry,
    temporal_exit,
    output_grad,
    joined_grad,
):
    clip_count, frames_local, patches, model = frames_in.shape
    bottles = bottleneck.shape[1]
    frame_groups = lax.axis_size("frame")
    data_groups = lax.axis_size("dp")
    assert clip_count == 1 and frames_local == 1
    entry_width = spatial_entry.shape[1]
    exit_width = spatial_exit.shape[1]
    group = patches // frame_groups
    assert group & (group - 1) == 0
    assert frame_groups & (frame_groups - 1) == 0 and data_groups & (data_groups - 1) == 0
    assert entry_width == 3 * exit_width and frame_groups >= 4
    bits = frame_groups.bit_length() - 1
    row_groups = 1 << ((data_groups.bit_length() - 1) // 2)
    column_groups = data_groups // row_groups
    rows = -(-(patches + bottles) // 16) * 16
    sent_rows = -(-(patches + bottles) // 8) * 8
    t_rows = patches
    wide = model // row_groups
    block = exit_width // column_groups
    owned = model // data_groups // frame_groups
    grad_factor = 1.0 / math.sqrt(patches * data_groups * frame_groups)

    def gather_set(count):
        return [
            pltpu.VMEM((row_groups, count, wide), BF16),
            pltpu.VMEM((data_groups, count, wide), BF16),
            pltpu.VMEM((column_groups, count, block), BF16),
            pltpu.VMEM((data_groups, count, block), BF16),
            pltpu.VMEM((row_groups, count, wide), BF16),
            pltpu.VMEM((data_groups, count, wide), BF16),
            pltpu.VMEM((3, column_groups, count, block), BF16),
            pltpu.VMEM((3, data_groups, count, block), BF16),
        ]

    moved = pltpu.VMEM((frame_groups, group, model), BF16)
    hbm = pl.BlockSpec(memory_space=pltpu.HBM)
    vmem = pl.BlockSpec(memory_space=pltpu.VMEM)
    out_shape = (
        jax.ShapeDtypeStruct((patches, model), BF16),
        jax.ShapeDtypeStruct((bottles, model), BF16),
        jax.ShapeDtypeStruct((owned, entry_width), BF16),
        jax.ShapeDtypeStruct((owned, exit_width), BF16),
        jax.ShapeDtypeStruct((owned, entry_width), BF16),
        jax.ShapeDtypeStruct((owned, exit_width), BF16),
    )
    outs = pl.pallas_call(
        functools.partial(kernel, frame_groups, row_groups, column_groups, grad_factor),
        out_shape=out_shape,
        in_specs=[hbm] * 8,
        out_specs=[vmem] * 6,
        scratch_shapes=[
            pltpu.VMEM((patches, model), BF16),
            pltpu.VMEM((bottles, model), BF16),
            moved,
            pltpu.VMEM((bottles, model), BF16),
            pltpu.VMEM(spatial_entry.shape, BF16),
            pltpu.VMEM(spatial_exit.shape, BF16),
            pltpu.VMEM(temporal_entry.shape, BF16),
            pltpu.VMEM(temporal_exit.shape, BF16),
            pltpu.VMEM(spatial_entry.shape[::-1], BF16),
            pltpu.VMEM(temporal_entry.shape[::-1], BF16),
            pltpu.VMEM((rows, model), F32),
            pltpu.VMEM((rows, model), F32),
            pltpu.VMEM((rows, model), F32),
            pltpu.VMEM((t_rows, model), F32),
            moved,
            moved,
            moved,
            moved,
            moved,
            *[pltpu.VMEM((frame_groups, group, exit_width), BF16)] * 2,
            pltpu.VMEM((bits, bottles, model), F32),
            pltpu.VMEM((bits, bottles, model), F32),
            *gather_set(sent_rows),
            *gather_set(t_rows),
            pltpu.VMEM((8, frame_groups, column_groups, owned, block), BF16),
            pltpu.VMEM((8, 2 * column_groups, owned, block), BF16),
            *[
                pltpu.VMEM((8, frame_groups >> s, column_groups, owned, block), BF16)
                for s in range(1, bits)
            ]
            * 2,
            pltpu.SemaphoreType.DMA((10,)),
            pltpu.SemaphoreType.DMA((2, 4)),
            pltpu.SemaphoreType.DMA((8,)),
            pltpu.SemaphoreType.DMA((15,)),
            pltpu.SemaphoreType.DMA((8, bits - 1)),
            pltpu.SemaphoreType.DMA,
            pltpu.SemaphoreType.DMA((len(PIECES), column_groups)),
            pltpu.SemaphoreType.DMA((8,)),
            pltpu.SemaphoreType.DMA,
            pltpu.SemaphoreType.DMA((2, bits)),
        ],
        compiler_params=pltpu.CompilerParams(
            collective_id=0, has_side_effects=True, vmem_limit_bytes=40 * 1024 * 1024
        ),
    )(
        *[
            pltpu.with_memory_space_constraint(x, pltpu.HBM)
            for x in (
                frames_in.reshape(patches, model),
                bottleneck.reshape(bottles, model),
                output_grad.reshape(frame_groups, group, model),
                joined_grad.reshape(bottles, model),
                spatial_entry,
                spatial_exit,
                temporal_entry,
                temporal_exit,
            )
        ]
    )
    outs = pl.pallas_call(
        hand_over,
        out_shape=[jax.ShapeDtypeStruct(out.shape, out.dtype) for out in outs],
        in_specs=[vmem] * len(outs),
        out_specs=[vmem] * len(outs),
        compiler_params=pltpu.CompilerParams(vmem_limit_bytes=40 * 1024 * 1024),
    )(*outs)
    return (outs[0].reshape(frames_in.shape), outs[1].reshape(bottleneck.shape), *outs[2:])


def solution(mesh):
    return jax.shard_map(
        per_device,
        mesh=mesh,
        in_specs=(
            P("dp", "frame", None, None),
            P("dp", None, None),
            P(),
            P(),
            P(),
            P(),
            P("dp", "frame", None, None),
            P("dp", None, None),
        ),
        out_specs=(
            P("dp", "frame", None, None),
            P("dp", None, None),
            P(("dp", "frame"), None),
            P(("dp", "frame"), None),
            P(("dp", "frame"), None),
            P(("dp", "frame"), None),
        ),
        check_vma=False,
    )
```

```python
import functools
import math

import jax
import jax.numpy as jnp
from jax import lax
from jax.experimental import pallas as pl
from jax.experimental.pallas import tpu as pltpu
from jax.sharding import PartitionSpec as P

HEADS = 8
LANES = 128
PIECES = (6, 7)
EPSILON = 1e-05
MESH = pl.DeviceIdType.MESH
F32 = jnp.float32
BF16 = jnp.bfloat16


def dot(left, right, left_dim=1, right_dim=0):
    return lax.dot_general(
        left, right, (((left_dim,), (right_dim,)), ((), ())), preferred_element_type=F32
    )


def normalize(widened):
    centred = widened - jnp.mean(widened, axis=-1, keepdims=True)
    inverse = lax.rsqrt(jnp.mean(centred * centred, axis=-1, keepdims=True) + EPSILON)
    return centred * inverse, inverse


def head_masks(heads, width, dtype):
    lanes = lax.broadcasted_iota(jnp.int32, (1, width), 1)
    size = width // heads
    return [
        jnp.where((lanes >= h * size) & (lanes < (h + 1) * size), 1.0, 0.0).astype(dtype)
        for h in range(heads)
    ]


def split(rows):
    width = rows.shape[1]
    lanes = max(LANES, width // HEADS)
    return [rows[:, i : i + lanes] for i in range(0, width, lanes)]


def stack_heads(rows, heads):
    return jnp.concatenate([rows * m for m in head_masks(heads, rows.shape[1], rows.dtype)], axis=0)


def merge_heads(stacked, heads):
    count = stacked.shape[0] // heads
    masks = head_masks(heads, stacked.shape[1], stacked.dtype)
    total = stacked[:count] * masks[0]
    for h in range(1, heads):
        total = total + stacked[h * count : (h + 1) * count] * masks[h]
    return total


def attend(normed_low, entry_ref, mask, ready=lambda i: None):
    width = entry_ref.shape[1] // 3
    parts = []
    for i in range(3):
        ready(i)
        parts.append(dot(normed_low, entry_ref[:, i * width : (i + 1) * width]).astype(BF16))
    factor = 1.0 / math.sqrt(width // HEADS)
    saved, attended = [], []
    for queries, key_rows, values in zip(*map(split, parts)):
        heads = HEADS * queries.shape[1] // width
        query_stack = stack_heads(queries, heads)
        scores = dot(query_stack, key_rows, 1, 1) * factor
        here = mask(scores.shape)
        scores = jnp.where(here, scores, -1e30)
        scores = scores - jnp.max(scores, axis=-1, keepdims=True)
        expon = jnp.where(here, jnp.exp(scores), 0.0)
        weights = expon / jnp.sum(expon, axis=-1, keepdims=True)
        weights_low = weights.astype(BF16)
        attended.append(merge_heads(dot(weights_low, values), heads).astype(BF16))
        saved.append((query_stack, key_rows, values, weights, weights_low))
    return jnp.concatenate(attended, axis=1), saved


def backward_mixture(cotangent, exit_ref, saved, emit):
    width = exit_ref.shape[1]
    factor = 1.0 / math.sqrt(width // HEADS)
    attended_grad = split(dot(cotangent, exit_ref[...]).astype(BF16))
    heads = HEADS * attended_grad[0].shape[1] // width
    grad_stacks = [stack_heads(g, heads) for g in attended_grad]
    values_grad = jnp.concatenate(
        [dot(s[4], g, 0, 0).astype(BF16) for s, g in zip(saved, grad_stacks)], axis=1
    )
    emit(2, values_grad)
    scores_grads = []
    for (_, _, values, weights, _), grad_stack in zip(saved, grad_stacks):
        softmax_grad = dot(grad_stack, values, 1, 1)
        centre = jnp.sum(weights * softmax_grad, axis=-1, keepdims=True)
        scores_grads.append((weights * (softmax_grad - centre) * factor).astype(BF16))
    keys_grad = jnp.concatenate(
        [dot(g, s[0], 0, 0).astype(BF16) for s, g in zip(saved, scores_grads)], axis=1
    )
    emit(1, keys_grad)
    queries_grad = jnp.concatenate(
        [merge_heads(dot(g, s[1]), heads).astype(BF16) for s, g in zip(saved, scores_grads)], axis=1
    )
    emit(0, queries_grad)
    return jnp.concatenate([queries_grad, keys_grad, values_grad], axis=1)


def backward_inputs(mixture_grad, turned_ref, cotangent, normed, inverse):
    normed_grad = dot(mixture_grad, turned_ref[...])
    inner = (
        normed_grad
        - jnp.mean(normed_grad, axis=-1, keepdims=True)
        - normed * jnp.mean(normed_grad * normed, axis=-1, keepdims=True)
    )
    return cotangent + inverse * inner


def kernel(
    frame_groups,
    row_groups,
    column_groups,
    grad_factor,
    frames_hbm,
    bottle_hbm,
    output_grad_hbm,
    joined_hbm,
    spatial_entry_hbm,
    spatial_exit_hbm,
    temporal_entry_hbm,
    temporal_exit_hbm,
    frames_delta_ref,
    bottle_delta_ref,
    spatialin_ref,
    spatialout_ref,
    temporalin_ref,
    temporalout_ref,
    frames_ref,
    bottle_ref,
    og_send,
    joined_ref,
    se_ref,
    so_ref,
    te_ref,
    to_ref,
    turned_se,
    turned_te,
    tokens,
    cot_ref,
    s_normed,
    t_normed,
    og_recv,
    st_send,
    st_recv,
    sg_send,
    sg_recv,
    at_send,
    at_recv,
    bot_sum,
    bot_recv,
    s_nl_send,
    s_nl,
    s_att_send,
    s_att,
    s_c_send,
    s_c,
    s_mg_send,
    s_mg,
    t_nl_send,
    t_nl,
    t_att_send,
    t_att,
    t_c_send,
    t_c,
    t_mg_send,
    t_mg,
    *tail,
):
    bits = frame_groups.bit_length() - 1
    part, final = tail[:2]
    received = tail[2 : 1 + bits]
    sums = (part,) + tuple(tail[1 + bits : 2 * bits])
    (
        load_sem,
        f_sem,
        d_sem,
        dr_sem,
        r_sem,
        rs_sem,
        p_sem,
        x_sem,
        xs_sem,
        b_sem,
    ) = tail[2 * bits :]
    frame = lax.axis_index("frame")
    data = lax.axis_index("dp")
    row_at = data // column_groups
    column_at = lax.rem(data, column_groups)
    data_groups = row_groups * column_groups
    patches, model = frames_ref.shape
    bottles = bottle_ref.shape[0]
    rows = tokens.shape[0]
    group = og_send.shape[1]
    width = to_ref.shape[1]
    block = width // column_groups
    owned = part.shape[3]
    side = [lax.rem(frame // (1 << s), 2) for s in range(bits)]

    loads = {}

    def load(name, src, dst):
        loads[name] = pltpu.make_async_copy(src, dst, load_sem.at[len(loads)])
        loads[name].start()

    load("frames", frames_hbm, frames_ref)
    load("bottle", bottle_hbm, bottle_ref)
    parts = [pl.ds(i * width, width) for i in range(3)]
    for i in range(3):
        load(i, spatial_entry_hbm.at[:, parts[i]], se_ref.at[:, parts[i]])

    barrier = pltpu.get_barrier_semaphore()
    for k in range(1, frame_groups):
        pl.semaphore_signal(
            barrier,
            inc=1,
            device_id={"frame": lax.rem(frame + k, frame_groups)},
            device_id_type=MESH,
        )
    for k in range(1, data_groups):
        pl.semaphore_signal(
            barrier, inc=1, device_id={"dp": lax.rem(data + k, data_groups)}, device_id_type=MESH
        )

    sent = []

    def push(src, dst, send_sem, recv_sem, device):
        copy = pltpu.make_async_remote_copy(
            src_ref=src,
            dst_ref=dst,
            send_sem=send_sem,
            recv_sem=recv_sem,
            device_id=device,
            device_id_type=MESH,
        )
        copy.start()
        return copy

    def drain(view, sem):
        pltpu.make_async_copy(view, view, sem).wait()

    def across(k):
        peer = frame
        for s in range(bits):
            if k >> s & 1:
                peer = peer + (1 << s) * (1 - 2 * side[s])
        return peer

    near = list(range(1, frame_groups))

    def exchange_frames(send, dst, phase, order):
        for k in order:
            peer = across(k)
            push(
                send.at[peer],
                dst.at[frame],
                f_sem.at[0, phase],
                f_sem.at[1, phase],
                {"frame": peer},
            )
        dst[frame] = send[frame]
        sent.append((dst.at[pl.ds(0, frame_groups - 1)], f_sem.at[0, phase]))

    def arrive_frames(dst, phase):
        drain(dst.at[pl.ds(0, frame_groups - 1)], f_sem.at[1, phase])

    def clip(row, column):
        return row * column_groups + column

    def row_peers():
        return [lax.rem(row_at + k, row_groups) for k in range(1, row_groups)]

    def column_peers():
        return [lax.rem(column_at + k, column_groups) for k in range(1, column_groups)]

    def put_blocks(dst, value):
        count, kept, size = dst.shape
        for i in range(count):
            dst[i] = value[:kept, i * size : (i + 1) * size]

    def send_slot(phase):
        return phase if phase < 5 else 5 if phase < 8 else 6 if phase == 8 else 7

    def share(send, dst, value, by_row, phase):
        put_blocks(send, value)
        mine = row_at if by_row else column_at
        for peer_row in row_peers():
            push(
                send.at[peer_row if by_row else column_at],
                dst.at[data],
                d_sem.at[send_slot(phase)],
                dr_sem.at[phase if by_row else 12 + min(phase, 2)],
                {"dp": clip(peer_row, column_at)},
            )
        for peer_column in column_peers():
            push(
                send.at[row_at if by_row else peer_column],
                dst.at[data],
                d_sem.at[send_slot(phase)],
                dr_sem.at[12 + min(phase, 2) if by_row else phase],
                {"dp": clip(row_at, peer_column)},
            )
        dst[data] = send[mine]
        sent.append((dst.at[pl.ds(0, data_groups - 1)], d_sem.at[send_slot(phase)]))
        return dst, by_row, phase

    def relay(shared):
        dst, by_row, phase = shared
        first = (row_groups if by_row else column_groups) - 1
        drain(dst.at[pl.ds(0, first)], dr_sem.at[phase])
        for peer_row in row_peers():
            for peer_column in column_peers():
                source = clip(peer_row, column_at) if by_row else clip(row_at, peer_column)
                target = clip(row_at, peer_column) if by_row else clip(peer_row, column_at)
                push(
                    dst.at[source],
                    dst.at[source],
                    d_sem.at[send_slot(phase)],
                    dr_sem.at[12 + min(phase, 2)],
                    {"dp": target},
                )

    def finish(shared):
        dst, by_row, phase = shared
        first = (row_groups if by_row else column_groups) - 1
        drain(dst.at[pl.ds(0, data_groups - 1 - first)], dr_sem.at[12 + min(phase, 2)])

    def share_direct(send, dst, value, by_row, phase):
        put_blocks(send, value)
        for k in reversed(range(1, data_groups)):
            peer_row = lax.rem(row_at + k // column_groups, row_groups)
            peer_column = lax.rem(column_at + k % column_groups, column_groups)
            push(
                send.at[peer_row if by_row else peer_column],
                dst.at[data],
                d_sem.at[send_slot(phase)],
                dr_sem.at[phase],
                {"dp": clip(peer_row, peer_column)},
            )
        dst[data] = send[row_at if by_row else column_at]
        if send_slot(phase) not in (5, 7):
            sent.append((dst.at[pl.ds(0, data_groups - 1)], d_sem.at[send_slot(phase)]))
        return dst, by_row, phase

    def finish_direct(shared):
        dst, _, phase = shared
        drain(dst.at[pl.ds(0, data_groups - 1)], dr_sem.at[phase])

    def gradient(slot, left, right):
        def product_of(low, high):
            count = (high - low) * data_groups
            pieces = [ref[:, low:high] for ref in (left, right)]
            if (high - low) % 16:
                pieces = [p.astype(F32) for p in pieces]
            pieces = [p.reshape(count, p.shape[2]).astype(BF16) for p in pieces]
            return dot(pieces[0], pieces[1], 0, 0)

        product = product_of(0, patches)
        if left.shape[1] > patches:
            product = product + product_of(patches, left.shape[1])
        for f in range(frame_groups):
            place = sum((f >> s & 1) << (bits - 1 - s) for s in range(bits))
            for c in range(column_groups):
                start = (c * frame_groups + f) * owned
                part[slot, place, c] = product[start : start + owned].astype(BF16)

    def send_half(item, step):
        first, count, index = item
        half = frame_groups >> (step + 1)
        slots = pl.ds(first, count)
        away = pl.ds((1 - side[step]) * half, half)
        if step == bits - 2 and index in PIECES:
            for k in reversed(range(column_groups)):
                column = lax.rem(column_at + k, column_groups)
                push(
                    sums[step].at[slots, away, column],
                    received[step].at[slots, :, column],
                    rs_sem,
                    p_sem.at[PIECES.index(index), k],
                    {"frame": across(1 << step)},
                )
            return
        push(
            sums[step].at[slots, away],
            received[step].at[slots],
            rs_sem,
            r_sem.at[index, step],
            {"frame": across(1 << step)},
        )

    def send_owner(item, k):
        first, count, index = item
        step = bits - 1
        slots = pl.ds(first, count)
        owner = lax.rem(column_at + k, column_groups)
        for far in (1, 0) if k else (1,):
            push(
                sums[step].at[slots, 1 - side[step] if far else side[step], owner],
                final.at[slots, far * column_groups + column_at],
                xs_sem,
                x_sem.at[index],
                {"dp": clip(row_at, owner), "frame": across(1 << step) if far else frame},
            )
        if not k:
            for slot in range(first, first + count):
                final[slot, column_at] = sums[step][slot, side[step], column_at]

    def halve(item, step):
        first, count, index = item
        half = frame_groups >> (step + 1)
        near = pl.ds(side[step] * half, half)
        if step == bits - 2 and index in PIECES:
            for k in reversed(range(column_groups)):
                column = lax.rem(column_at + k, column_groups)
                view = received[step].at[pl.ds(first, count), :, column]
                drain(view, p_sem.at[PIECES.index(index), k])
                for slot in range(first, first + count):
                    kept = sums[step][slot, near, column].astype(F32)
                    total = kept + received[step][slot, :, column].astype(F32)
                    sums[step + 1][slot, :, column] = total.astype(BF16)
                send_owner(item, k)
            return
        drain(received[step].at[pl.ds(first, count)], r_sem.at[index, step])
        for slot in range(first, first + count):
            kept = sums[step][slot, near].astype(F32)
            total = kept + received[step][slot].astype(F32)
            sums[step + 1][slot] = total.astype(BF16)
        if step < bits - 2:
            send_half(item, step + 1)
            return
        for k in reversed(range(column_groups)):
            send_owner(item, k)

    def settle(item):
        first, count, index = item
        drain(final.at[pl.ds(first, count), pl.ds(0, 2 * column_groups - 1)], x_sem.at[index])
        for slot in range(first, first + count):
            out, start = outputs[slot]
            for c in range(column_groups):
                near, far = final[slot, c], final[slot, column_groups + c]
                total = (near.astype(F32) + far.astype(F32)) * grad_factor
                out[:, start + c * block : start + (c + 1) * block] = total.astype(BF16)

    def flat(ref, count):
        return ref[...].astype(F32).reshape(count, ref.shape[2]).astype(BF16)

    outputs = [(temporalout_ref, 0)]
    outputs += [(temporalin_ref, i * width) for i in (2, 1, 0)]
    outputs += [(spatialout_ref, 0)]
    outputs += [(spatialin_ref, i * width) for i in (2, 1, 0)]

    with jax.named_scope("a01_norm"):
        loads["frames"].wait()
        loads["bottle"].wait()
        tokens[:patches] = frames_ref[...].astype(F32)
        tokens[patches:] = jnp.zeros((rows - patches, model), F32)
        tokens[patches : patches + bottles] = bottle_ref[...].astype(F32)
        normed, s_inverse = normalize(tokens[...])
        s_normed[...] = normed
        s_low = normed.astype(BF16)
        load("so", spatial_exit_hbm, so_ref)
        load("og", output_grad_hbm, og_send)
        load("te", temporal_entry_hbm, te_ref)
        load("to", temporal_exit_hbm, to_ref)
        load("joined", joined_hbm, joined_ref)
    def real_rows(shape):
        return lax.broadcasted_iota(jnp.int32, shape, 1) < patches + bottles

    def enter(i):
        loads[i].wait()


    attended, s_saved = attend(s_low, se_ref, real_rows, enter)
    with jax.named_scope("a02_enter"):
        loads["og"].wait()
        pl.semaphore_wait(barrier, frame_groups + data_groups - 2)
        t_c_shared = share(t_c_send, t_c, flat(og_send, patches), True, 4)
        s_nl_shared = share(s_nl_send, s_nl, s_low, True, 0)
    with jax.named_scope("a02_states"):
        loads["so"].wait()
        states = (tokens[:patches] + dot(attended[:patches], so_ref[...], 1, 1)).astype(BF16)
        st_send[...] = states.astype(F32).reshape(frame_groups, group, model).astype(BF16)
    with jax.named_scope("a03_enter"):
        exchange_frames(st_send, st_recv, 0, near[::-1])
        exchange_frames(og_send, og_recv, 1, near)
        s_att_shared = share(s_att_send, s_att, attended, False, 1)

    t_rows = frame_groups * group
    with jax.named_scope("a04_turn"):
        loads["te"].wait()
        turned_te[...] = te_ref[...].T
        turned_se[...] = se_ref[...].T
    with jax.named_scope("a04_relays"):
        relay(t_c_shared)
        relay(s_nl_shared)
    def same_patch(shape):
        row_patch = lax.broadcasted_iota(jnp.int32, shape, 0) & (group - 1)
        column_patch = lax.broadcasted_iota(jnp.int32, shape, 1) & (group - 1)
        return row_patch == column_patch

    with jax.named_scope("a05_waitst"):
        arrive_frames(st_recv, 0)
    with jax.named_scope("a06_tempfwd"):
        normed, t_inverse = normalize(st_recv[...].astype(F32).reshape(t_rows, model))
        t_normed[...] = normed
        t_low = normed.astype(BF16)
        t_nl_shared = share_direct(t_nl_send, t_nl, t_low, True, 2)
        attended, t_saved = attend(t_low, te_ref, same_patch)
        at_send[...] = attended.astype(F32).reshape(at_send.shape).astype(BF16)
        exchange_frames(at_send, at_recv, 3, near)
    with jax.named_scope("a06_waitog"):
        arrive_frames(og_recv, 1)
    t_cot = og_recv[...].astype(F32).reshape(t_rows, model)
    t_cot_low = t_cot.astype(BF16)
    t_shared = {}

    def keep_temporal(i, value):
        t_shared[i] = share_direct(t_mg_send.at[i], t_mg.at[i], value, False, 5 + i)

    with jax.named_scope("a07_tempbwd"):
        loads["to"].wait()
        mixture_grad = backward_mixture(t_cot_low, to_ref, t_saved, keep_temporal)
        state_grads = backward_inputs(mixture_grad, turned_te, t_cot, t_normed[...], t_inverse)
        sg_send[...] = state_grads.reshape(frame_groups, group, model).astype(BF16)
        exchange_frames(sg_send, sg_recv, 2, near[::-1])

    with jax.named_scope("a08_relays"):
        relay(s_att_shared)
        arrive_frames(at_recv, 3)
        t_att_shared = share_direct(t_att_send, t_att, flat(at_recv, patches), False, 3)
        cot_ref[patches:] = jnp.zeros((rows - patches, model), F32)
        loads["joined"].wait()
        cot_ref[patches : patches + bottles] = (
            (joined_ref[...].astype(F32) / frame_groups).astype(BF16).astype(F32)
        )
    temporal = [(slot, 1, slot) for slot in range(4)]
    spatial = [(4 + slot, 1, 4 + slot) for slot in range(4)]
    def reduce_entry(slot):
        finish_direct(t_shared[3 - slot])
        gradient(slot, t_nl, t_mg.at[3 - slot])
        send_half(temporal[slot], 0)

    with jax.named_scope("b1_first"):
        finish_direct(t_nl_shared)
        reduce_entry(1)
    with jax.named_scope("a09_waitsg"):
        arrive_frames(sg_recv, 2)
    cot_ref[:patches] = sg_recv[...].astype(F32).reshape(patches, model)
    s_cot_low = cot_ref[...].astype(BF16)
    s_c_shared = share_direct(s_c_send, s_c, s_cot_low, True, 8)
    s_shared = {}

    def keep_spatial(i, value):
        s_shared[i] = share_direct(s_mg_send.at[i], s_mg.at[i], value, False, 9 + i)
        if i == 2:
            with jax.named_scope("b3_third"):
                halve(temporal[2], 0)
                reduce_entry(3)
        if i == 0:
            halve(temporal[3], 0)

    with jax.named_scope("b2_second"):
        halve(temporal[1], 0)
        reduce_entry(2)
    with jax.named_scope("b3_spatbwd"):
        mixture_grad = backward_mixture(s_cot_low, so_ref, s_saved, keep_spatial)
    with jax.named_scope("b4_inputs"):
        tokens_grad = backward_inputs(mixture_grad, turned_se, cot_ref[...], s_normed[...], s_inverse)
        frames_delta_ref[...] = tokens_grad[:patches].astype(BF16)
        bot_sum[0] = tokens_grad[patches : patches + bottles]

    bottle_copies = []

    def send_bottles(step):
        bottle_copies.append(
            push(
                bot_sum.at[step],
                bot_recv.at[step],
                b_sem.at[0, step],
                b_sem.at[1, step],
                {"frame": across(1 << step)},
            )
        )

    def add_bottles(step):
        bottle_copies[step].wait_recv()
        total = bot_sum[step] + bot_recv[step]
        if step < bits - 1:
            bot_sum[step + 1] = total
            send_bottles(step + 1)
        else:
            bottle_delta_ref[...] = total.astype(BF16)

    send_bottles(0)
    with jax.named_scope("b6_w"):
        finish(t_c_shared)
        finish_direct(t_att_shared)
    with jax.named_scope("b6_exit"):
        gradient(0, t_c, t_att)
        send_half(temporal[0], 0)
    with jax.named_scope("b7_halve"):
        add_bottles(0)
        halve(temporal[1], 1)
        halve(temporal[0], 0)
    finish(s_nl_shared)
    finish(s_att_shared)
    with jax.named_scope("c0_w"):
        finish_direct(s_c_shared)
    with jax.named_scope("c0_mm"):
        gradient(4, s_c, s_att)
        send_half(spatial[0], 0)
        halve(temporal[2], 1)
    for n, i in enumerate((2, 1, 0)):
        with jax.named_scope("c%d_w" % (n + 1)):
            finish_direct(s_shared[i])
        with jax.named_scope("c%d_mm" % (n + 1)):
            gradient(5 + n, s_nl, s_mg.at[i])
            send_half(spatial[n + 1], 0)
        with jax.named_scope("c%d_halve" % (n + 1)):
            halve(spatial[n], 0)
            if n < 2:
                halve(temporal[3 - 3 * n], 1)
            else:
                halve(spatial[0], 1)
    with jax.named_scope("c4_halve"):
        halve(spatial[3], 0)
    for step in range(1, bits - 1):
        with jax.named_scope("d%d_t" % step):
            add_bottles(step)
            if step > 1:
                for it in temporal:
                    halve(it, step)
        for n, it in enumerate(spatial):
            with jax.named_scope("d%d_s%d" % (step, n)):
                if n or step > 1:
                    halve(it, step)
    with jax.named_scope("e1_t"):
        add_bottles(bits - 1)
        for it in temporal[1:] + temporal[:1]:
            settle(it)
    for n, it in enumerate(spatial):
        with jax.named_scope("e2_s%d" % n):
            settle(it)
    with jax.named_scope("e3_drain"):
        sent.append((t_mg.at[:, pl.ds(0, data_groups - 1)], d_sem.at[5]))
        sent.append((s_mg.at[:, pl.ds(0, data_groups - 1)], d_sem.at[7]))
        sent.append((part.at[:, pl.ds(0, frame_groups - 2)], rs_sem))
        sent.append((final.at[:, pl.ds(0, 2 * column_groups - 1)], xs_sem))
        for view, sem in sent:
            drain(view, sem)
        for copy in bottle_copies:
            copy.wait_send()


def hand_over(*refs):
    count = len(refs) // 2
    for source, target in zip(refs[:count], refs[count:]):
        target[...] = source[...]


def per_device(
    frames_in,
    bottleneck,
    spatial_entry,
    spatial_exit,
    temporal_entry,
    temporal_exit,
    output_grad,
    joined_grad,
):
    clip_count, frames_local, patches, model = frames_in.shape
    bottles = bottleneck.shape[1]
    frame_groups = lax.axis_size("frame")
    data_groups = lax.axis_size("dp")
    assert clip_count == 1 and frames_local == 1
    entry_width = spatial_entry.shape[1]
    exit_width = spatial_exit.shape[1]
    group = patches // frame_groups
    assert group & (group - 1) == 0
    assert frame_groups & (frame_groups - 1) == 0 and data_groups & (data_groups - 1) == 0
    assert entry_width == 3 * exit_width and frame_groups >= 4
    bits = frame_groups.bit_length() - 1
    row_groups = 1 << ((data_groups.bit_length() - 1) // 2)
    column_groups = data_groups // row_groups
    rows = -(-(patches + bottles) // 16) * 16
    sent_rows = -(-(patches + bottles) // 8) * 8
    t_rows = patches
    wide = model // row_groups
    block = exit_width // column_groups
    owned = model // data_groups // frame_groups
    grad_factor = 1.0 / math.sqrt(patches * data_groups * frame_groups)

    def gather_set(count):
        return [
            pltpu.VMEM((row_groups, count, wide), BF16),
            pltpu.VMEM((data_groups, count, wide), BF16),
            pltpu.VMEM((column_groups, count, block), BF16),
            pltpu.VMEM((data_groups, count, block), BF16),
            pltpu.VMEM((row_groups, count, wide), BF16),
            pltpu.VMEM((data_groups, count, wide), BF16),
            pltpu.VMEM((3, column_groups, count, block), BF16),
            pltpu.VMEM((3, data_groups, count, block), BF16),
        ]

    moved = pltpu.VMEM((frame_groups, group, model), BF16)
    hbm = pl.BlockSpec(memory_space=pltpu.HBM)
    vmem = pl.BlockSpec(memory_space=pltpu.VMEM)
    out_shape = (
        jax.ShapeDtypeStruct((patches, model), BF16),
        jax.ShapeDtypeStruct((bottles, model), BF16),
        jax.ShapeDtypeStruct((owned, entry_width), BF16),
        jax.ShapeDtypeStruct((owned, exit_width), BF16),
        jax.ShapeDtypeStruct((owned, entry_width), BF16),
        jax.ShapeDtypeStruct((owned, exit_width), BF16),
    )
    outs = pl.pallas_call(
        functools.partial(kernel, frame_groups, row_groups, column_groups, grad_factor),
        out_shape=out_shape,
        in_specs=[hbm] * 8,
        out_specs=[vmem] * 6,
        scratch_shapes=[
            pltpu.VMEM((patches, model), BF16),
            pltpu.VMEM((bottles, model), BF16),
            moved,
            pltpu.VMEM((bottles, model), BF16),
            pltpu.VMEM(spatial_entry.shape, BF16),
            pltpu.VMEM(spatial_exit.shape, BF16),
            pltpu.VMEM(temporal_entry.shape, BF16),
            pltpu.VMEM(temporal_exit.shape, BF16),
            pltpu.VMEM(spatial_entry.shape[::-1], BF16),
            pltpu.VMEM(temporal_entry.shape[::-1], BF16),
            pltpu.VMEM((rows, model), F32),
            pltpu.VMEM((rows, model), F32),
            pltpu.VMEM((rows, model), F32),
            pltpu.VMEM((t_rows, model), F32),
            moved,
            moved,
            moved,
            moved,
            moved,
            *[pltpu.VMEM((frame_groups, group, exit_width), BF16)] * 2,
            pltpu.VMEM((bits, bottles, model), F32),
            pltpu.VMEM((bits, bottles, model), F32),
            *gather_set(sent_rows),
            *gather_set(t_rows),
            pltpu.VMEM((8, frame_groups, column_groups, owned, block), BF16),
            pltpu.VMEM((8, 2 * column_groups, owned, block), BF16),
            *[
                pltpu.VMEM((8, frame_groups >> s, column_groups, owned, block), BF16)
                for s in range(1, bits)
            ]
            * 2,
            pltpu.SemaphoreType.DMA((10,)),
            pltpu.SemaphoreType.DMA((2, 4)),
            pltpu.SemaphoreType.DMA((8,)),
            pltpu.SemaphoreType.DMA((15,)),
            pltpu.SemaphoreType.DMA((8, bits - 1)),
            pltpu.SemaphoreType.DMA,
            pltpu.SemaphoreType.DMA((len(PIECES), column_groups)),
            pltpu.SemaphoreType.DMA((8,)),
            pltpu.SemaphoreType.DMA,
            pltpu.SemaphoreType.DMA((2, bits)),
        ],
        compiler_params=pltpu.CompilerParams(
            collective_id=0, has_side_effects=True, vmem_limit_bytes=40 * 1024 * 1024
        ),
    )(
        *[
            pltpu.with_memory_space_constraint(x, pltpu.HBM)
            for x in (
                frames_in.reshape(patches, model),
                bottleneck.reshape(bottles, model),
                output_grad.reshape(frame_groups, group, model),
                joined_grad.reshape(bottles, model),
                spatial_entry,
                spatial_exit,
                temporal_entry,
                temporal_exit,
            )
        ]
    )
    outs = pl.pallas_call(
        hand_over,
        out_shape=[jax.ShapeDtypeStruct(out.shape, out.dtype) for out in outs],
        in_specs=[vmem] * len(outs),
        out_specs=[vmem] * len(outs),
        compiler_params=pltpu.CompilerParams(vmem_limit_bytes=40 * 1024 * 1024),
    )(*outs)
    return (outs[0].reshape(frames_in.shape), outs[1].reshape(bottleneck.shape), *outs[2:])


def solution(mesh):
    return jax.shard_map(
        per_device,
        mesh=mesh,
        in_specs=(
            P("dp", "frame", None, None),
            P("dp", None, None),
            P(),
            P(),
            P(),
            P(),
            P("dp", "frame", None, None),
            P("dp", None, None),
        ),
        out_specs=(
            P("dp", "frame", None, None),
            P("dp", None, None),
            P(("dp", "frame"), None),
            P(("dp", "frame"), None),
            P(("dp", "frame"), None),
            P(("dp", "frame"), None),
        ),
        check_vma=False,
    )
```
